128 devices in a mesh: range: 32 (over y, x, core), dop: 4 (over z).
Axes of the slice: x: 4, y: 4, z: 4, core: 2. Of those that a mesh axis runs over, the one named last changes fastest.
Arguments:
- echoes: float32 [2, 128, 16, 16384], P(None, None, None, ('range', 'dop')), may hold values from -200 to 200
- triplet: int32 [128, 3], replicated, may hold values from 0 to 127, as said below
- bin_taper: float32 [128, 3], replicated, may hold values from 0.2 to 1
- phases: float32 [16], replicated, may hold values from -3.140625 to 3.140625
- excluded: int32 [128, 1024], P('dop', 'range'), may hold values 0 or 1
- guard_len: int32 [128], P('dop'), may hold values from 1 to 4, as said below
- train_len: int32 [128], P('dop'), may hold values from 32 to 64, as said below
Outputs:
- cfar_ratio: float32 [128, 16384], P('dop', 'range')
The draws below stay inside these ranges and needn't reach their ends.
Inputs may be any that keep to these rules, and one draw needn't show every extreme that they name: `triplet`: row b holds a bin below b, b itself, and a bin above b, each within 2 of b counted cyclically over 128 bins. `guard_len`: some bin has exactly 4. `train_len`: some bin has exactly 64.
All inputs are finite; a program needn't handle non-finite values. No bound on the sum of `excluded` on one device may be relied on, other than what follows from the above.
Results may differ from the reference program's by a relative error of at most 0.0003.
Values sent between devices are 32-bit elements; how exact they have to be, the bound alone decides.
No kernel may reach another device: no remote copies, remote signals or barrier semaphores. Data moves between devices by JAX's collectives and lax.ppermute only.
A program may use at most 64 MiB of HBM per device.

```python
import math
import jax
import jax.numpy as jnp
from jax import lax

CH = 16
BINS = 128
SLOTS = 3
RANGE = 16384
BLOCK = 16
NBLK = 1024
GUARD_MAX = 4
TRAIN_MAX = 64


def draw_echoes(key, part):
    keys = jax.random.split(jax.random.fold_in(key, 7), 5)
    spread = 0.6 / math.sqrt(CH)
    mix_real = jnp.eye(CH, dtype=jnp.float32)[None, :, :] + spread * jax.random.truncated_normal(keys[0], -3.0, 3.0, (BINS, CH, CH), jnp.float32)
    mix_imag = spread * jax.random.truncated_normal(keys[1], -3.0, 3.0, (BINS, CH, CH), jnp.float32)
    noise_real = jax.random.truncated_normal(keys[2], -4.0, 4.0, (BINS, CH, RANGE), jnp.float32)
    noise_imag = jax.random.truncated_normal(keys[3], -4.0, 4.0, (BINS, CH, RANGE), jnp.float32)
    level = jnp.exp(jax.random.uniform(keys[4], (BINS, RANGE), jnp.float32, math.log(0.3), math.log(3.0)))
    amplitude = jnp.sqrt(level)[:, None, :]
    highest = lax.Precision.HIGHEST
    real_out = (jnp.einsum('bij,bjr->bir', mix_real, noise_real, precision=highest) - jnp.einsum('bij,bjr->bir', mix_imag, noise_imag, precision=highest)) * amplitude
    imag_out = (jnp.einsum('bij,bjr->bir', mix_real, noise_imag, precision=highest) + jnp.einsum('bij,bjr->bir', mix_imag, noise_real, precision=highest)) * amplitude
    return jnp.stack([real_out, imag_out]).astype(jnp.float32)


def draw_triplet(key, part):
    first_key, second_key = jax.random.split(jax.random.fold_in(key, 11))
    centre = jnp.arange(BINS, dtype=jnp.int32)
    low_bin = (centre - jax.random.randint(first_key, (BINS,), 1, 3, jnp.int32)) % BINS
    high_bin = (centre + jax.random.randint(second_key, (BINS,), 1, 3, jnp.int32)) % BINS
    return jnp.stack([low_bin, centre, high_bin], axis=1).astype(jnp.int32)


def draw_guard_len(key, part):
    first_key, second_key = jax.random.split(jax.random.fold_in(key, 13))
    values = jax.random.randint(first_key, (BINS,), 1, GUARD_MAX + 1, jnp.int32)
    chosen = jax.random.randint(second_key, (), 0, BINS, jnp.int32)
    return values.at[chosen].set(GUARD_MAX).astype(jnp.int32)


def draw_train_len(key, part):
    first_key, second_key = jax.random.split(jax.random.fold_in(key, 17))
    values = jax.random.randint(first_key, (BINS,), TRAIN_MAX // 2, TRAIN_MAX + 1, jnp.int32)
    chosen = jax.random.randint(second_key, (), 0, BINS, jnp.int32)
    return values.at[chosen].set(TRAIN_MAX).astype(jnp.int32)


def plant(array, rng, least, top_value):
    place = [jax.random.randint(jax.random.fold_in(rng, axis), (), 0, length) for axis, length in enumerate(array.shape)]
    main_axis = array.shape.index(max(array.shape))
    next_to = place[:main_axis] + [(place[main_axis] + 1) % array.shape[main_axis]] + place[main_axis + 1:]
    return array.at[tuple(place)].set(least).at[tuple(next_to)].set(top_value)


def setup_inputs(seed: int = 0) -> dict:
    key_list = jax.random.split(jax.random.key(seed), 8)
    echoes = draw_echoes(jax.random.fold_in(key_list[7], 71), 0)
    triplet = draw_triplet(jax.random.fold_in(key_list[7], 71), 0)
    bin_taper = jnp.clip(jax.random.uniform(key_list[2], (BINS, SLOTS), jnp.float32, 0.2, 1.0), 0.2, 1.0)
    phases = jnp.clip(jax.random.uniform(key_list[3], (CH,), jnp.float32, -3.140625, 3.140625), -3.140625, 3.140625)
    excluded = plant((jax.random.randint(key_list[4], (BINS, NBLK), 0, 4) < 1).astype(jnp.int32), jax.random.fold_in(key_list[4], 1), 0, 1)
    guard_len = draw_guard_len(jax.random.fold_in(key_list[7], 71), 0)
    train_len = draw_train_len(jax.random.fold_in(key_list[7], 71), 0)
    return {"echoes": echoes, "triplet": triplet, "bin_taper": bin_taper, "phases": phases, "excluded": excluded, "guard_len": guard_len, "train_len": train_len}


full_precision = lax.Precision.HIGHEST
epsilon = 1e-06

def gram_blocks(snapshot, kept_mask):
    snap_real = snapshot[0]
    snap_imag = snapshot[1]
    kept_real = snap_real * kept_mask[:, None, :]
    kept_imag = snap_imag * kept_mask[:, None, :]
    cov_real = jnp.einsum('bir,bjr->bij', kept_real, snap_real, precision=full_precision) + jnp.einsum('bir,bjr->bij', kept_imag, snap_imag, precision=full_precision)
    cov_imag = jnp.einsum('bir,bjr->bij', kept_imag, snap_real, precision=full_precision) - jnp.einsum('bir,bjr->bij', kept_real, snap_imag, precision=full_precision)
    bin_count = snapshot.shape[1]
    space_time = snapshot.shape[2]
    return jnp.concatenate([cov_real, cov_imag], axis=1).reshape(bin_count, 2 * space_time * space_time)

def solve_system(gram_term, taper_rows, phases, total_range):
    bin_count = gram_term.shape[0]
    space_time = taper_rows.shape[1] * phases.shape[0]
    blocks = gram_term.reshape(bin_count, 2, space_time, space_time)
    real_part = blocks[:, 0]
    imag_part = blocks[:, 1]
    system = jnp.concatenate([jnp.concatenate([real_part, -imag_part], axis=2), jnp.concatenate([imag_part, real_part], axis=2)], axis=1) / total_range
    cosines = (taper_rows[:, :, None] * jnp.cos(phases)[None, None, :]).reshape(bin_count, space_time)
    sines = (taper_rows[:, :, None] * jnp.sin(phases)[None, None, :]).reshape(bin_count, space_time)
    right_side = jnp.concatenate([cosines, sines], axis=1)[:, :, None]
    factor = jnp.linalg.cholesky(system)
    halfway = lax.linalg.triangular_solve(factor, right_side, left_side=True, lower=True)
    solved = lax.linalg.triangular_solve(factor, halfway, left_side=True, lower=True, transpose_a=True)
    return solved[:, :, 0]

def apply_weights(snapshot, weights):
    space_time = snapshot.shape[2]
    weight_real = weights[:, :space_time]
    weight_imag = weights[:, space_time:]
    real_out = jnp.einsum('bi,bir->br', weight_real, snapshot[0], precision=full_precision) + jnp.einsum('bi,bir->br', weight_imag, snapshot[1], precision=full_precision)
    imag_out = jnp.einsum('bi,bir->br', weight_real, snapshot[1], precision=full_precision) - jnp.einsum('bi,bir->br', weight_imag, snapshot[0], precision=full_precision)
    return real_out * real_out + imag_out * imag_out

def detect(power_map, padded, guard_len, train_len, gate_start, total_range, reach_len):
    bin_count = power_map.shape[0]
    cell_total = power_map.shape[1]
    prefix = jnp.concatenate([jnp.zeros((bin_count, 1), padded.dtype), jnp.cumsum(padded, axis=1)], axis=1)
    cell_ids = jnp.arange(cell_total, dtype=jnp.int32)[None, :]
    guard_col = guard_len[:, None].astype(jnp.int32)
    train_col = train_len[:, None].astype(jnp.int32)
    padded_at = cell_ids + reach_len
    left_sum = jnp.take_along_axis(prefix, padded_at - guard_col, axis=1) - jnp.take_along_axis(prefix, padded_at - guard_col - train_col, axis=1)
    right_sum = jnp.take_along_axis(prefix, padded_at + guard_col + train_col + 1, axis=1) - jnp.take_along_axis(prefix, padded_at + guard_col + 1, axis=1)
    position = gate_start + cell_ids
    left_count = jnp.maximum(jnp.minimum(position - guard_col - 1, total_range - 1) - jnp.maximum(position - guard_col - train_col, 0) + 1, 0)
    right_count = jnp.maximum(jnp.minimum(position + guard_col + train_col, total_range - 1) - jnp.maximum(position + guard_col + 1, 0) + 1, 0)
    noise_level = (left_sum + right_sum) / (left_count + right_count).astype(jnp.float32)
    return power_map / (noise_level + epsilon)

def reference(echoes, triplet, bin_taper, phases, excluded, guard_len, train_len):
    total_range = echoes.shape[3]
    space_time = SLOTS * CH
    kept_all = (1 - jnp.repeat(excluded, BLOCK, axis=1)).astype(jnp.float32)

    def one_bin(bin_index):
        bin_rows = lax.dynamic_slice_in_dim(triplet, bin_index, 1, 0).reshape(-1)
        snapshot = jnp.take(echoes, bin_rows, axis=1).reshape(2, 1, space_time, total_range)
        kept_mask = lax.dynamic_slice_in_dim(kept_all, bin_index, 1, 0)
        gram_term = gram_blocks(snapshot, kept_mask)
        taper_rows = lax.dynamic_slice_in_dim(bin_taper, bin_index, 1, 0)
        weights = solve_system(gram_term, taper_rows, phases, total_range)
        return apply_weights(snapshot, weights)[0]
    power_map = lax.map(one_bin, jnp.arange(BINS, dtype=jnp.int32))
    reach_len = GUARD_MAX + TRAIN_MAX
    padded = jnp.pad(power_map, ((0, 0), (reach_len, reach_len)))
    return detect(power_map, padded, guard_len, train_len, 0, total_range, reach_len)
```

```python
import functools
import jax
import jax.numpy as jnp
from jax import lax
from jax.experimental import pallas as pl
from jax.experimental.pallas import tpu as pltpu
from jax.sharding import PartitionSpec as P

CH = 16
SLOTS = 3
ST = 48
BINS = 128
BLOCK = 16
GATES = 128
TOTAL = 16384
EPS = 1e-6
HALF = 64
XN = 4
ZN = 4
f32 = jnp.float32
bf16 = jnp.bfloat16

VM = pl.BlockSpec(memory_space=pltpu.VMEM)
SM = pl.BlockSpec(memory_space=pltpu.SMEM)


def axes():
    rank = lax.axis_index("range")
    return rank % 2, (rank // 2) % XN, rank // (2 * XN), lax.axis_index("dop")


def iota(shape, dim):
    return lax.broadcasted_iota(jnp.int32, shape, dim)


def split(x):
    hi = x.astype(bf16)
    return hi, (x - hi.astype(f32)).astype(bf16)


def gram_kernel(own, trip, echo, e0, e1, e2, e3, out, kept):
    core, _, _, dop = axes()
    half = core if own else 1 - core
    block = dop * (GATES // BLOCK) + iota((32, GATES), 1) // BLOCK
    pick = (iota((32, GATES), 0) == block).astype(f32)
    for k, ref in enumerate((e0, e1, e2, e3)):
        src = lax.rem(dop - k + ZN, ZN)
        left = jnp.dot(ref[...].astype(f32), pick, preferred_element_type=f32)
        kept[pl.ds(pl.multiple_of(src * 32, 32), 32), :] = 1.0 - left

    zero = jnp.zeros((16, 2 * GATES), bf16)

    def operands(b):
        m = jnp.broadcast_to(kept[pl.ds(b, 1), :], (CH, GATES)).astype(bf16)
        rh, rl, xh, yh, xl, yl = [], [], [], [], [], []
        for t in range(SLOTS):
            s = trip[b * SLOTS + t]
            uh, ul = split(echo[0, s])
            vh, vl = split(echo[1, s])
            rh.append(jnp.concatenate([uh, vh], 1))
            rl.append(jnp.concatenate([ul, vl], 1))
            muh, mul, mvh, mvl = uh * m, ul * m, vh * m, vl * m
            xh.append(jnp.concatenate([muh, mvh], 1))
            yh.append(jnp.concatenate([mvh, -muh], 1))
            xl.append(jnp.concatenate([mul, mvl], 1))
            yl.append(jnp.concatenate([mvl, -mul], 1))
        return rh, rl, jnp.concatenate(xh + yh + xl + yl, 0)

    row = iota((ST, GATES), 0)
    lane = iota((ST, GATES), 1)
    low = row >= lane % HALF

    def pair(q):
        b = (q // 8) * 32 + half * 16 + (q % 8) * 2
        rha, rla, la = operands(b)
        rhb, rlb, lb = operands(b + 1)
        rhs = jnp.concatenate(rha + [zero] + rhb + [zero] + rla + [zero] + rlb + [zero], 0)
        dims = (((1,), (1,)), ((), ()))
        ga = lax.dot_general(la, rhs, dims, preferred_element_type=f32)
        gb = lax.dot_general(lb, rhs, dims, preferred_element_type=f32)
        ga = ga[:96] + ga[96:]
        gb = gb[:96] + gb[96:]
        ga = ga[:, :GATES] + ga[:, GATES:]
        gb = gb[:, :GATES] + gb[:, GATES:]
        re = jnp.where(lane < HALF, ga[:ST], gb[:ST])
        im = jnp.where(lane < HALF, ga[ST:], gb[ST:])
        out[q] = jnp.where(low, re, im)

    unroll = 2

    def step(i, c):
        for j in range(unroll):
            pair(i * unroll + j)
        return c

    lax.fori_loop(0, 32 // unroll, step, 0)


def gram(own, trip, echo, ex):
    return pl.pallas_call(
        functools.partial(gram_kernel, own),
        out_shape=jax.ShapeDtypeStruct((32, ST, GATES), f32),
        in_specs=[SM] + [VM] * 5,
        out_specs=VM,
        scratch_shapes=[pltpu.VMEM((BINS, GATES), f32)],
        name="gram_own" if own else "gram_peer",
    )(trip, echo, *ex)


def merge_kernel(axis, count, n_in, *refs):
    ins, outs = refs[:n_in], refs[n_in:]
    core, x, _, dop = axes()
    me = dop if axis == "z" else x
    size = outs[0].shape[0]
    for k, ref in enumerate(outs):
        base = lax.rem(me + k, count) * size if count > 1 else 0

        def step(i, c):
            total = ins[0][base + i]
            for r in ins[1:]:
                total = total + r[base + i]
            ref[i] = total
            return c

        if size <= 2:
            for i in range(size):
                step(i, 0)
        else:
            lax.fori_loop(0, size, step, 0)


def merge(axis, count, parts):
    size = parts[0].shape[0] // count
    return pl.pallas_call(
        functools.partial(merge_kernel, axis, count, len(parts)),
        out_shape=[jax.ShapeDtypeStruct((size, ST, GATES), f32)] * count,
        in_specs=[VM] * len(parts),
        out_specs=[VM] * count,
        name="merge_" + axis,
    )(*parts)


def solve_kernel(p0, p1, p2, p3, sr, si, out):
    row = iota((ST, GATES), 0)
    lane = iota((ST, GATES), 1)
    col = lane % HALF
    first = lane < HALF
    are, aim = [], []
    for q in range(2):
        p = (p0[q] + p1[q] + p2[q] + p3[q]) * (1.0 / TOTAL)
        full = jnp.concatenate([p, jnp.zeros((GATES - ST, GATES), f32)], 0).T
        pt = jnp.where(first, full[:ST], pltpu.roll(full[HALF : HALF + ST], HALF, 1))
        re = jnp.where(row >= col, p, pt)
        im = jnp.where(row < col, p, jnp.where(row == col, 0.0, -pt))
        aug = col >= ST
        are.append(jnp.where(aug, sr[q], re))
        aim.append(jnp.where(aug, si[q], im))
    base = jnp.where(first, 0, HALF)
    for k in range(ST):
        idx = base + k
        hit = row == k
        for q in range(2):
            cr = jnp.take_along_axis(are[q], idx, 1)
            ci = jnp.take_along_axis(aim[q], idx, 1)
            inv = 1.0 / cr[k : k + 1]
            nr = are[q][k : k + 1] * inv
            ni = aim[q][k : k + 1] * inv
            are[q] = jnp.where(hit, nr, are[q] - (cr * nr - ci * ni))
            aim[q] = jnp.where(hit, ni, aim[q] - (cr * ni + ci * nr))
    rows = []
    pad = jnp.zeros((GATES - ST, GATES), f32)
    lane1 = iota((1, GATES), 1)
    for q in range(2):
        wr = jnp.concatenate([are[q], pad], 0).T
        wi = jnp.concatenate([aim[q], pad], 0).T
        for h in (ST, HALF + ST):
            rows.append(
                jnp.where(lane1 < HALF, wr[h : h + 1], pltpu.roll(wi[h : h + 1], HALF, 1))
            )
    out[...] = jnp.concatenate(rows + [jnp.zeros((4, GATES), f32)], 0)


def solve(parts, sr, si):
    return pl.pallas_call(
        solve_kernel,
        out_shape=jax.ShapeDtypeStruct((8, GATES), f32),
        in_specs=[VM] * 6,
        out_specs=VM,
        name="solve",
    )(*parts, sr, si)


def power_kernel(trip, echo, w0, w1, o0, o1, o2, o3, wt):
    core, x, _, dop = axes()
    wt[0] = w0[...].T
    wt[1] = w1[...].T

    def one(b):
        z = b // 32
        c = lax.rem(b // 16, 2)
        bx = lax.rem(b // 4, XN)
        slot = lax.rem(dop - z + ZN, ZN) * 4 + lax.rem(x - bx + XN, XN)
        col = slot * 8 + lax.rem(b, 4)
        cc = lax.rem(c + core, 2)
        idx = jnp.full((CH, GATES), col, jnp.int32)
        re = jnp.zeros((CH, GATES), f32)
        im = jnp.zeros((CH, GATES), f32)
        for t in range(SLOTS):
            s = trip[b * SLOTS + t]
            u = echo[0, s]
            v = echo[1, s]
            wr = jnp.take_along_axis(wt[cc, t * CH : (t + 1) * CH, :], idx, 1)
            wi = jnp.take_along_axis(wt[cc, HALF + t * CH : HALF + (t + 1) * CH, :], idx, 1)
            re = re + wr * u + wi * v
            im = im + wr * v - wi * u
        re = jnp.sum(re, 0, keepdims=True)
        im = jnp.sum(im, 0, keepdims=True)
        return re * re + im * im

    for k, ref in enumerate((o0, o1, o2, o3)):
        first = lax.rem(dop + k, ZN) * 32

        def step(i, c):
            rows = [one(first + i * 8 + j) for j in range(8)]
            ref[pl.ds(pl.multiple_of(i * 8, 8), 8), :] = jnp.concatenate(rows, 0)
            return c

        lax.fori_loop(0, 4, step, 0)


def power(trip, echo, w0, w1):
    return pl.pallas_call(
        power_kernel,
        out_shape=[jax.ShapeDtypeStruct((32, GATES), f32)] * 4,
        in_specs=[SM] + [VM] * 3,
        out_specs=[VM] * 4,
        scratch_shapes=[pltpu.VMEM((2, GATES, GATES), f32)],
        name="power",
    )(trip, echo, w0, w1)


def cfar_kernel(p0, p1, p2, p3, h0, h1, h2, h3, guard, train, out, line):
    _, _, _, dop = axes()
    rank = lax.axis_index("range")
    for k, ref in enumerate((p0, p1, p2, p3)):
        line[1 + lax.rem(dop - k + ZN, ZN)] = ref[...]
    for j, ref in enumerate((h0, h1, h2, h3)):

        @pl.when(dop == (j + 3) % 4)
        def _():
            line[0] = ref[...]

        @pl.when(dop == j)
        def _():
            line[5] = ref[...]

    width = 6 * GATES
    p = jnp.concatenate([line[j] for j in range(6)], 1)
    g = guard[...]
    t = train[...]
    total = p
    acc = jnp.where((t & 1) == 1, p, 0.0)
    for k in range(1, 7):
        total = total + pltpu.roll(total, width - (1 << (k - 1)), 1)
        acc = jnp.where((t >> k) & 1 == 1, total + pltpu.roll(acc, width - (1 << k), 1), acc)
    right = acc
    shift = g + 1
    for k in range(3):
        right = jnp.where((shift >> k) & 1 == 1, pltpu.roll(right, width - (1 << k), 1), right)
    left = acc
    shift = g + t
    for k in range(7):
        left = jnp.where((shift >> k) & 1 == 1, pltpu.roll(left, 1 << k, 1), left)
    lo, hi = GATES, GATES + 4 * GATES
    both = left[:, lo:hi] + right[:, lo:hi]
    pos = rank * (4 * GATES) + iota((32, 4 * GATES), 1)
    left_count = jnp.maximum(jnp.minimum(pos - g - 1, TOTAL - 1) - jnp.maximum(pos - g - t, 0) + 1, 0)
    right_count = jnp.maximum(jnp.minimum(pos + g + t, TOTAL - 1) - jnp.maximum(pos + g + 1, 0) + 1, 0)
    noise = both / (left_count + right_count).astype(f32)
    out[...] = p[:, lo:hi] / (noise + EPS)


def cfar(parts, halos, guard, train):
    return pl.pallas_call(
        cfar_kernel,
        out_shape=jax.ShapeDtypeStruct((32, 4 * GATES), f32),
        in_specs=[VM] * 10,
        out_specs=VM,
        scratch_shapes=[pltpu.VMEM((6, 32, GATES), f32)],
        name="cfar",
    )(*parts, *halos, guard, train)


def turn(axis, k):
    if axis == "z":
        return "dop", [(i, (i + k) % ZN) for i in range(ZN)]
    pairs = []
    for y in range(4):
        for x in range(XN):
            for c in range(2):
                to = {"x": (y, (x + k) % XN, c), "y": ((y + k) % 4, x, c), "core": (y, x, 1 - c)}[axis]
                pairs.append(((y * XN + x) * 2 + c, (to[0] * XN + to[1]) * 2 + to[2]))
    return "range", pairs


def send(value, axis, k):
    return lax.ppermute(value, *turn(axis, k))


def steering(bin_taper, phases):
    core, x, _, dop = axes()
    first = dop * 32 + core * 16 + x * 4
    taper = lax.dynamic_slice_in_dim(bin_taper, first, 4, 0)

    def lay(values):
        full = (taper[:, :, None] * values[None, None, :]).reshape(2, 2, ST)
        full = jnp.broadcast_to(full[:, :, :, None], (2, 2, ST, HALF))
        return jnp.concatenate([full[:, 0], full[:, 1]], axis=2)

    return lay(jnp.cos(phases)), lay(jnp.sin(phases))


def shards(echoes, triplet, bin_taper, phases, excluded, guard_len, train_len):
    trip = triplet.reshape(-1)
    ex = [excluded] + [send(excluded, "z", k) for k in (1, 2, 3)]
    peer = gram(False, trip, echoes, ex)
    got = send(peer, "core", 1)
    mine = gram(True, trip, echoes, ex)
    pieces = merge("z", ZN, [mine, got])
    parts = [pieces[0]] + [send(pieces[k], "z", k) for k in (1, 2, 3)]
    pieces = merge("x", XN, parts)
    parts = [pieces[0]] + [send(pieces[k], "x", k) for k in (1, 2, 3)]
    (total,) = merge("y", 1, parts)
    parts = [total] + [send(total, "y", k) for k in (1, 2, 3)]
    sr, si = steering(bin_taper, phases)
    w = solve(parts, sr, si)
    w = jnp.concatenate([w] + [send(w, "x", k) for k in (1, 2, 3)], 0)
    w = jnp.concatenate([w] + [send(w, "z", k) for k in (1, 2, 3)], 0)
    other = send(w, "core", 1)
    pw = power(trip, echoes, w, other)
    parts = [pw[0]] + [send(pw[k], "z", k) for k in (1, 2, 3)]
    halos = []
    ranges = lax.axis_size("range")
    for j in range(4):
        pairs = [(r * ZN + 3, (r + 1) * ZN + (3 + j) % 4) for r in range(ranges - 1)]
        pairs += [(r * ZN, (r - 1) * ZN + j) for r in range(1, ranges)]
        halos.append(lax.ppermute(pw[j], ("range", "dop"), pairs))
    return cfar(parts, halos, guard_len[:, None], train_len[:, None])


def solution(mesh):
    placed = (
        P(None, None, None, ("range", "dop")),
        P(),
        P(),
        P(),
        P("dop", "range"),
        P("dop"),
        P("dop"),
    )
    return jax.shard_map(
        shards, mesh=mesh, in_specs=placed, out_specs=P("dop", "range"), check_vma=False
    )
```

```python
import functools
import jax
import jax.numpy as jnp
from jax import lax
from jax.experimental import pallas as pl
from jax.experimental.pallas import tpu as pltpu
from jax.sharding import PartitionSpec as P

CH = 16
SLOTS = 3
ST = 48
BINS = 128
BLOCK = 16
GATES = 128
TOTAL = 16384
EPS = 1e-6
HALF = 64
XN = 4
YN = 4
ZN = 4
f32 = jnp.float32
bf16 = jnp.bfloat16

VM = pl.BlockSpec(memory_space=pltpu.VMEM)
SM = pl.BlockSpec(memory_space=pltpu.SMEM)


def core_and_dop():
    return lax.axis_index("range") % 2, lax.axis_index("dop")


def iota(shape, dim):
    return lax.broadcasted_iota(jnp.int32, shape, dim)


def split(x):
    hi = x.astype(bf16)
    return hi, (x - hi.astype(f32)).astype(bf16)


def lanes(*parts):
    return jnp.concatenate(parts, 1)


def rows(*parts):
    return jnp.concatenate(parts, 0)


def gram_kernel(trip, near, far, m0, m1, m2, out, kept):
    core, dop = core_and_dop()
    block = dop * (GATES // BLOCK) + (iota((64, 2 * GATES), 1) % GATES) // BLOCK
    block = block + 32 * (iota((64, 2 * GATES), 1) // GATES)
    pick = (iota((64, 2 * GATES), 0) == block).astype(f32)
    masks = rows(m0[...], m1[...], m2[...]).astype(f32)
    left = 1.0 - jnp.dot(masks, pick, preferred_element_type=f32)
    for k in range(4):
        kept[dop ^ k] = left[16 * k : 16 * k + 16]

    zero = jnp.zeros((16, 4 * GATES), bf16)

    def operands(z, i):
        b = z * 32 + core * 16 + i
        m = kept[z, pl.ds(i, 1), :]
        mn = jnp.broadcast_to(m[:, :GATES], (CH, GATES)).astype(bf16)
        mf = jnp.broadcast_to(m[:, GATES:], (CH, GATES)).astype(bf16)
        rh, rl, xh, yh, xl, yl = [], [], [], [], [], []
        for t in range(SLOTS):
            s = trip[b, t]
            unh, unl = split(near[0, s])
            ufh, ufl = split(far[0, s])
            vnh, vnl = split(near[1, s])
            vfh, vfl = split(far[1, s])
            rh.append(lanes(unh, ufh, vnh, vfh))
            rl.append(lanes(unl, ufl, vnl, vfl))
            a, c, d, e = unh * mn, ufh * mf, vnh * mn, vfh * mf
            xh.append(lanes(a, c, d, e))
            yh.append(lanes(d, e, -a, -c))
            a, c, d, e = unl * mn, ufl * mf, vnl * mn, vfl * mf
            xl.append(lanes(a, c, d, e))
            yl.append(lanes(d, e, -a, -c))
        return rh, rl, rows(*xh, *yh, *xl, *yl)

    row = iota((ST, GATES), 0)
    lane = iota((ST, GATES), 1)
    low = row >= lane % HALF
    first = lane < HALF
    first24 = first[:24]

    def pair(z, i):
        rha, rla, la = operands(z, i)
        rhb, rlb, lb = operands(z, i + 1)
        rhs = rows(*rha, zero, *rhb, zero, *rla, zero, *rlb, zero)
        dims = (((1,), (1,)), ((), ()))
        ga = lax.dot_general(la, rhs, dims, preferred_element_type=f32)
        gb = lax.dot_general(lb, rhs, dims, preferred_element_type=f32)
        ga = ga[:96] + ga[96:]
        gb = gb[:96] + gb[96:]
        ga = ga[:, :GATES] + ga[:, GATES:]
        gb = gb[:, :GATES] + gb[:, GATES:]
        re = jnp.where(first, ga[:ST], gb[:ST])
        im = jnp.where(first, ga[ST:], gb[ST:])
        p = jnp.where(low, re, im)
        r = pltpu.roll(p, HALF, 1)
        out[i * ZN + z] = jnp.where(first24, p[:24], r[24:])
        out[(i + 1) * ZN + z] = jnp.where(first24, r[:24], p[24:])

    def step(j, c):
        z = j // 8
        pair(z, (j % 8) * 2)
        return c

    lax.fori_loop(0, 32, step, 0)


def gram(trip, near, far, masks):
    return pl.pallas_call(
        gram_kernel,
        out_shape=jax.ShapeDtypeStruct((64, 24, GATES), f32),
        in_specs=[SM] + [VM] * 5,
        out_specs=VM,
        scratch_shapes=[pltpu.VMEM((ZN, 16, 2 * GATES), f32)],
        name="gram",
    )(trip, near, far, *masks)


def solve_kernel(parts, taper, trig, out):
    core, dop = core_and_dop()
    b = dop * 32 + core * 16 + lax.axis_index("range") // 2
    row = iota((ST, GATES), 0)
    lane = iota((ST, GATES), 1)
    total = parts[0]
    for j in range(1, 64):
        total = total + parts[j]
    total = total * (1.0 / TOTAL)
    p = rows(total, pltpu.roll(total, HALF, 1))
    full = rows(p, jnp.zeros((GATES - ST, GATES), f32)).T[:ST]
    re = jnp.where(row >= lane, p, full)
    im = jnp.where(row < lane, p, jnp.where(row == lane, 0.0, -full))
    chan = iota((CH, GATES), 0)
    cosine = jnp.zeros((CH, GATES), f32)
    sine = jnp.zeros((CH, GATES), f32)
    for j in range(CH):
        cosine = jnp.where(chan == j, trig[j], cosine)
        sine = jnp.where(chan == j, trig[CH + j], sine)
    sr = rows(*[taper[b, t] * cosine for t in range(SLOTS)])
    si = rows(*[taper[b, t] * sine for t in range(SLOTS)])
    are = jnp.where(lane < ST, re, sr)
    aim = jnp.where(lane < ST, im, si)
    for k in range(0, ST, 2):
        i0 = jnp.full((ST, GATES), k, jnp.int32)
        i1 = jnp.full((ST, GATES), k + 1, jnp.int32)
        c0r = jnp.take_along_axis(are, i0, 1)
        c0i = jnp.take_along_axis(aim, i0, 1)
        c1r = jnp.take_along_axis(are, i1, 1)
        c1i = jnp.take_along_axis(aim, i1, 1)
        r0, q0 = are[k : k + 1], aim[k : k + 1]
        r1, q1 = are[k + 1 : k + 2], aim[k + 1 : k + 2]
        a, d = c0r[k : k + 1], c1r[k + 1 : k + 2]
        br, bi = c1r[k : k + 1], c1i[k : k + 1]
        inv = 1.0 / (a * d - (br * br + bi * bi))
        a, d, br, bi = a * inv, d * inv, br * inv, bi * inv
        n0r = d * r0 - (br * r1 - bi * q1)
        n0i = d * q0 - (br * q1 + bi * r1)
        n1r = a * r1 - (br * r0 + bi * q0)
        n1i = a * q1 - (br * q0 - bi * r0)
        ur = (c0r * n0r - c0i * n0i) + (c1r * n1r - c1i * n1i)
        ui = (c0r * n0i + c0i * n0r) + (c1r * n1i + c1i * n1r)
        are = jnp.where(row == k, n0r, jnp.where(row == k + 1, n1r, are - ur))
        aim = jnp.where(row == k, n0i, jnp.where(row == k + 1, n1i, aim - ui))
    pad = jnp.zeros((GATES - ST, GATES), f32)
    wr = rows(are, pad).T[ST : ST + 1]
    wi = rows(aim, pad).T[ST : ST + 1]
    lane1 = iota((1, GATES), 1)
    top = jnp.where(lane1 < ST, wr, pltpu.roll(wi, ST, 1))
    low = jnp.where(lane1 < ST, -wi, pltpu.roll(wr, ST, 1))
    live = lane1 < 2 * ST
    tile = rows(jnp.where(live, top, 0.0), jnp.where(live, low, 0.0), jnp.zeros((6, GATES), f32))
    for j in range(64):
        out[j] = tile


def solve(parts, taper, trig):
    return pl.pallas_call(
        solve_kernel,
        out_shape=jax.ShapeDtypeStruct((64, 8, GATES), f32),
        in_specs=[VM, SM, SM],
        out_specs=VM,
        name="solve",
    )(parts, taper, trig)


def power_kernel(trip, near, far, w, out):
    core, dop = core_and_dop()
    zero = jnp.zeros((32, 2 * GATES), bf16)

    def one(z, i):
        b = z * 32 + core * 16 + i
        uh, ul, vh, vl = [], [], [], []
        for t in range(SLOTS):
            s = trip[b, t]
            h, l = split(lanes(near[0, s], far[0, s]))
            uh.append(h)
            ul.append(l)
            h, l = split(lanes(near[1, s], far[1, s]))
            vh.append(h)
            vl.append(l)
        rhs = rows(*uh, *vh, zero, *ul, *vl, zero)
        wt = w[i * ZN + z]
        hi = wt.astype(bf16).astype(f32)
        lhs = rows(hi, wt - hi).astype(bf16)
        y = jnp.dot(lanes(lhs, lhs), rhs, preferred_element_type=f32)
        y = y[:8] + y[8:]
        y = y * y
        return y[0:1] + y[1:2]

    def step(j, c):
        z = j // 2
        i = (j % 2) * 8
        y = rows(*[one(z, i + k) for k in range(8)])
        at = pl.ds(pl.multiple_of(i, 8), 8)
        out[core * ZN + z, at, :] = y[:, :GATES]
        out[(1 - core) * ZN + z, at, :] = y[:, GATES:]
        return c

    lax.fori_loop(0, 8, step, 0)


def power(trip, near, far, w):
    return pl.pallas_call(
        power_kernel,
        out_shape=jax.ShapeDtypeStruct((8, 16, GATES), f32),
        in_specs=[SM] + [VM] * 3,
        out_specs=VM,
        name="power",
    )(trip, near, far, w)


def cfar_kernel(p, before, after, guard, train, out):
    rank = lax.axis_index("range")
    width = 6 * GATES
    pieces = [before[...]] + [rows(p[z], p[ZN + z]) for z in range(ZN)] + [after[...]]
    p = lanes(*pieces)
    row = iota((32, 1), 0)
    g = jnp.zeros((32, 1), jnp.int32)
    t = jnp.zeros((32, 1), jnp.int32)
    for j in range(32):
        g = jnp.where(row == j, guard[j], g)
        t = jnp.where(row == j, train[j], t)
    total = p
    acc = jnp.where((t & 1) == 1, p, 0.0)
    for k in range(1, 7):
        total = total + pltpu.roll(total, width - (1 << (k - 1)), 1)
        acc = jnp.where((t >> k) & 1 == 1, total + pltpu.roll(acc, width - (1 << k), 1), acc)
    right = acc
    shift = g + 1
    for k in range(3):
        right = jnp.where((shift >> k) & 1 == 1, pltpu.roll(right, width - (1 << k), 1), right)
    left = acc
    shift = g + t
    for k in range(7):
        left = jnp.where((shift >> k) & 1 == 1, pltpu.roll(left, 1 << k, 1), left)
    lo, hi = GATES, GATES + 4 * GATES
    both = left[:, lo:hi] + right[:, lo:hi]
    pos = rank * (4 * GATES) + iota((32, 4 * GATES), 1)
    left_count = jnp.maximum(jnp.minimum(pos - g - 1, TOTAL - 1) - jnp.maximum(pos - g - t, 0) + 1, 0)
    right_count = jnp.maximum(jnp.minimum(pos + g + t, TOTAL - 1) - jnp.maximum(pos + g + 1, 0) + 1, 0)
    noise = both / (left_count + right_count).astype(f32)
    out[...] = p[:, lo:hi] / (noise + EPS)


def cfar(p, before, after, guard, train):
    return pl.pallas_call(
        cfar_kernel,
        out_shape=jax.ShapeDtypeStruct((32, 4 * GATES), f32),
        in_specs=[VM] * 3 + [SM] * 2,
        out_specs=VM,
        name="cfar",
    )(p, before, after, guard, train)


BOTH = ("range", "dop")
CORE_SWAP = [(i, i ^ 1) for i in range(32)]
SAME_CORE = [
    [((y * XN + x) * 2 + c) * ZN + z for y in range(YN) for x in range(XN) for z in range(ZN)]
    for c in range(2)
]
CHIP_LINE = [[8 * i + j for j in range(8)] for i in range(16)]


def flipped(bit):
    return [(i, i ^ bit) for i in range(ZN)]


def shards(echoes, triplet, bin_taper, phases, excluded, guard_len, train_len):
    core, dop = core_and_dop()
    other = lax.ppermute(excluded, "range", CORE_SWAP)
    far = lax.ppermute(echoes, "range", CORE_SWAP)
    mine = lax.dynamic_slice_in_dim(lanes(excluded, other), core * 16, 16, 0)
    m1 = lax.ppermute(mine, "dop", flipped(1))
    m2 = lax.ppermute(rows(mine, m1), "dop", flipped(2))
    part = gram(triplet, echoes, far, [mine, m1, m2])
    part = lax.all_to_all(part, BOTH, 0, 0, tiled=True, axis_index_groups=SAME_CORE)
    trig = jnp.concatenate([jnp.cos(phases), jnp.sin(phases)])
    w = solve(part, bin_taper, trig)
    w = lax.all_to_all(w, BOTH, 0, 0, tiled=True, axis_index_groups=SAME_CORE)
    pw = power(triplet, echoes, far, w)
    pw = lax.all_to_all(pw, BOTH, 0, 0, tiled=True, axis_index_groups=CHIP_LINE)
    ranges = lax.axis_size("range")
    up = [(i, i + 1) for i in range(ranges - 1)]
    down = [(i + 1, i) for i in range(ranges - 1)]
    before = lax.ppermute(rows(pw[ZN - 1], pw[2 * ZN - 1]), "range", up)
    after = lax.ppermute(rows(pw[0], pw[ZN]), "range", down)
    return cfar(pw, before, after, guard_len, train_len)


def solution(mesh):
    placed = (
        P(None, None, None, ("range", "dop")),
        P(),
        P(),
        P(),
        P("dop", "range"),
        P("dop"),
        P("dop"),
    )
    return jax.shard_map(
        shards, mesh=mesh, in_specs=placed, out_specs=P("dop", "range"), check_vma=False
    )
```

```python
import functools
import jax
import jax.numpy as jnp
from jax import lax
from jax.experimental import pallas as pl
from jax.experimental.pallas import tpu as pltpu
from jax.sharding import PartitionSpec as P

CH = 16
SLOTS = 3
ST = 48
BINS = 128
BLOCK = 16
GATES = 128
TOTAL = 16384
EPS = 1e-6
HALF = 64
XN = 4
YN = 4
ZN = 4
f32 = jnp.float32
bf16 = jnp.bfloat16
VMEM_LIMIT = 16 * 2**20

VM = pl.BlockSpec(memory_space=pltpu.VMEM)
SM = pl.BlockSpec(memory_space=pltpu.SMEM)


def core_and_dop():
    return lax.axis_index("range") % 2, lax.axis_index("dop")


def iota(shape, dim):
    return lax.broadcasted_iota(jnp.int32, shape, dim)


def split(x):
    hi = x.astype(bf16)
    return hi, (x - hi.astype(f32)).astype(bf16)


def lanes(*parts):
    return jnp.concatenate(parts, 1)


def rows(*parts):
    return jnp.concatenate(parts, 0)


def prep_kernel(echo, out):
    def step(i, c):
        for j in range(4):
            for p in range(2):
                x = echo[p, i * 4 + j]
                hi, rest = split(x)
                x = x - hi.astype(f32)
                out[0, p, i * 4 + j] = hi
                out[1, p, i * 4 + j] = rest
                out[2, p, i * 4 + j] = (x - rest.astype(f32)).astype(bf16)
        return c

    lax.fori_loop(0, BINS // 4, step, 0)


def prep(echo, name):
    return pl.pallas_call(
        prep_kernel,
        out_shape=jax.ShapeDtypeStruct((3, 2, BINS, CH, GATES), bf16),
        in_specs=[VM],
        out_specs=VM,
        name=name,
        compiler_params=pltpu.CompilerParams(vmem_limit_bytes=VMEM_LIMIT),
    )(echo)


def gram_kernel(second, trip, near, far, *refs):
    masks = refs[: 1 if second else 2]
    done, out, kept = (refs[1], refs[2], refs[3]) if second else (None, refs[2], refs[3])
    core, dop = core_and_dop()
    block = dop * (GATES // BLOCK) + (iota((64, 2 * GATES), 1) % GATES) // BLOCK
    block = block + 32 * (iota((64, 2 * GATES), 1) // GATES)
    pick = (iota((64, 2 * GATES), 0) == block).astype(f32)
    left = 1.0 - jnp.dot(rows(*[m[...] for m in masks]).astype(f32), pick, preferred_element_type=f32)
    for k in range(2):
        kept[k] = left[16 * k : 16 * k + 16]
    zero = jnp.zeros((16, 4 * GATES), bf16)
    base = 2 if second else 0

    def operands(k, i):
        b = (dop ^ (base + k)) * 32 + core * 16 + i
        m = kept[k, pl.ds(i, 1), :]
        mn = jnp.broadcast_to(m[:, :GATES], (CH, GATES)).astype(bf16)
        mf = jnp.broadcast_to(m[:, GATES:], (CH, GATES)).astype(bf16)
        plain, left, right = [[], []], [[], []], [[], []]
        for t in range(SLOTS):
            s = trip[b, t]
            for h in range(2):
                un, uf, vn, vf = near[h, 0, s], far[h, 0, s], near[h, 1, s], far[h, 1, s]
                plain[h].append(lanes(un, uf, vn, vf))
                un, uf, vn, vf = un * mn, uf * mf, vn * mn, vf * mf
                left[h].append(lanes(un, uf, vn, vf))
                right[h].append(lanes(vn, vf, -un, -uf))
        return plain[0], plain[1], rows(*left[0], *right[0], *left[1], *right[1])

    row = iota((ST, GATES), 0)
    lane = iota((ST, GATES), 1)
    low = row >= lane % HALF
    first = lane < HALF
    first24 = first[:24]

    def store(k, i, value):
        if second:
            out[i * ZN + (dop ^ (2 + k))] = value
        else:
            out[k * 16 + i] = value

    def pair(k, i):
        rha, rla, la = operands(k, i)
        rhb, rlb, lb = operands(k, i + 1)
        rhs = rows(*rha, zero, *rhb, zero, *rla, zero, *rlb, zero)
        dims = (((1,), (1,)), ((), ()))
        g = lax.dot_general(rows(la, lb), rhs, dims, preferred_element_type=f32)
        ga, gb = g[:192], g[192:]
        ga = ga[:96] + ga[96:]
        gb = gb[:96] + gb[96:]
        ga = ga[:, :GATES] + ga[:, GATES:]
        gb = gb[:, :GATES] + gb[:, GATES:]
        re = jnp.where(first, ga[:ST], gb[:ST])
        im = jnp.where(first, ga[ST:], gb[ST:])
        p = jnp.where(low, re, im)
        r = pltpu.roll(p, HALF, 1)
        store(k, i, jnp.where(first24, p[:24], r[24:]))
        store(k, i + 1, jnp.where(first24, r[:24], p[24:]))

    def step(k, c):
        for i in range(0, 16, 2):
            pair(k, i)
        return c

    lax.fori_loop(0, 2, step, 0)
    if second:
        for k in range(2):
            for i in range(16):
                out[i * ZN + (dop ^ k)] = done[k * 16 + i]


def gram(second, trip, near, far, extra):
    return pl.pallas_call(
        functools.partial(gram_kernel, second),
        out_shape=jax.ShapeDtypeStruct((64 if second else 32, 24, GATES), f32),
        in_specs=[SM] + [VM] * 4,
        out_specs=VM,
        scratch_shapes=[pltpu.VMEM((2, 16, 2 * GATES), f32)],
        name="gram_b" if second else "gram_a",
        compiler_params=pltpu.CompilerParams(vmem_limit_bytes=VMEM_LIMIT),
    )(trip, near, far, *extra)


def solve_kernel(parts, taper, trig, out):
    core, dop = core_and_dop()
    b = dop * 32 + core * 16 + lax.axis_index("range") // 2
    row = iota((ST, GATES), 0)
    lane = iota((ST, GATES), 1)
    total = parts[0]
    for j in range(1, 64):
        total = total + parts[j]
    total = total * (1.0 / TOTAL)
    p = rows(total, pltpu.roll(total, HALF, 1))
    full = rows(p, jnp.zeros((GATES - ST, GATES), f32)).T[:ST]
    re = jnp.where(row >= lane, p, full)
    im = jnp.where(row < lane, p, jnp.where(row == lane, 0.0, -full))
    chan = iota((CH, GATES), 0)
    cosine = jnp.zeros((CH, GATES), f32)
    sine = jnp.zeros((CH, GATES), f32)
    for j in range(CH):
        cosine = jnp.where(chan == j, trig[j], cosine)
        sine = jnp.where(chan == j, trig[CH + j], sine)
    sr = rows(*[taper[b, t] * cosine for t in range(SLOTS)])
    si = rows(*[taper[b, t] * sine for t in range(SLOTS)])
    are = jnp.where(lane < ST, re, sr)
    aim = jnp.where(lane < ST, im, si)
    for k in range(0, ST, 2):
        i0 = jnp.full((ST, GATES), k, jnp.int32)
        i1 = jnp.full((ST, GATES), k + 1, jnp.int32)
        c0r = jnp.take_along_axis(are, i0, 1)
        c0i = jnp.take_along_axis(aim, i0, 1)
        c1r = jnp.take_along_axis(are, i1, 1)
        c1i = jnp.take_along_axis(aim, i1, 1)
        r0, q0 = are[k : k + 1], aim[k : k + 1]
        r1, q1 = are[k + 1 : k + 2], aim[k + 1 : k + 2]
        a, d = c0r[k : k + 1], c1r[k + 1 : k + 2]
        br, bi = c1r[k : k + 1], c1i[k : k + 1]
        inv = 1.0 / (a * d - (br * br + bi * bi))
        a, d, br, bi = a * inv, d * inv, br * inv, bi * inv
        n0r = d * r0 - (br * r1 - bi * q1)
        n0i = d * q0 - (br * q1 + bi * r1)
        n1r = a * r1 - (br * r0 + bi * q0)
        n1i = a * q1 - (br * q0 - bi * r0)
        ur = (c0r * n0r - c0i * n0i) + (c1r * n1r - c1i * n1i)
        ui = (c0r * n0i + c0i * n0r) + (c1r * n1i + c1i * n1r)
        are = jnp.where(row == k, n0r, jnp.where(row == k + 1, n1r, are - ur))
        aim = jnp.where(row == k, n0i, jnp.where(row == k + 1, n1i, aim - ui))
    pad = jnp.zeros((GATES - ST, GATES), f32)
    wr = rows(are, pad).T[ST : ST + 1]
    wi = rows(aim, pad).T[ST : ST + 1]
    lane1 = iota((1, GATES), 1)
    w = jnp.where(lane1 < ST, wr, jnp.where(lane1 < 2 * ST, pltpu.roll(wi, ST, 1), 0.0))
    for j in range(64):
        out[j] = w


def solve(parts, taper, trig):
    return pl.pallas_call(
        solve_kernel,
        out_shape=jax.ShapeDtypeStruct((64, 1, GATES), f32),
        in_specs=[VM, SM, SM],
        out_specs=VM,
        name="solve",
        compiler_params=pltpu.CompilerParams(vmem_limit_bytes=VMEM_LIMIT),
    )(parts, taper, trig)


def power_kernel(trip, near, far, w, own, other):
    core, dop = core_and_dop()
    zero = jnp.zeros((32, 2 * GATES), bf16)
    row = iota((8, GATES), 0)
    lane = iota((8, GATES), 1)

    def one(k, i):
        z = dop ^ k
        b = z * 32 + core * 16 + i
        wt = jnp.broadcast_to(w[i * ZN + z], (8, GATES))
        turned = jnp.where(
            lane < ST,
            -pltpu.roll(wt, GATES - ST, 1),
            jnp.where(lane < 2 * ST, pltpu.roll(wt, ST, 1), 0.0),
        )
        wt = jnp.where(row % 2 == 0, wt, turned)
        hi = wt.astype(bf16).astype(f32)
        mid = (wt - hi).astype(bf16).astype(f32)
        lo = wt - hi - mid
        wt = jnp.where(row < 2, hi, jnp.where(row < 4, mid, jnp.where(row < 6, lo, 0.0)))
        lhs = rows(wt, jnp.zeros((8, GATES), f32)).astype(bf16)
        rhs = []
        for h in range(3):
            for p in range(2):
                for t in range(SLOTS):
                    s = trip[b, t]
                    rhs.append(lanes(near[h, p, s], far[h, p, s]))
            rhs.append(zero)
        y = jnp.dot(lanes(lhs, lhs, lhs), rows(*rhs), preferred_element_type=f32)
        re = y[0:1] + y[2:3] + y[4:5]
        im = y[1:2] + y[3:4] + y[5:6]
        return re * re + im * im

    def step(j, c):
        k = j // 2
        i = (j % 2) * 8
        y = rows(*[one(k, i + n) for n in range(8)])
        at = pl.ds(pl.multiple_of(i, 8), 8)
        own[k, at, :] = y[:, :GATES]
        other[k, at, :] = y[:, GATES:]
        return c

    lax.fori_loop(0, 8, step, 0)


def power(trip, near, far, w):
    return pl.pallas_call(
        power_kernel,
        out_shape=[jax.ShapeDtypeStruct((ZN, 16, GATES), f32)] * 2,
        in_specs=[SM] + [VM] * 3,
        out_specs=[VM] * 2,
        name="power",
        compiler_params=pltpu.CompilerParams(vmem_limit_bytes=VMEM_LIMIT),
    )(trip, near, far, w)


def cfar_kernel(p0, p1, p2, p3, before, after, guard, train, out, line):
    core, dop = core_and_dop()
    rank = lax.axis_index("range")
    width = 6 * GATES
    for k, ref in enumerate((p0, p1, p2, p3)):
        at = 1 + (dop ^ k)
        line[at, core] = ref[0]
        line[at, 1 - core] = ref[1]
    for at, ref in ((0, before), (5, after)):
        line[at, 1 - core] = ref[0]
        line[at, core] = ref[1]
    p = lanes(*[rows(line[j, 0], line[j, 1]) for j in range(6)])
    row = iota((32, 1), 0)
    g = jnp.zeros((32, 1), jnp.int32)
    t = jnp.zeros((32, 1), jnp.int32)
    for j in range(32):
        g = jnp.where(row == j, guard[j], g)
        t = jnp.where(row == j, train[j], t)
    total = p
    acc = jnp.where((t & 1) == 1, p, 0.0)
    for k in range(1, 7):
        total = total + pltpu.roll(total, width - (1 << (k - 1)), 1)
        acc = jnp.where((t >> k) & 1 == 1, total + pltpu.roll(acc, width - (1 << k), 1), acc)
    right = acc
    shift = g + 1
    for k in range(3):
        right = jnp.where((shift >> k) & 1 == 1, pltpu.roll(right, width - (1 << k), 1), right)
    left = acc
    shift = g + t
    for k in range(7):
        left = jnp.where((shift >> k) & 1 == 1, pltpu.roll(left, 1 << k, 1), left)
    lo, hi = GATES, GATES + 4 * GATES
    both = left[:, lo:hi] + right[:, lo:hi]
    pos = rank * (4 * GATES) + iota((32, 4 * GATES), 1)
    left_count = jnp.maximum(jnp.minimum(pos - g - 1, TOTAL - 1) - jnp.maximum(pos - g - t, 0) + 1, 0)
    right_count = jnp.maximum(jnp.minimum(pos + g + t, TOTAL - 1) - jnp.maximum(pos + g + 1, 0) + 1, 0)
    noise = both / (left_count + right_count).astype(f32)
    out[...] = p[:, lo:hi] / (noise + EPS)


def cfar(pieces, before, after, guard, train):
    return pl.pallas_call(
        cfar_kernel,
        out_shape=jax.ShapeDtypeStruct((32, 4 * GATES), f32),
        in_specs=[VM] * 6 + [SM] * 2,
        out_specs=VM,
        scratch_shapes=[pltpu.VMEM((6, 2, 16, GATES), f32)],
        name="cfar",
        compiler_params=pltpu.CompilerParams(vmem_limit_bytes=VMEM_LIMIT),
    )(*pieces, before, after, guard, train)


BOTH = ("range", "dop")
CORE_SWAP = [(i, i ^ 1) for i in range(32)]
SAME_CORE = [
    [((y * XN + x) * 2 + c) * ZN + z for y in range(YN) for x in range(XN) for z in range(ZN)]
    for c in range(2)
]


def flipped(bit):
    return [(i, i ^ bit) for i in range(ZN)]


def swap(value):
    return lax.ppermute(value, "range", CORE_SWAP)


def shards(echoes, triplet, bin_taper, phases, excluded, guard_len, train_len):
    core, dop = core_and_dop()
    other = swap(excluded)
    ready, other = lax.optimization_barrier((echoes, other))
    far = prep(swap(ready), "prep_far")
    near = prep(echoes, "prep_near")
    mine = lax.dynamic_slice_in_dim(lanes(excluded, other), core * 16, 16, 0)
    m1 = lax.ppermute(mine, "dop", flipped(1))
    m2 = lax.ppermute(rows(mine, m1), "dop", flipped(2))
    part = gram(False, triplet, near, far, [mine, m1])
    part = gram(True, triplet, near, far, [m2, part])
    part = lax.all_to_all(part, BOTH, 0, 0, tiled=True, axis_index_groups=SAME_CORE)
    trig = jnp.concatenate([jnp.cos(phases), jnp.sin(phases)])
    w = solve(part, bin_taper, trig)
    w = lax.all_to_all(w, BOTH, 0, 0, tiled=True, axis_index_groups=SAME_CORE)
    own, away = power(triplet, near, far, w)
    came = swap(away)
    pieces = [jnp.stack([own[k], came[k]]) for k in range(ZN)]
    pieces = [pieces[0]] + [lax.ppermute(pieces[k], "dop", flipped(k)) for k in (1, 2, 3)]
    p0, p1, p2, p3 = pieces
    ranges = lax.axis_size("range")
    up = [(i, i + 1) for i in range(ranges - 1)]
    down = [(i + 1, i) for i in range(ranges - 1)]
    last = jnp.where(dop == 0, p3, jnp.where(dop == 1, p2, jnp.where(dop == 2, p1, p0)))
    head = jnp.where(dop == 0, p0, jnp.where(dop == 1, p1, jnp.where(dop == 2, p2, p3)))
    before = lax.ppermute(last, "range", up)
    after = lax.ppermute(head, "range", down)
    return cfar(pieces, before, after, guard_len, train_len)


def solution(mesh):
    placed = (
        P(None, None, None, ("range", "dop")),
        P(),
        P(),
        P(),
        P("dop", "range"),
        P("dop"),
        P("dop"),
    )
    return jax.shard_map(
        shards, mesh=mesh, in_specs=placed, out_specs=P("dop", "range"), check_vma=False
    )
```

```python
import functools
import jax
import jax.numpy as jnp
from jax import lax
from jax.experimental import pallas as pl
from jax.experimental.pallas import tpu as pltpu
from jax.sharding import PartitionSpec as P

CH = 16
SLOTS = 3
ST = 48
BINS = 128
BLOCK = 16
GATES = 128
TOTAL = 16384
EPS = 1e-6
HALF = 64
XN = 4
YN = 4
ZN = 4
WINDOW = 20
f32 = jnp.float32
bf16 = jnp.bfloat16
VMEM_LIMIT = 16 * 2**20

VM = pl.BlockSpec(memory_space=pltpu.VMEM)
SM = pl.BlockSpec(memory_space=pltpu.SMEM)


def core_and_dop():
    return lax.axis_index("range") % 2, lax.axis_index("dop")


def iota(shape, dim):
    return lax.broadcasted_iota(jnp.int32, shape, dim)


def split(x):
    hi = x.astype(bf16)
    return hi, (x - hi.astype(f32)).astype(bf16)


def lanes(*parts):
    return jnp.concatenate(parts, 1)


def rows(*parts):
    return jnp.concatenate(parts, 0)


def pack_kernel(echo, near, send, sems):
    core, _ = core_and_dop()
    copies = []
    for out, half in ((near, core), (send, 1 - core)):
        for z in range(ZN):
            first = z * 32 + half * 16
            for start, at, count in (
                (first, 2, 16),
                ((first + BINS - 2) % BINS, 0, 2),
                ((first + 16) % BINS, 18, 2),
            ):
                copies.append(
                    pltpu.make_async_copy(
                        echo.at[:, pl.ds(start, count)],
                        out.at[:, pl.ds(z * WINDOW + at, count)],
                        sems.at[len(copies)],
                    )
                )
    for c in copies:
        c.start()
    for c in copies:
        c.wait()


def pack(echo):
    return pl.pallas_call(
        pack_kernel,
        out_shape=[jax.ShapeDtypeStruct((2, ZN * WINDOW, CH, GATES), f32)] * 2,
        in_specs=[pl.BlockSpec(memory_space=pltpu.HBM)],
        out_specs=[VM] * 2,
        scratch_shapes=[pltpu.SemaphoreType.DMA((6 * ZN,))],
        name="pack",
        compiler_params=pltpu.CompilerParams(vmem_limit_bytes=VMEM_LIMIT),
    )(echo)


def place(trip, b, t, z, core):
    return z * WINDOW + ((trip[b, t] - (z * 32 + core * 16) + BINS + 2) & (BINS - 1))


def gram_kernel(second, trip, near, far, *refs):
    masks = refs[: 1 if second else 2]
    done, out, kept = (refs[1], refs[2], refs[3]) if second else (None, refs[2], refs[3])
    core, dop = core_and_dop()
    block = dop * (GATES // BLOCK) + (iota((64, 2 * GATES), 1) % GATES) // BLOCK
    block = block + 32 * (iota((64, 2 * GATES), 1) // GATES)
    pick = (iota((64, 2 * GATES), 0) == block).astype(f32)
    left = 1.0 - jnp.dot(rows(*[m[...] for m in masks]).astype(f32), pick, preferred_element_type=f32)
    for k in range(2):
        kept[k] = left[16 * k : 16 * k + 16]
    zero = jnp.zeros((16, 4 * GATES), bf16)
    base = 2 if second else 0

    def operands(k, i):
        z = dop ^ (base + k)
        b = z * 32 + core * 16 + i
        m = kept[k, pl.ds(i, 1), :]
        mn = jnp.broadcast_to(m[:, :GATES], (CH, GATES)).astype(bf16)
        mf = jnp.broadcast_to(m[:, GATES:], (CH, GATES)).astype(bf16)
        plain, left, right = [[], []], [[], []], [[], []]
        for t in range(SLOTS):
            s = place(trip, b, t, z, core)
            un, uf, vn, vf = split(near[0, s]), split(far[0, s]), split(near[1, s]), split(far[1, s])
            for h in range(2):
                plain[h].append(lanes(un[h], uf[h], vn[h], vf[h]))
                a, c, d, e = un[h] * mn, uf[h] * mf, vn[h] * mn, vf[h] * mf
                left[h].append(lanes(a, c, d, e))
                right[h].append(lanes(d, e, -a, -c))
        return plain[0], plain[1], rows(*left[0], *right[0], *left[1], *right[1])

    row = iota((ST, GATES), 0)
    lane = iota((ST, GATES), 1)
    low = row >= lane % HALF
    first = lane < HALF
    first24 = first[:24]

    def store(k, i, value):
        if second:
            out[i * ZN + (dop ^ (2 + k))] = value
        else:
            out[k * 16 + i] = value

    def pair(k, i):
        rha, rla, la = operands(k, i)
        rhb, rlb, lb = operands(k, i + 1)
        rhs = rows(*rha, zero, *rhb, zero, *rla, zero, *rlb, zero)
        dims = (((1,), (1,)), ((), ()))
        g = lax.dot_general(rows(la, lb), rhs, dims, preferred_element_type=f32)
        ga, gb = g[:192], g[192:]
        ga = ga[:96] + ga[96:]
        gb = gb[:96] + gb[96:]
        ga = ga[:, :GATES] + ga[:, GATES:]
        gb = gb[:, :GATES] + gb[:, GATES:]
        re = jnp.where(first, ga[:ST], gb[:ST])
        im = jnp.where(first, ga[ST:], gb[ST:])
        p = jnp.where(low, re, im)
        r = pltpu.roll(p, HALF, 1)
        store(k, i, jnp.where(first24, p[:24], r[24:]))
        store(k, i + 1, jnp.where(first24, r[:24], p[24:]))

    def step(k, c):
        for i in range(0, 16, 2):
            pair(k, i)
        return c

    lax.fori_loop(0, 2, step, 0)
    if second:
        for k in range(2):
            for i in range(16):
                out[i * ZN + (dop ^ k)] = done[k * 16 + i]


def gram(second, trip, near, far, extra):
    return pl.pallas_call(
        functools.partial(gram_kernel, second),
        out_shape=jax.ShapeDtypeStruct((64 if second else 32, 24, GATES), f32),
        in_specs=[SM] + [VM] * 4,
        out_specs=VM,
        scratch_shapes=[pltpu.VMEM((2, 16, 2 * GATES), f32)],
        name="gram_b" if second else "gram_a",
        compiler_params=pltpu.CompilerParams(vmem_limit_bytes=VMEM_LIMIT),
    )(trip, near, far, *extra)


def solve_kernel(parts, taper, trig, out):
    core, dop = core_and_dop()
    b = dop * 32 + core * 16 + lax.axis_index("range") // 2
    row = iota((ST, GATES), 0)
    lane = iota((ST, GATES), 1)
    total = parts[0]
    for j in range(1, 64):
        total = total + parts[j]
    total = total * (1.0 / TOTAL)
    p = rows(total, pltpu.roll(total, HALF, 1))
    full = rows(p, jnp.zeros((GATES - ST, GATES), f32)).T[:ST]
    re = jnp.where(row >= lane, p, full)
    im = jnp.where(row < lane, p, jnp.where(row == lane, 0.0, -full))
    chan = iota((CH, GATES), 0)
    cosine = jnp.zeros((CH, GATES), f32)
    sine = jnp.zeros((CH, GATES), f32)
    for j in range(CH):
        cosine = jnp.where(chan == j, trig[j], cosine)
        sine = jnp.where(chan == j, trig[CH + j], sine)
    sr = rows(*[taper[b, t] * cosine for t in range(SLOTS)])
    si = rows(*[taper[b, t] * sine for t in range(SLOTS)])
    are = jnp.where(lane < ST, re, sr)
    aim = jnp.where(lane < ST, im, si)
    for k in range(0, ST, 2):
        i0 = jnp.full((ST, GATES), k, jnp.int32)
        i1 = jnp.full((ST, GATES), k + 1, jnp.int32)
        c0r = jnp.take_along_axis(are, i0, 1)
        c0i = jnp.take_along_axis(aim, i0, 1)
        c1r = jnp.take_along_axis(are, i1, 1)
        c1i = jnp.take_along_axis(aim, i1, 1)
        r0, q0 = are[k : k + 1], aim[k : k + 1]
        r1, q1 = are[k + 1 : k + 2], aim[k + 1 : k + 2]
        a, d = c0r[k : k + 1], c1r[k + 1 : k + 2]
        br, bi = c1r[k : k + 1], c1i[k : k + 1]
        inv = 1.0 / (a * d - (br * br + bi * bi))
        a, d, br, bi = a * inv, d * inv, br * inv, bi * inv
        n0r = d * r0 - (br * r1 - bi * q1)
        n0i = d * q0 - (br * q1 + bi * r1)
        n1r = a * r1 - (br * r0 + bi * q0)
        n1i = a * q1 - (br * q0 - bi * r0)
        ur = (c0r * n0r - c0i * n0i) + (c1r * n1r - c1i * n1i)
        ui = (c0r * n0i + c0i * n0r) + (c1r * n1i + c1i * n1r)
        are = jnp.where(row == k, n0r, jnp.where(row == k + 1, n1r, are - ur))
        aim = jnp.where(row == k, n0i, jnp.where(row == k + 1, n1i, aim - ui))
    pad = jnp.zeros((GATES - ST, GATES), f32)
    wr = rows(are, pad).T[ST : ST + 1]
    wi = rows(aim, pad).T[ST : ST + 1]
    lane1 = iota((1, GATES), 1)
    w = jnp.where(lane1 < ST, wr, jnp.where(lane1 < 2 * ST, pltpu.roll(wi, ST, 1), 0.0))
    for j in range(64):
        out[j] = w


def solve(parts, taper, trig):
    return pl.pallas_call(
        solve_kernel,
        out_shape=jax.ShapeDtypeStruct((64, 1, GATES), f32),
        in_specs=[VM, SM, SM],
        out_specs=VM,
        name="solve",
        compiler_params=pltpu.CompilerParams(vmem_limit_bytes=VMEM_LIMIT),
    )(parts, taper, trig)


def power_kernel(trip, near, far, w, own, other):
    core, dop = core_and_dop()
    zero = jnp.zeros((32, 2 * GATES), bf16)
    row = iota((8, GATES), 0)
    lane = iota((8, GATES), 1)

    def one(k, i):
        z = dop ^ k
        b = z * 32 + core * 16 + i
        wt = jnp.broadcast_to(w[i * ZN + z], (8, GATES))
        turned = jnp.where(
            lane < ST,
            -pltpu.roll(wt, GATES - ST, 1),
            jnp.where(lane < 2 * ST, pltpu.roll(wt, ST, 1), 0.0),
        )
        wt = jnp.where(row % 2 == 0, wt, turned)
        hi = wt.astype(bf16).astype(f32)
        mid = (wt - hi).astype(bf16).astype(f32)
        lo = wt - hi - mid
        wt = jnp.where(row < 2, hi, jnp.where(row < 4, mid, jnp.where(row < 6, lo, 0.0)))
        lhs = rows(wt, jnp.zeros((8, GATES), f32)).astype(bf16)
        rhs = [[], [], []]
        for p in range(2):
            for t in range(SLOTS):
                s = place(trip, b, t, z, core)
                x = lanes(near[p, s], far[p, s])
                hi, rest = split(x)
                x = x - hi.astype(f32)
                rhs[0].append(hi)
                rhs[1].append(rest)
                rhs[2].append((x - rest.astype(f32)).astype(bf16))
        rhs = [*rhs[0], zero, *rhs[1], zero, *rhs[2], zero]
        y = jnp.dot(lanes(lhs, lhs, lhs), rows(*rhs), preferred_element_type=f32)
        re = y[0:1] + y[2:3] + y[4:5]
        im = y[1:2] + y[3:4] + y[5:6]
        return re * re + im * im

    def step(j, c):
        k = j // 2
        i = (j % 2) * 8
        y = rows(*[one(k, i + n) for n in range(8)])
        at = pl.ds(pl.multiple_of(i, 8), 8)
        own[k, at, :] = y[:, :GATES]
        other[k, at, :] = y[:, GATES:]
        return c

    lax.fori_loop(0, 8, step, 0)


def power(trip, near, far, w):
    return pl.pallas_call(
        power_kernel,
        out_shape=[jax.ShapeDtypeStruct((ZN, 16, GATES), f32)] * 2,
        in_specs=[SM] + [VM] * 3,
        out_specs=[VM] * 2,
        name="power",
        compiler_params=pltpu.CompilerParams(vmem_limit_bytes=VMEM_LIMIT),
    )(trip, near, far, w)


def cfar_kernel(p0, p1, p2, p3, inner, outer, guard, train, out, line):
    core, dop = core_and_dop()
    rank = lax.axis_index("range")
    width = 6 * GATES
    for k, ref in enumerate((p0, p1, p2, p3)):
        at = 1 + (dop ^ k)
        line[at, core] = ref[0]
        line[at, 1 - core] = ref[1]
    for at, ref in ((5 * (1 - core), inner), (5 * core, outer)):
        line[at, 1 - core] = ref[0]
        line[at, core] = ref[1]
    p = lanes(*[rows(line[j, 0], line[j, 1]) for j in range(6)])
    row = iota((32, 1), 0)
    g = jnp.zeros((32, 1), jnp.int32)
    t = jnp.zeros((32, 1), jnp.int32)
    for j in range(32):
        g = jnp.where(row == j, guard[j], g)
        t = jnp.where(row == j, train[j], t)
    total = p
    acc = jnp.where((t & 1) == 1, p, 0.0)
    for k in range(1, 7):
        total = total + pltpu.roll(total, width - (1 << (k - 1)), 1)
        acc = jnp.where((t >> k) & 1 == 1, total + pltpu.roll(acc, width - (1 << k), 1), acc)
    right = acc
    shift = g + 1
    for k in range(3):
        right = jnp.where((shift >> k) & 1 == 1, pltpu.roll(right, width - (1 << k), 1), right)
    left = acc
    shift = g + t
    for k in range(7):
        left = jnp.where((shift >> k) & 1 == 1, pltpu.roll(left, 1 << k, 1), left)
    lo, hi = GATES, GATES + 4 * GATES
    both = left[:, lo:hi] + right[:, lo:hi]
    pos = rank * (4 * GATES) + iota((32, 4 * GATES), 1)
    left_count = jnp.maximum(jnp.minimum(pos - g - 1, TOTAL - 1) - jnp.maximum(pos - g - t, 0) + 1, 0)
    right_count = jnp.maximum(jnp.minimum(pos + g + t, TOTAL - 1) - jnp.maximum(pos + g + 1, 0) + 1, 0)
    noise = both / (left_count + right_count).astype(f32)
    out[...] = p[:, lo:hi] / (noise + EPS)


def cfar(pieces, inner, outer, guard, train):
    return pl.pallas_call(
        cfar_kernel,
        out_shape=jax.ShapeDtypeStruct((32, 4 * GATES), f32),
        in_specs=[VM] * 6 + [SM] * 2,
        out_specs=VM,
        scratch_shapes=[pltpu.VMEM((6, 2, 16, GATES), f32)],
        name="cfar",
        compiler_params=pltpu.CompilerParams(vmem_limit_bytes=VMEM_LIMIT),
    )(*pieces, inner, outer, guard, train)


BOTH = ("range", "dop")
CORE_SWAP = [(i, i ^ 1) for i in range(32)]
SAME_CORE = [
    [((y * XN + x) * 2 + c) * ZN + z for y in range(YN) for x in range(XN) for z in range(ZN)]
    for c in range(2)
]


def flipped(bit):
    return [(i, i ^ bit) for i in range(ZN)]


def swap(value):
    return lax.ppermute(value, "range", CORE_SWAP)


def shards(echoes, triplet, bin_taper, phases, excluded, guard_len, train_len):
    core, dop = core_and_dop()
    other = swap(excluded)
    near, far = pack(echoes)
    far, other = lax.optimization_barrier((far, other))
    far = swap(far)
    mine = lax.dynamic_slice_in_dim(lanes(excluded, other), core * 16, 16, 0)
    m1 = lax.ppermute(mine, "dop", flipped(1))
    m2 = lax.ppermute(rows(mine, m1), "dop", flipped(2))
    part = gram(False, triplet, near, far, [mine, m1])
    part = gram(True, triplet, near, far, [m2, part])
    part = lax.all_to_all(part, BOTH, 0, 0, tiled=True, axis_index_groups=SAME_CORE)
    trig = jnp.concatenate([jnp.cos(phases), jnp.sin(phases)])
    w = solve(part, bin_taper, trig)
    w = lax.all_to_all(w, BOTH, 0, 0, tiled=True, axis_index_groups=SAME_CORE)
    own, away = power(triplet, near, far, w)
    came = swap(away)
    pieces = [jnp.stack([own[k], came[k]]) for k in range(ZN)]
    pieces = [pieces[0]] + [lax.ppermute(pieces[k], "dop", flipped(k)) for k in (1, 2, 3)]
    p0, p1, p2, p3 = pieces
    ranges = lax.axis_size("range")
    tail = jnp.where(dop == 0, p3, jnp.where(dop == 1, p2, jnp.where(dop == 2, p1, p0)))
    head = jnp.where(dop == 0, p0, jnp.where(dop == 1, p1, jnp.where(dop == 2, p2, p3)))
    inner = swap(jnp.where(core == 0, tail, head))
    pairs = [(i, i + 1 if i % 2 else i - 1) for i in range(1, ranges - 1)]
    outer = lax.ppermute(jnp.where(core == 0, head, tail), "range", pairs)
    return cfar(pieces, inner, outer, guard_len, train_len)


def solution(mesh):
    placed = (
        P(None, None, None, ("range", "dop")),
        P(),
        P(),
        P(),
        P("dop", "range"),
        P("dop"),
        P("dop"),
    )
    return jax.shard_map(
        shards, mesh=mesh, in_specs=placed, out_specs=P("dop", "range"), check_vma=False
    )
```

```python
import functools
import jax
import jax.numpy as jnp
from jax import lax
from jax.experimental import pallas as pl
from jax.experimental.pallas import tpu as pltpu
from jax.sharding import PartitionSpec as P

CH = 16
SLOTS = 3
ST = 48
BINS = 128
BLOCK = 16
GATES = 128
TOTAL = 16384
EPS = 1e-6
HALF = 64
XN = 4
YN = 4
ZN = 4
WINDOW = 20
PACKED = ST * ST
f32 = jnp.float32
bf16 = jnp.bfloat16
VMEM_LIMIT = 16 * 2**20

VM = pl.BlockSpec(memory_space=pltpu.VMEM)
SM = pl.BlockSpec(memory_space=pltpu.SMEM)


def core_and_dop():
    return lax.axis_index("range") % 2, lax.axis_index("dop")


def iota(shape, dim):
    return lax.broadcasted_iota(jnp.int32, shape, dim)


def split(x):
    hi = x.astype(bf16)
    return hi, (x - hi.astype(f32)).astype(bf16)


def lanes(*parts):
    return jnp.concatenate(parts, 1)


def rows(*parts):
    return jnp.concatenate(parts, 0)


def pack_kernel(echo, near, send, sems):
    core, _ = core_and_dop()
    copies = []
    for out, half in ((near, core), (send, 1 - core)):
        for z in range(ZN):
            first = z * 32 + half * 16
            for start, at, count in (
                (first, 2, 16),
                ((first + BINS - 2) % BINS, 0, 2),
                ((first + 16) % BINS, 18, 2),
            ):
                copies.append(
                    pltpu.make_async_copy(
                        echo.at[:, pl.ds(start, count)],
                        out.at[:, pl.ds(z * WINDOW + at, count)],
                        sems.at[len(copies)],
                    )
                )
    for c in copies:
        c.start()
    for c in copies:
        c.wait()


def pack(echo):
    return pl.pallas_call(
        pack_kernel,
        out_shape=[jax.ShapeDtypeStruct((2, ZN * WINDOW, CH, GATES), f32)] * 2,
        in_specs=[pl.BlockSpec(memory_space=pltpu.HBM)],
        out_specs=[VM] * 2,
        scratch_shapes=[pltpu.SemaphoreType.DMA((6 * ZN,))],
        name="pack",
        compiler_params=pltpu.CompilerParams(vmem_limit_bytes=VMEM_LIMIT),
    )(echo)


def place(trip, b, t, z, core):
    return z * WINDOW + ((trip[b, t] - (z * 32 + core * 16) + BINS + 2) & (BINS - 1))


def gram_kernel(second, trip, near, far, *refs):
    masks = refs[: 1 if second else 2]
    done, out, kept = (refs[1], refs[2], refs[3]) if second else (None, refs[2], refs[3])
    core, dop = core_and_dop()
    block = dop * (GATES // BLOCK) + (iota((64, 2 * GATES), 1) % GATES) // BLOCK
    block = block + 32 * (iota((64, 2 * GATES), 1) // GATES)
    pick = (iota((64, 2 * GATES), 0) == block).astype(f32)
    left = 1.0 - jnp.dot(rows(*[m[...] for m in masks]).astype(f32), pick, preferred_element_type=f32)
    for k in range(2):
        kept[k] = left[16 * k : 16 * k + 16]
    zero = jnp.zeros((16, 4 * GATES), bf16)
    base = 2 if second else 0

    def operands(k, i):
        z = dop ^ (base + k)
        b = z * 32 + core * 16 + i
        m = kept[k, pl.ds(i, 1), :]
        mn = jnp.broadcast_to(m[:, :GATES], (CH, GATES)).astype(bf16)
        mf = jnp.broadcast_to(m[:, GATES:], (CH, GATES)).astype(bf16)
        plain, left, right = [[], []], [[], []], [[], []]
        for t in range(SLOTS):
            s = place(trip, b, t, z, core)
            un, uf, vn, vf = split(near[0, s]), split(far[0, s]), split(near[1, s]), split(far[1, s])
            for h in range(2):
                plain[h].append(lanes(un[h], uf[h], vn[h], vf[h]))
                a, c, d, e = un[h] * mn, uf[h] * mf, vn[h] * mn, vf[h] * mf
                left[h].append(lanes(a, c, d, e))
                right[h].append(lanes(d, e, -a, -c))
        return plain[0], plain[1], rows(*left[0], *right[0], *left[1], *right[1])

    row = iota((ST, GATES), 0)
    lane = iota((ST, GATES), 1)
    low = row >= lane % HALF
    first = lane < HALF
    lane16 = iota((CH, GATES), 1)
    mine8 = iota((8, GATES), 1) // 16 == iota((8, GATES), 0)

    def store(k, i, p, at):
        q = i * ZN + (dop ^ (2 + k)) if second else k * 16 + i
        p0, p1, p2 = p[:16], p[16:32], p[32:]
        p0 = p0 if at == 0 else pltpu.roll(p0, GATES - at, 1)
        p1 = pltpu.roll(p1, (GATES + 48 - at) % GATES, 1)
        p2 = pltpu.roll(p2, (GATES + 96 - at) % GATES, 1)
        tail = [pltpu.roll(p2[h : h + 8], 0, 1, stride=16, stride_axis=0) for h in (0, 8)]
        main = jnp.where(lane16 < 48, p0, jnp.where(lane16 < 96, p1, p2))
        for j in range(16):
            out[q, :, j * GATES : (j + 1) * GATES] = main[j : j + 1]
        for j in range(2):
            extra = jnp.sum(jnp.where(mine8, tail[j], 0.0), 0, keepdims=True)
            out[q, :, (16 + j) * GATES : (17 + j) * GATES] = extra

    def pair(k, i):
        rha, rla, la = operands(k, i)
        rhb, rlb, lb = operands(k, i + 1)
        rhs = rows(*rha, zero, *rhb, zero, *rla, zero, *rlb, zero)
        dims = (((1,), (1,)), ((), ()))
        g = lax.dot_general(rows(la, lb), rhs, dims, preferred_element_type=f32)
        ga, gb = g[:192], g[192:]
        ga = ga[:96] + ga[96:]
        gb = gb[:96] + gb[96:]
        ga = ga[:, :GATES] + ga[:, GATES:]
        gb = gb[:, :GATES] + gb[:, GATES:]
        re = jnp.where(first, ga[:ST], gb[:ST])
        im = jnp.where(first, ga[ST:], gb[ST:])
        p = jnp.where(low, re, im)
        store(k, i, p, 0)
        store(k, i + 1, p, HALF)

    def step(k, c):
        for i in range(0, 16, 2):
            pair(k, i)
        return c

    lax.fori_loop(0, 2, step, 0)
    if second:
        for k in range(2):
            for i in range(16):
                out[i * ZN + (dop ^ k)] = done[k * 16 + i]


def gram(second, trip, near, far, extra):
    return pl.pallas_call(
        functools.partial(gram_kernel, second),
        out_shape=jax.ShapeDtypeStruct((64 if second else 32, 1, PACKED), f32),
        in_specs=[SM] + [VM] * 4,
        out_specs=VM,
        scratch_shapes=[pltpu.VMEM((2, 16, 2 * GATES), f32)],
        name="gram_b" if second else "gram_a",
        compiler_params=pltpu.CompilerParams(vmem_limit_bytes=VMEM_LIMIT),
    )(trip, near, far, *extra)


def solve_kernel(parts, taper, trig, out):
    core, dop = core_and_dop()
    b = dop * 32 + core * 16 + lax.axis_index("range") // 2
    row = iota((ST, GATES), 0)
    lane = iota((ST, GATES), 1)
    line = []
    for j in range(PACKED // GATES):
        line.append(jnp.sum(parts[:, 0, j * GATES : (j + 1) * GATES], 0, keepdims=True) * (1.0 / TOTAL))
    main = rows(*line[:16])
    corner = rows(*[pltpu.roll(line[16 + j // 8], (GATES + 32 - 16 * (j % 8)) % GATES, 1) for j in range(16)])
    p2 = jnp.where(lane[:16] < 32, pltpu.roll(main, 32, 1), corner)
    p = rows(main, pltpu.roll(main, GATES - 48, 1), p2)
    full = rows(p, jnp.zeros((GATES - ST, GATES), f32)).T[:ST]
    re = jnp.where(row >= lane, p, full)
    im = jnp.where(row < lane, p, jnp.where(row == lane, 0.0, -full))
    chan = iota((CH, GATES), 0)
    cosine = jnp.zeros((CH, GATES), f32)
    sine = jnp.zeros((CH, GATES), f32)
    for j in range(CH):
        cosine = jnp.where(chan == j, trig[j], cosine)
        sine = jnp.where(chan == j, trig[CH + j], sine)
    sr = rows(*[taper[b, t] * cosine for t in range(SLOTS)])
    si = rows(*[taper[b, t] * sine for t in range(SLOTS)])
    are = jnp.where(lane < ST, re, sr)
    aim = jnp.where(lane < ST, im, si)
    for k in range(0, ST, 2):
        i0 = jnp.full((ST, GATES), k, jnp.int32)
        i1 = jnp.full((ST, GATES), k + 1, jnp.int32)
        c0r = jnp.take_along_axis(are, i0, 1)
        c0i = jnp.take_along_axis(aim, i0, 1)
        c1r = jnp.take_along_axis(are, i1, 1)
        c1i = jnp.take_along_axis(aim, i1, 1)
        r0, q0 = are[k : k + 1], aim[k : k + 1]
        r1, q1 = are[k + 1 : k + 2], aim[k + 1 : k + 2]
        a, d = c0r[k : k + 1], c1r[k + 1 : k + 2]
        br, bi = c1r[k : k + 1], c1i[k : k + 1]
        inv = 1.0 / (a * d - (br * br + bi * bi))
        a, d, br, bi = a * inv, d * inv, br * inv, bi * inv
        n0r = d * r0 - (br * r1 - bi * q1)
        n0i = d * q0 - (br * q1 + bi * r1)
        n1r = a * r1 - (br * r0 + bi * q0)
        n1i = a * q1 - (br * q0 - bi * r0)
        ur = (c0r * n0r - c0i * n0i) + (c1r * n1r - c1i * n1i)
        ui = (c0r * n0i + c0i * n0r) + (c1r * n1i + c1i * n1r)
        are = jnp.where(row == k, n0r, jnp.where(row == k + 1, n1r, are - ur))
        aim = jnp.where(row == k, n0i, jnp.where(row == k + 1, n1i, aim - ui))
    pad = jnp.zeros((GATES - ST, GATES), f32)
    wr = rows(are, pad).T[ST : ST + 1]
    wi = rows(aim, pad).T[ST : ST + 1]
    lane1 = iota((1, GATES), 1)
    w = jnp.where(lane1 < ST, wr, jnp.where(lane1 < 2 * ST, pltpu.roll(wi, ST, 1), 0.0))
    for j in range(64):
        out[j] = w


def solve(parts, taper, trig):
    return pl.pallas_call(
        solve_kernel,
        out_shape=jax.ShapeDtypeStruct((64, 1, GATES), f32),
        in_specs=[VM, SM, SM],
        out_specs=VM,
        name="solve",
        compiler_params=pltpu.CompilerParams(vmem_limit_bytes=VMEM_LIMIT),
    )(parts, taper, trig)


def power_kernel(trip, near, far, w, own, other):
    core, dop = core_and_dop()
    zero = jnp.zeros((32, 2 * GATES), bf16)
    row = iota((8, GATES), 0)
    lane = iota((8, GATES), 1)

    def one(k, i):
        z = dop ^ k
        b = z * 32 + core * 16 + i
        wt = jnp.broadcast_to(w[i * ZN + z], (8, GATES))
        turned = jnp.where(
            lane < ST,
            -pltpu.roll(wt, GATES - ST, 1),
            jnp.where(lane < 2 * ST, pltpu.roll(wt, ST, 1), 0.0),
        )
        wt = jnp.where(row % 2 == 0, wt, turned)
        hi = wt.astype(bf16).astype(f32)
        mid = (wt - hi).astype(bf16).astype(f32)
        lo = wt - hi - mid
        wt = jnp.where(row < 2, hi, jnp.where(row < 4, mid, jnp.where(row < 6, lo, 0.0)))
        lhs = rows(wt, jnp.zeros((8, GATES), f32)).astype(bf16)
        rhs = [[], [], []]
        for p in range(2):
            for t in range(SLOTS):
                s = place(trip, b, t, z, core)
                x = lanes(near[p, s], far[p, s])
                hi, rest = split(x)
                x = x - hi.astype(f32)
                rhs[0].append(hi)
                rhs[1].append(rest)
                rhs[2].append((x - rest.astype(f32)).astype(bf16))
        rhs = [*rhs[0], zero, *rhs[1], zero, *rhs[2], zero]
        y = jnp.dot(lanes(lhs, lhs, lhs), rows(*rhs), preferred_element_type=f32)
        re = y[0:1] + y[2:3] + y[4:5]
        im = y[1:2] + y[3:4] + y[5:6]
        return re * re + im * im

    def step(j, c):
        k = j // 2
        i = (j % 2) * 8
        y = rows(*[one(k, i + n) for n in range(8)])
        at = pl.ds(pl.multiple_of(i, 8), 8)
        own[k, at, :] = y[:, :GATES]
        other[k, at, :] = y[:, GATES:]
        return c

    lax.fori_loop(0, 8, step, 0)


def power(trip, near, far, w):
    return pl.pallas_call(
        power_kernel,
        out_shape=[jax.ShapeDtypeStruct((ZN, 16, GATES), f32)] * 2,
        in_specs=[SM] + [VM] * 3,
        out_specs=[VM] * 2,
        name="power",
        compiler_params=pltpu.CompilerParams(vmem_limit_bytes=VMEM_LIMIT),
    )(trip, near, far, w)


def cfar_kernel(p0, p1, p2, p3, inner, outer, guard, train, out, line):
    core, dop = core_and_dop()
    rank = lax.axis_index("range")
    width = 6 * GATES
    for k, ref in enumerate((p0, p1, p2, p3)):
        at = 1 + (dop ^ k)
        line[at, core] = ref[0]
        line[at, 1 - core] = ref[1]
    for at, ref in ((5 * (1 - core), inner), (5 * core, outer)):
        line[at, 1 - core] = ref[0]
        line[at, core] = ref[1]
    p = lanes(*[rows(line[j, 0], line[j, 1]) for j in range(6)])
    row = iota((32, 1), 0)
    g = jnp.zeros((32, 1), jnp.int32)
    t = jnp.zeros((32, 1), jnp.int32)
    for j in range(32):
        g = jnp.where(row == j, guard[j], g)
        t = jnp.where(row == j, train[j], t)
    total = p
    acc = jnp.where((t & 1) == 1, p, 0.0)
    for k in range(1, 7):
        total = total + pltpu.roll(total, width - (1 << (k - 1)), 1)
        acc = jnp.where((t >> k) & 1 == 1, total + pltpu.roll(acc, width - (1 << k), 1), acc)
    right = acc
    shift = g + 1
    for k in range(3):
        right = jnp.where((shift >> k) & 1 == 1, pltpu.roll(right, width - (1 << k), 1), right)
    left = acc
    shift = g + t
    for k in range(7):
        left = jnp.where((shift >> k) & 1 == 1, pltpu.roll(left, 1 << k, 1), left)
    lo, hi = GATES, GATES + 4 * GATES
    both = left[:, lo:hi] + right[:, lo:hi]
    pos = rank * (4 * GATES) + iota((32, 4 * GATES), 1)
    left_count = jnp.maximum(jnp.minimum(pos - g - 1, TOTAL - 1) - jnp.maximum(pos - g - t, 0) + 1, 0)
    right_count = jnp.maximum(jnp.minimum(pos + g + t, TOTAL - 1) - jnp.maximum(pos + g + 1, 0) + 1, 0)
    noise = both / (left_count + right_count).astype(f32)
    out[...] = p[:, lo:hi] / (noise + EPS)


def cfar(pieces, inner, outer, guard, train):
    return pl.pallas_call(
        cfar_kernel,
        out_shape=jax.ShapeDtypeStruct((32, 4 * GATES), f32),
        in_specs=[VM] * 6 + [SM] * 2,
        out_specs=VM,
        scratch_shapes=[pltpu.VMEM((6, 2, 16, GATES), f32)],
        name="cfar",
        compiler_params=pltpu.CompilerParams(vmem_limit_bytes=VMEM_LIMIT),
    )(*pieces, inner, outer, guard, train)


BOTH = ("range", "dop")
CORE_SWAP = [(i, i ^ 1) for i in range(32)]
SAME_CORE = [
    [((y * XN + x) * 2 + c) * ZN + z for y in range(YN) for x in range(XN) for z in range(ZN)]
    for c in range(2)
]


def flipped(bit):
    return [(i, i ^ bit) for i in range(ZN)]


def swap(value):
    return lax.ppermute(value, "range", CORE_SWAP)


def shards(echoes, triplet, bin_taper, phases, excluded, guard_len, train_len):
    core, dop = core_and_dop()
    other = swap(excluded)
    near, far = pack(echoes)
    far, other = lax.optimization_barrier((far, other))
    far = swap(far)
    mine = lax.dynamic_slice_in_dim(lanes(excluded, other), core * 16, 16, 0)
    m1 = lax.ppermute(mine, "dop", flipped(1))
    m2 = lax.ppermute(rows(mine, m1), "dop", flipped(2))
    part = gram(False, triplet, near, far, [mine, m1])
    part = gram(True, triplet, near, far, [m2, part])
    part = lax.all_to_all(part, BOTH, 0, 0, tiled=True, axis_index_groups=SAME_CORE)
    trig = jnp.concatenate([jnp.cos(phases), jnp.sin(phases)])
    w = solve(part, bin_taper, trig)
    w = lax.all_to_all(w, BOTH, 0, 0, tiled=True, axis_index_groups=SAME_CORE)
    own, away = power(triplet, near, far, w)
    came = swap(away)
    pieces = [jnp.stack([own[k], came[k]]) for k in range(ZN)]
    pieces = [pieces[0]] + [lax.ppermute(pieces[k], "dop", flipped(k)) for k in (1, 2, 3)]
    p0, p1, p2, p3 = pieces
    ranges = lax.axis_size("range")
    tail = jnp.where(dop == 0, p3, jnp.where(dop == 1, p2, jnp.where(dop == 2, p1, p0)))
    head = jnp.where(dop == 0, p0, jnp.where(dop == 1, p1, jnp.where(dop == 2, p2, p3)))
    inner = swap(jnp.where(core == 0, tail, head))
    pairs = [(i, i + 1 if i % 2 else i - 1) for i in range(1, ranges - 1)]
    outer = lax.ppermute(jnp.where(core == 0, head, tail), "range", pairs)
    return cfar(pieces, inner, outer, guard_len, train_len)


def solution(mesh):
    placed = (
        P(None, None, None, ("range", "dop")),
        P(),
        P(),
        P(),
        P("dop", "range"),
        P("dop"),
        P("dop"),
    )
    return jax.shard_map(
        shards, mesh=mesh, in_specs=placed, out_specs=P("dop", "range"), check_vma=False
    )
```

```python
import functools
import jax
import jax.numpy as jnp
from jax import lax
from jax.experimental import pallas as pl
from jax.experimental.pallas import tpu as pltpu
from jax.sharding import PartitionSpec as P

CH = 16
SLOTS = 3
ST = 48
BINS = 128
BLOCK = 16
GATES = 128
TOTAL = 16384
EPS = 1e-6
HALF = 64
XN = 4
YN = 4
ZN = 4
WINDOW = 20
PACKED = ST * ST
f32 = jnp.float32
bf16 = jnp.bfloat16
VMEM_LIMIT = 16 * 2**20

VM = pl.BlockSpec(memory_space=pltpu.VMEM)
SM = pl.BlockSpec(memory_space=pltpu.SMEM)


def core_and_dop():
    return lax.axis_index("range") % 2, lax.axis_index("dop")


def iota(shape, dim):
    return lax.broadcasted_iota(jnp.int32, shape, dim)


def split(x):
    hi = x.astype(bf16)
    return hi, (x - hi.astype(f32)).astype(bf16)


def lanes(*parts):
    return jnp.concatenate(parts, 1)


def rows(*parts):
    return jnp.concatenate(parts, 0)


def pack_kernel(echo, near, send, sems):
    core, _ = core_and_dop()
    copies = []
    for out, half in ((near, core), (send, 1 - core)):
        for z in range(ZN):
            first = z * 32 + half * 16
            for start, at, count in (
                (first, 2, 16),
                ((first + BINS - 2) % BINS, 0, 2),
                ((first + 16) % BINS, 18, 2),
            ):
                copies.append(
                    pltpu.make_async_copy(
                        echo.at[:, pl.ds(start, count)],
                        out.at[:, pl.ds(z * WINDOW + at, count)],
                        sems.at[len(copies)],
                    )
                )
    for c in copies:
        c.start()
    for c in copies:
        c.wait()


def pack(echo):
    return pl.pallas_call(
        pack_kernel,
        out_shape=[jax.ShapeDtypeStruct((2, ZN * WINDOW, CH, GATES), f32)] * 2,
        in_specs=[pl.BlockSpec(memory_space=pltpu.HBM)],
        out_specs=[VM] * 2,
        scratch_shapes=[pltpu.SemaphoreType.DMA((6 * ZN,))],
        name="pack",
        compiler_params=pltpu.CompilerParams(vmem_limit_bytes=52 * 2**20),
    )(echo)


def places(triplet):
    core, _ = core_and_dop()
    mine = lax.dynamic_index_in_dim(triplet.reshape(ZN, 2, 16, SLOTS), core, 1, keepdims=False)
    group = iota((ZN, 16, SLOTS), 0)
    where = group * WINDOW + ((mine - (group * 32 + core * 16) + BINS + 2) & (BINS - 1))
    return where.reshape(ZN * 16 * SLOTS)


def gram_kernel(second, place, near, far, *refs):
    masks = refs[: 1 if second else 2]
    done, out, kept = (refs[1], refs[2], refs[3]) if second else (None, refs[2], refs[3])
    core, dop = core_and_dop()
    block = dop * (GATES // BLOCK) + (iota((64, 2 * GATES), 1) % GATES) // BLOCK
    block = block + 32 * (iota((64, 2 * GATES), 1) // GATES)
    pick = (iota((64, 2 * GATES), 0) == block).astype(f32)
    left = 1.0 - jnp.dot(rows(*[m[...] for m in masks]).astype(f32), pick, preferred_element_type=f32)
    for k in range(2):
        kept[k] = left[16 * k : 16 * k + 16]
    zero = jnp.zeros((16, 4 * GATES), bf16)
    base = 2 if second else 0

    def operands(k, i):
        z = dop ^ (base + k)
        m = kept[k, pl.ds(i, 1), :]
        mn = jnp.broadcast_to(m[:, :GATES], (CH, GATES)).astype(bf16)
        mf = jnp.broadcast_to(m[:, GATES:], (CH, GATES)).astype(bf16)
        hi, lo, left, right, rest, last = [], [], [], [], [], []
        for t in range(SLOTS):
            s = place[(z * 16 + i) * SLOTS + t]
            un, uf, vn, vf = split(near[0, s]), split(far[0, s]), split(near[1, s]), split(far[1, s])
            hi.append(lanes(un[0], uf[0], vn[0], vf[0]))
            lo.append(lanes(un[1], uf[1], vn[1], vf[1]))
            a, c, d, e = un[0] * mn, uf[0] * mf, vn[0] * mn, vf[0] * mf
            left.append(lanes(a, c, d, e))
            right.append(lanes(d, e, -a, -c))
            a, c, d, e = un[1] * mn, uf[1] * mf, vn[1] * mn, vf[1] * mf
            rest.append(lanes(a, c, d, e))
            last.append(lanes(d, e, -a, -c))
        return hi, lo, rows(*left, *right, *rest, *last)

    row = iota((ST, GATES), 0)
    lane = iota((ST, GATES), 1)
    low = row >= lane % HALF
    high = row <= lane % HALF
    first = lane < HALF
    lane16 = iota((CH, GATES), 1)
    mine8 = iota((8, GATES), 1) // 16 == iota((8, GATES), 0)

    def store(k, i, p):
        q = i * ZN + (dop ^ (2 + k)) if second else k * 16 + i
        p0, p1 = p[:16], pltpu.roll(p[16:32], 48, 1)
        p2 = pltpu.roll(p[32:], 96, 1)
        tail = [pltpu.roll(p2[h : h + 8], 0, 1, stride=16, stride_axis=0) for h in (0, 8)]
        main = jnp.where(lane16 < 48, p0, jnp.where(lane16 < 96, p1, p2))
        for j in range(16):
            out[q, :, j * GATES : (j + 1) * GATES] = main[j : j + 1]
        for j in range(2):
            extra = jnp.sum(jnp.where(mine8, tail[j], 0.0), 0, keepdims=True)
            out[q, :, (16 + j) * GATES : (17 + j) * GATES] = extra

    def pair(k, i):
        ha, wa, la = operands(k, i)
        hb, wb, lb = operands(k, i + 1)
        rhs = rows(*ha, zero, *hb, zero, *wa, zero, *wb, zero)
        dims = (((1,), (1,)), ((), ()))
        g = lax.dot_general(rows(la, lb), rhs, dims, preferred_element_type=f32)
        ga, gb = g[:192], g[192:]
        ga = ga[:96] + ga[96:]
        gb = gb[:96] + gb[96:]
        ga = ga[:, :GATES] + ga[:, GATES:]
        gb = gb[:, :GATES] + gb[:, GATES:]
        re = jnp.where(first, ga[:ST], gb[:ST])
        im = jnp.where(first, ga[ST:], gb[ST:])
        p = jnp.where(low, re, im)
        store(k, i, p)
        store(k, i + 1, pltpu.roll(p, HALF, 1))

    def step(k, c):
        for i in range(0, 16, 2):
            pair(k, i)
        return c

    lax.fori_loop(0, 2, step, 0)
    if second:
        for k in range(2):
            for i in range(16):
                out[i * ZN + (dop ^ k)] = done[k * 16 + i]


def gram(second, place, near, far, extra):
    return pl.pallas_call(
        functools.partial(gram_kernel, second),
        out_shape=jax.ShapeDtypeStruct((64 if second else 32, 1, PACKED), f32),
        in_specs=[SM] + [VM] * 4,
        out_specs=VM,
        scratch_shapes=[pltpu.VMEM((2, 16, 2 * GATES), f32)],
        name="gram_b" if second else "gram_a",
        compiler_params=pltpu.CompilerParams(vmem_limit_bytes=VMEM_LIMIT),
    )(place, near, far, *extra)


def solve_kernel(parts, sr, si, out):
    row = iota((ST, GATES), 0)
    lane = iota((ST, GATES), 1)
    line = []
    for j in range(PACKED // GATES):
        line.append(jnp.sum(parts[:, 0, j * GATES : (j + 1) * GATES], 0, keepdims=True) * (1.0 / TOTAL))
    main = rows(*line[:16])
    corner = rows(*[pltpu.roll(line[16 + j // 8], (GATES + 32 - 16 * (j % 8)) % GATES, 1) for j in range(16)])
    p2 = jnp.where(lane[:16] < 32, pltpu.roll(main, 32, 1), corner)
    p = rows(main, pltpu.roll(main, GATES - 48, 1), p2)
    full = rows(p, jnp.zeros((GATES - ST, GATES), f32)).T[:ST]
    re = jnp.where(row >= lane, p, full)
    im = jnp.where(row < lane, p, jnp.where(row == lane, 0.0, -full))
    are = jnp.where(lane < ST, re, sr[...])
    aim = jnp.where(lane < ST, im, si[...])
    for k in range(0, ST, 2):
        i0 = jnp.full((ST, GATES), k, jnp.int32)
        i1 = jnp.full((ST, GATES), k + 1, jnp.int32)
        c0r = jnp.take_along_axis(are, i0, 1)
        c0i = jnp.take_along_axis(aim, i0, 1)
        c1r = jnp.take_along_axis(are, i1, 1)
        c1i = jnp.take_along_axis(aim, i1, 1)
        r0, q0 = are[k : k + 1], aim[k : k + 1]
        r1, q1 = are[k + 1 : k + 2], aim[k + 1 : k + 2]
        a, d = c0r[k : k + 1], c1r[k + 1 : k + 2]
        br, bi = c1r[k : k + 1], c1i[k : k + 1]
        inv = 1.0 / (a * d - (br * br + bi * bi))
        a, d, br, bi = a * inv, d * inv, br * inv, bi * inv
        n0r = d * r0 - (br * r1 - bi * q1)
        n0i = d * q0 - (br * q1 + bi * r1)
        n1r = a * r1 - (br * r0 + bi * q0)
        n1i = a * q1 - (br * q0 - bi * r0)
        ur = (c0r * n0r - c0i * n0i) + (c1r * n1r - c1i * n1i)
        ui = (c0r * n0i + c0i * n0r) + (c1r * n1i + c1i * n1r)
        are = jnp.where(row == k, n0r, jnp.where(row == k + 1, n1r, are - ur))
        aim = jnp.where(row == k, n0i, jnp.where(row == k + 1, n1i, aim - ui))
    pad = jnp.zeros((GATES - ST, GATES), f32)
    wr = rows(are, pad).T[ST : ST + 1]
    wi = rows(aim, pad).T[ST : ST + 1]
    lane1 = iota((1, GATES), 1)
    w = jnp.where(lane1 < ST, wr, jnp.where(lane1 < 2 * ST, pltpu.roll(wi, ST, 1), 0.0))
    for j in range(64):
        out[j] = w


def solve(parts, sr, si):
    return pl.pallas_call(
        solve_kernel,
        out_shape=jax.ShapeDtypeStruct((64, 1, GATES), f32),
        in_specs=[VM] * 3,
        out_specs=VM,
        name="solve",
        compiler_params=pltpu.CompilerParams(vmem_limit_bytes=VMEM_LIMIT),
    )(parts, sr, si)


def power_kernel(place, near, far, w, out, edge):
    core, dop = core_and_dop()
    zero = jnp.zeros((32, 2 * GATES), bf16)
    row = iota((8, GATES), 0)
    lane = iota((8, GATES), 1)

    def one(k, i):
        z = dop ^ k
        wt = jnp.broadcast_to(w[i * ZN + z], (8, GATES))
        turned = jnp.where(
            lane < ST,
            -pltpu.roll(wt, GATES - ST, 1),
            jnp.where(lane < 2 * ST, pltpu.roll(wt, ST, 1), 0.0),
        )
        wt = jnp.where(row % 2 == 0, wt, turned)
        hi = wt.astype(bf16).astype(f32)
        mid = (wt - hi).astype(bf16).astype(f32)
        lo = wt - hi - mid
        wt = jnp.where(row < 2, hi, jnp.where(row < 4, mid, jnp.where(row < 6, lo, 0.0)))
        lhs = rows(wt, jnp.zeros((8, GATES), f32)).astype(bf16)
        rhs = [[], [], []]
        for p in range(2):
            for t in range(SLOTS):
                s = place[(z * 16 + i) * SLOTS + t]
                x = lanes(near[p, s], far[p, s])
                hi, rest = split(x)
                x = x - hi.astype(f32)
                rhs[0].append(hi)
                rhs[1].append(rest)
                rhs[2].append((x - rest.astype(f32)).astype(bf16))
        rhs = [*rhs[0], zero, *rhs[1], zero, *rhs[2], zero]
        y = jnp.dot(lanes(lhs, lhs, lhs), rows(*rhs), preferred_element_type=f32)
        re = y[0:1] + y[2:3] + y[4:5]
        im = y[1:2] + y[3:4] + y[5:6]
        return re * re + im * im

    def step(j, c):
        k = j // 2
        i = (j % 2) * 8
        y = rows(*[one(k, i + n) for n in range(8)])
        at = pl.ds(pl.multiple_of(i, 8), 8)
        mine, away = y[:, :GATES], y[:, GATES:]
        out[k, 0, at, :] = mine
        out[k, 1, at, :] = away
        edge[k ^ 3, at, :] = jnp.where((dop == 3) == (core == 1), mine, away)
        return c

    lax.fori_loop(0, 8, step, 0)


def power(place, near, far, w):
    return pl.pallas_call(
        power_kernel,
        out_shape=[
            jax.ShapeDtypeStruct((ZN, 2, 16, GATES), f32),
            jax.ShapeDtypeStruct((ZN, 16, GATES), f32),
        ],
        in_specs=[SM] + [VM] * 3,
        out_specs=[VM] * 2,
        name="power",
        compiler_params=pltpu.CompilerParams(vmem_limit_bytes=VMEM_LIMIT),
    )(place, near, far, w)


def chosen(refs, slot, index):
    value = refs[0][slot]
    for k in range(1, ZN):
        value = jnp.where(index == k, refs[k][slot], value)
    return value


def leave_kernel(r0, r1, r2, r3, out):
    core, dop = core_and_dop()
    refs = (r0, r1, r2, r3)
    for k in range(ZN):
        out[k] = refs[k][1]
    index = dop ^ (3 * (1 - core))
    out[4] = chosen(refs, 0, index)
    out[5] = chosen(refs, 2, index)


def leave(pieces):
    return pl.pallas_call(
        leave_kernel,
        out_shape=jax.ShapeDtypeStruct((6, 16, GATES), f32),
        in_specs=[VM] * 4,
        out_specs=VM,
        name="leave",
        compiler_params=pltpu.CompilerParams(vmem_limit_bytes=VMEM_LIMIT),
    )(*pieces)


def cfar_kernel(r0, r1, r2, r3, came, guard, train, out, line):
    core, dop = core_and_dop()
    rank = lax.axis_index("range")
    width = 6 * GATES
    refs = (r0, r1, r2, r3)
    for k in range(ZN):
        at = 1 + (dop ^ k)
        line[at, core] = refs[k][0]
        line[at, 1 - core] = came[k]
    index = dop ^ (3 * core)
    inner, outer = 5 * (1 - core), 5 * core
    line[inner, core] = chosen(refs, 1, index)
    line[inner, 1 - core] = came[4]
    line[outer, core] = chosen(refs, 2, index)
    line[outer, 1 - core] = came[5]
    p = lanes(*[rows(line[j, 0], line[j, 1]) for j in range(6)])
    g = guard[:, :1]
    t = train[:, :1]
    total = p
    acc = jnp.where((t & 1) == 1, p, 0.0)
    for k in range(1, 7):
        total = total + pltpu.roll(total, width - (1 << (k - 1)), 1)
        acc = jnp.where((t >> k) & 1 == 1, total + pltpu.roll(acc, width - (1 << k), 1), acc)
    right = acc
    shift = g + 1
    for k in range(3):
        right = jnp.where((shift >> k) & 1 == 1, pltpu.roll(right, width - (1 << k), 1), right)
    left = acc
    shift = g + t
    for k in range(7):
        left = jnp.where((shift >> k) & 1 == 1, pltpu.roll(left, 1 << k, 1), left)
    lo, hi = GATES, GATES + 4 * GATES
    both = left[:, lo:hi] + right[:, lo:hi]
    pos = rank * (4 * GATES) + iota((32, 4 * GATES), 1)
    left_count = jnp.maximum(jnp.minimum(pos - g - 1, TOTAL - 1) - jnp.maximum(pos - g - t, 0) + 1, 0)
    right_count = jnp.maximum(jnp.minimum(pos + g + t, TOTAL - 1) - jnp.maximum(pos + g + 1, 0) + 1, 0)
    noise = both / (left_count + right_count).astype(f32)
    out[...] = p[:, lo:hi] / (noise + EPS)


def cfar(pieces, came, guard, train):
    return pl.pallas_call(
        cfar_kernel,
        out_shape=jax.ShapeDtypeStruct((32, 4 * GATES), f32),
        in_specs=[VM] * 7,
        out_specs=VM,
        scratch_shapes=[pltpu.VMEM((6, 2, 16, GATES), f32)],
        name="cfar",
        compiler_params=pltpu.CompilerParams(vmem_limit_bytes=VMEM_LIMIT),
    )(*pieces, came, guard, train)


BOTH = ("range", "dop")
CORE_SWAP = [(i, i ^ 1) for i in range(32)]
SAME_CORE = [
    [((y * XN + x) * 2 + c) * ZN + z for y in range(YN) for x in range(XN) for z in range(ZN)]
    for c in range(2)
]


def flipped(bit):
    return [(i, i ^ bit) for i in range(ZN)]


def swap(value):
    return lax.ppermute(value, "range", CORE_SWAP)


def steering(bin_taper, phases):
    core, dop = core_and_dop()
    b = dop * 32 + core * 16 + lax.axis_index("range") // 2
    taper = lax.dynamic_index_in_dim(bin_taper, b, 0, keepdims=False)

    def lay(values):
        return jnp.broadcast_to((taper[:, None] * values[None, :]).reshape(ST, 1), (ST, GATES))

    return lay(jnp.cos(phases)), lay(jnp.sin(phases))


def shards(echoes, triplet, bin_taper, phases, excluded, guard_len, train_len):
    core, dop = core_and_dop()
    place = places(triplet)
    other = swap(excluded)
    near, far = pack(echoes)
    far, other = lax.optimization_barrier((far, other))
    far = swap(far)
    mine = lax.dynamic_slice_in_dim(lanes(excluded, other), core * 16, 16, 0)
    m1 = lax.ppermute(mine, "dop", flipped(1))
    m2 = lax.ppermute(rows(mine, m1), "dop", flipped(2))
    part = gram(False, place, near, far, [mine, m1])
    part = gram(True, place, near, far, [m2, part])
    part = lax.all_to_all(part, BOTH, 0, 0, tiled=True, axis_index_groups=SAME_CORE)
    sr, si = steering(bin_taper, phases)
    guard = jnp.broadcast_to(guard_len[:, None], (32, GATES))
    train = jnp.broadcast_to(train_len[:, None], (32, GATES))
    sr, si, guard, train = lax.optimization_barrier((sr, si, guard, train))
    w = solve(part, sr, si)
    w = lax.all_to_all(w, BOTH, 0, 0, tiled=True, axis_index_groups=SAME_CORE)
    pw, edge = power(place, near, far, w)
    chips = lax.axis_size("range") // 2
    pairs = []
    for chip in range(chips):
        for c in range(2):
            here = (chip * 2 + c) * ZN
            if chip + 1 < chips:
                pairs.append((here + ZN - 1, here + 2 * ZN))
            if chip > 0:
                pairs.append((here, here - ZN - 1))
    edge = lax.ppermute(edge, BOTH, pairs)
    pieces = [jnp.concatenate([pw[k], edge[k : k + 1]]) for k in range(ZN)]
    pieces = [pieces[0]] + [lax.ppermute(pieces[k], "dop", flipped(k)) for k in (1, 2, 3)]
    came = swap(leave(pieces))
    return cfar(pieces, came, guard, train)


def solution(mesh):
    placed = (
        P(None, None, None, ("range", "dop")),
        P(),
        P(),
        P(),
        P("dop", "range"),
        P("dop"),
        P("dop"),
    )
    return jax.shard_map(
        shards, mesh=mesh, in_specs=placed, out_specs=P("dop", "range"), check_vma=False
    )
```

```python
import functools
import jax
import jax.numpy as jnp
from jax import lax
from jax.experimental import pallas as pl
from jax.experimental.pallas import tpu as pltpu
from jax.sharding import PartitionSpec as P

CH = 16
SLOTS = 3
ST = 48
BINS = 128
BLOCK = 16
GATES = 128
TOTAL = 16384
EPS = 1e-6
HALF = 64
XN = 4
YN = 4
ZN = 4
WINDOW = 68
PACKED = ST * ST
f32 = jnp.float32
bf16 = jnp.bfloat16
VMEM_LIMIT = 16 * 2**20

VM = pl.BlockSpec(memory_space=pltpu.VMEM)
SM = pl.BlockSpec(memory_space=pltpu.SMEM)


def core_and_dop():
    return lax.axis_index("range") % 2, lax.axis_index("dop")


def iota(shape, dim):
    return lax.broadcasted_iota(jnp.int32, shape, dim)


def split(x):
    hi = x.astype(bf16)
    return hi, (x - hi.astype(f32)).astype(bf16)


def lanes(*parts):
    return jnp.concatenate(parts, 1)


def rows(*parts):
    return jnp.concatenate(parts, 0)


def pack_kernel(echo, near, send, sems):
    core, _ = core_and_dop()
    copies = []
    for out, half in ((near, core), (send, 1 - core)):
        first = half * 64
        for start, at, count in (
            (first, 2, 64),
            ((first + BINS - 2) % BINS, 0, 2),
            ((first + 64) % BINS, 66, 2),
        ):
            copies.append(
                pltpu.make_async_copy(
                    echo.at[:, pl.ds(start, count)],
                    out.at[:, pl.ds(at, count)],
                    sems.at[len(copies)],
                )
            )
    for c in copies:
        c.start()
    for c in copies:
        c.wait()


def pack(echo):
    return pl.pallas_call(
        pack_kernel,
        out_shape=[jax.ShapeDtypeStruct((2, WINDOW, CH, GATES), f32)] * 2,
        in_specs=[pl.BlockSpec(memory_space=pltpu.HBM)],
        out_specs=[VM] * 2,
        scratch_shapes=[pltpu.SemaphoreType.DMA((6,))],
        name="pack",
        compiler_params=pltpu.CompilerParams(vmem_limit_bytes=52 * 2**20),
    )(echo)


def places(triplet):
    core, _ = core_and_dop()
    mine = lax.dynamic_slice_in_dim(triplet, core * 64, 64, 0)
    return ((mine - core * 64 + BINS + 2) & (BINS - 1)).reshape(64 * SLOTS)


def gram_kernel(place, near, far, m0, m1, m2, m3, out, kept):
    core, dop = core_and_dop()
    block = dop * (GATES // BLOCK) + iota((32, GATES), 1) // BLOCK
    pick = (iota((32, GATES), 0) == block).astype(f32)
    for k, ref in enumerate((m0, m1, m2, m3)):
        m = dop ^ k
        left = 1.0 - jnp.dot(ref[...].astype(f32), pick, preferred_element_type=f32)
        kept[(m // 2) ^ core, pl.ds(pl.multiple_of((m % 2) * 32, 32), 32), :] = left
    zero = jnp.zeros((16, 4 * GATES), bf16)

    def operands(i):
        mn = jnp.broadcast_to(kept[0, pl.ds(i, 1), :], (CH, GATES)).astype(bf16)
        mf = jnp.broadcast_to(kept[1, pl.ds(i, 1), :], (CH, GATES)).astype(bf16)
        hi, lo, left, right, rest, last = [], [], [], [], [], []
        for t in range(SLOTS):
            s = place[i * SLOTS + t]
            un, uf, vn, vf = split(near[0, s]), split(far[0, s]), split(near[1, s]), split(far[1, s])
            hi.append(lanes(un[0], uf[0], vn[0], vf[0]))
            lo.append(lanes(un[1], uf[1], vn[1], vf[1]))
            a, c, d, e = un[0] * mn, uf[0] * mf, vn[0] * mn, vf[0] * mf
            left.append(lanes(a, c, d, e))
            right.append(lanes(d, e, -a, -c))
            a, c, d, e = un[1] * mn, uf[1] * mf, vn[1] * mn, vf[1] * mf
            rest.append(lanes(a, c, d, e))
            last.append(lanes(d, e, -a, -c))
        return hi, lo, rows(*left, *right, *rest, *last)

    row = iota((ST, GATES), 0)
    lane = iota((ST, GATES), 1)
    low = row >= lane % HALF
    high = row <= lane % HALF
    first = lane < HALF
    lane16 = iota((CH, GATES), 1)
    mine8 = iota((8, GATES), 1) // 16 == iota((8, GATES), 0)

    def store(q, p):
        p0, p1 = p[:16], pltpu.roll(p[16:32], 48, 1)
        p2 = pltpu.roll(p[32:], 96, 1)
        tail = [pltpu.roll(p2[h : h + 8], 0, 1, stride=16, stride_axis=0) for h in (0, 8)]
        main = jnp.where(lane16 < 48, p0, jnp.where(lane16 < 96, p1, p2))
        for j in range(16):
            out[q, :, j * GATES : (j + 1) * GATES] = main[j : j + 1]
        for j in range(2):
            extra = jnp.sum(jnp.where(mine8, tail[j], 0.0), 0, keepdims=True)
            out[q, :, (16 + j) * GATES : (17 + j) * GATES] = extra

    def pair(i):
        ha, wa, la = operands(i)
        hb, wb, lb = operands(i + 1)
        rhs = rows(*ha, zero, *hb, zero, *wa, zero, *wb, zero)
        dims = (((1,), (1,)), ((), ()))
        g = lax.dot_general(rows(la, lb), rhs, dims, preferred_element_type=f32)
        ga, gb = g[:192], g[192:]
        ga = ga[:96] + ga[96:]
        gb = gb[:96] + gb[96:]
        ga = ga[:, :GATES] + ga[:, GATES:]
        gb = gb[:, :GATES] + gb[:, GATES:]
        re = jnp.where(first, ga[:ST], gb[:ST])
        im = jnp.where(first, ga[ST:], gb[ST:])
        p = jnp.where(low, re, im)
        store(i, p)
        store(i + 1, pltpu.roll(p, HALF, 1))

    def step(j, c):
        for n in range(0, 16, 2):
            pair(j * 16 + n)
        return c

    lax.fori_loop(0, 4, step, 0)


def gram(place, near, far, masks):
    return pl.pallas_call(
        gram_kernel,
        out_shape=jax.ShapeDtypeStruct((64, 1, PACKED), f32),
        in_specs=[SM] + [VM] * 6,
        out_specs=VM,
        scratch_shapes=[pltpu.VMEM((2, 64, GATES), f32)],
        name="gram",
        compiler_params=pltpu.CompilerParams(vmem_limit_bytes=VMEM_LIMIT),
    )(place, near, far, *masks)


def solve_kernel(parts, sr, si, out):
    row = iota((ST, GATES), 0)
    lane = iota((ST, GATES), 1)
    line = []
    for j in range(PACKED // GATES):
        line.append(jnp.sum(parts[:, 0, j * GATES : (j + 1) * GATES], 0, keepdims=True) * (1.0 / TOTAL))
    main = rows(*line[:16])
    corner = rows(*[pltpu.roll(line[16 + j // 8], (GATES + 32 - 16 * (j % 8)) % GATES, 1) for j in range(16)])
    p2 = jnp.where(lane[:16] < 32, pltpu.roll(main, 32, 1), corner)
    p = rows(main, pltpu.roll(main, GATES - 48, 1), p2)
    full = rows(p, jnp.zeros((GATES - ST, GATES), f32)).T[:ST]
    re = jnp.where(row >= lane, p, full)
    im = jnp.where(row < lane, p, jnp.where(row == lane, 0.0, -full))
    are = jnp.where(lane < ST, re, sr[...])
    aim = jnp.where(lane < ST, im, si[...])
    for k in range(0, ST, 2):
        i0 = jnp.full((ST, GATES), k, jnp.int32)
        i1 = jnp.full((ST, GATES), k + 1, jnp.int32)
        c0r = jnp.take_along_axis(are, i0, 1)
        c0i = jnp.take_along_axis(aim, i0, 1)
        c1r = jnp.take_along_axis(are, i1, 1)
        c1i = jnp.take_along_axis(aim, i1, 1)
        r0, q0 = are[k : k + 1], aim[k : k + 1]
        r1, q1 = are[k + 1 : k + 2], aim[k + 1 : k + 2]
        a, d = c0r[k : k + 1], c1r[k + 1 : k + 2]
        br, bi = c1r[k : k + 1], c1i[k : k + 1]
        inv = 1.0 / (a * d - (br * br + bi * bi))
        a, d, br, bi = a * inv, d * inv, br * inv, bi * inv
        n0r = d * r0 - (br * r1 - bi * q1)
        n0i = d * q0 - (br * q1 + bi * r1)
        n1r = a * r1 - (br * r0 + bi * q0)
        n1i = a * q1 - (br * q0 - bi * r0)
        ur = (c0r * n0r - c0i * n0i) + (c1r * n1r - c1i * n1i)
        ui = (c0r * n0i + c0i * n0r) + (c1r * n1i + c1i * n1r)
        are = jnp.where(row == k, n0r, jnp.where(row == k + 1, n1r, are - ur))
        aim = jnp.where(row == k, n0i, jnp.where(row == k + 1, n1i, aim - ui))
    pad = jnp.zeros((GATES - ST, GATES), f32)
    wr = rows(are, pad).T[ST : ST + 1]
    wi = rows(aim, pad).T[ST : ST + 1]
    lane1 = iota((1, GATES), 1)
    w = jnp.where(lane1 < ST, wr, jnp.where(lane1 < 2 * ST, pltpu.roll(wi, ST, 1), 0.0))
    for j in range(64):
        out[j] = w


def solve(parts, sr, si):
    return pl.pallas_call(
        solve_kernel,
        out_shape=jax.ShapeDtypeStruct((64, 1, GATES), f32),
        in_specs=[VM] * 3,
        out_specs=VM,
        name="solve",
        compiler_params=pltpu.CompilerParams(vmem_limit_bytes=VMEM_LIMIT),
    )(parts, sr, si)


def power_kernel(place, near, far, w, out):
    core, dop = core_and_dop()
    zero = jnp.zeros((32, 2 * GATES), bf16)
    row = iota((8, GATES), 0)
    lane = iota((8, GATES), 1)

    def one(i):
        wt = jnp.broadcast_to(w[i], (8, GATES))
        turned = jnp.where(
            lane < ST,
            -pltpu.roll(wt, GATES - ST, 1),
            jnp.where(lane < 2 * ST, pltpu.roll(wt, ST, 1), 0.0),
        )
        wt = jnp.where(row % 2 == 0, wt, turned)
        hi = wt.astype(bf16).astype(f32)
        mid = (wt - hi).astype(bf16).astype(f32)
        lo = wt - hi - mid
        wt = jnp.where(row < 2, hi, jnp.where(row < 4, mid, jnp.where(row < 6, lo, 0.0)))
        lhs = rows(wt, jnp.zeros((8, GATES), f32)).astype(bf16)
        rhs = [[], [], []]
        for p in range(2):
            for t in range(SLOTS):
                s = place[i * SLOTS + t]
                x = lanes(near[p, s], far[p, s])
                hi, rest = split(x)
                x = x - hi.astype(f32)
                rhs[0].append(hi)
                rhs[1].append(rest)
                rhs[2].append((x - rest.astype(f32)).astype(bf16))
        rhs = [*rhs[0], zero, *rhs[1], zero, *rhs[2], zero]
        y = jnp.dot(lanes(lhs, lhs, lhs), rows(*rhs), preferred_element_type=f32)
        re = y[0:1] + y[2:3] + y[4:5]
        im = y[1:2] + y[3:4] + y[5:6]
        return re * re + im * im

    def step(j, c):
        group = j // 4
        y = rows(*[one(j * 8 + n) for n in range(8)])
        at = pl.ds(pl.multiple_of((j % 4) * 8, 8), 8)
        out[(2 * core + group) ^ dop, at, :] = y[:, :GATES]
        out[(2 - 2 * core + group) ^ dop, at, :] = y[:, GATES:]
        return c

    lax.fori_loop(0, 8, step, 0)


def power(place, near, far, w):
    return pl.pallas_call(
        power_kernel,
        out_shape=jax.ShapeDtypeStruct((ZN, 32, GATES), f32),
        in_specs=[SM] + [VM] * 3,
        out_specs=VM,
        name="power",
        compiler_params=pltpu.CompilerParams(vmem_limit_bytes=VMEM_LIMIT),
    )(place, near, far, w)


def cfar_kernel(p0, p1, p2, p3, inner, outer, guard, train, out, line):
    core, dop = core_and_dop()
    rank = lax.axis_index("range")
    width = 6 * GATES
    for k, ref in enumerate((p0, p1, p2, p3)):
        line[1 + (k ^ (2 * core + dop % 2))] = ref[...]
    line[5 * (1 - core)] = inner[...]
    line[5 * core] = outer[...]
    p = lanes(*[line[j] for j in range(6)])
    g = guard[:, :1]
    t = train[:, :1]
    total = p
    acc = jnp.where((t & 1) == 1, p, 0.0)
    for k in range(1, 7):
        total = total + pltpu.roll(total, width - (1 << (k - 1)), 1)
        acc = jnp.where((t >> k) & 1 == 1, total + pltpu.roll(acc, width - (1 << k), 1), acc)
    right = acc
    shift = g + 1
    for k in range(3):
        right = jnp.where((shift >> k) & 1 == 1, pltpu.roll(right, width - (1 << k), 1), right)
    left = acc
    shift = g + t
    for k in range(7):
        left = jnp.where((shift >> k) & 1 == 1, pltpu.roll(left, 1 << k, 1), left)
    lo, hi = GATES, GATES + 4 * GATES
    both = left[:, lo:hi] + right[:, lo:hi]
    pos = rank * (4 * GATES) + iota((32, 4 * GATES), 1)
    left_count = jnp.maximum(jnp.minimum(pos - g - 1, TOTAL - 1) - jnp.maximum(pos - g - t, 0) + 1, 0)
    right_count = jnp.maximum(jnp.minimum(pos + g + t, TOTAL - 1) - jnp.maximum(pos + g + 1, 0) + 1, 0)
    noise = both / (left_count + right_count).astype(f32)
    out[...] = p[:, lo:hi] / (noise + EPS)


def cfar(pieces, inner, outer, guard, train):
    return pl.pallas_call(
        cfar_kernel,
        out_shape=jax.ShapeDtypeStruct((32, 4 * GATES), f32),
        in_specs=[VM] * 8,
        out_specs=VM,
        scratch_shapes=[pltpu.VMEM((6, 32, GATES), f32)],
        name="cfar",
        compiler_params=pltpu.CompilerParams(vmem_limit_bytes=VMEM_LIMIT),
    )(*pieces, inner, outer, guard, train)


BOTH = ("range", "dop")
CORE_SWAP = [(i, i ^ 1) for i in range(32)]
SAME_CORE = [
    [((y * XN + x) * 2 + c) * ZN + z for y in range(YN) for x in range(XN) for z in range(ZN)]
    for c in range(2)
]


def flipped(bit):
    return [(i, i ^ bit) for i in range(ZN)]


def swap(value):
    return lax.ppermute(value, "range", CORE_SWAP)


def steering(bin_taper, phases):
    core, dop = core_and_dop()
    b = core * 64 + (lax.axis_index("range") // 2) * ZN + dop
    taper = lax.dynamic_index_in_dim(bin_taper, b, 0, keepdims=False)

    def lay(values):
        return jnp.broadcast_to((taper[:, None] * values[None, :]).reshape(ST, 1), (ST, GATES))

    return lay(jnp.cos(phases)), lay(jnp.sin(phases))


def chip_pairs(target):
    pairs = []
    for chip in range(XN * YN):
        for c in range(2):
            for z in range(ZN):
                to = target(c, z)
                pairs.append(((chip * 2 + c) * ZN + z, (chip * 2 + to[0]) * ZN + to[1]))
    return pairs


def shards(echoes, triplet, bin_taper, phases, excluded, guard_len, train_len):
    core, dop = core_and_dop()
    near, far = pack(echoes)
    far = swap(far)
    masks = [
        lax.ppermute(excluded, BOTH, chip_pairs(lambda c, z: (z // 2, (2 * c + z % 2) ^ k)))
        for k in range(ZN)
    ]
    place = places(triplet)
    part = gram(place, near, far, masks)
    part = lax.all_to_all(part, BOTH, 0, 0, tiled=True, axis_index_groups=SAME_CORE)
    sr, si = steering(bin_taper, phases)
    guard = jnp.broadcast_to(guard_len[:, None], (32, GATES))
    train = jnp.broadcast_to(train_len[:, None], (32, GATES))
    sr, si, guard, train = lax.optimization_barrier((sr, si, guard, train))
    w = solve(part, sr, si)
    w = lax.all_to_all(w, BOTH, 0, 0, tiled=True, axis_index_groups=SAME_CORE)
    pw = power(place, near, far, w)
    pieces = [
        lax.ppermute(pw[k], BOTH, chip_pairs(lambda c, z: ((z ^ k) // 2, 2 * c + (z ^ k) % 2)))
        for k in range(ZN)
    ]
    at = 2 * core + dop % 2
    at_tail = at ^ 3

    def chosen(index):
        value = pieces[0]
        for k in range(1, ZN):
            value = jnp.where(index == k, pieces[k], value)
        return value

    tail, head = chosen(at_tail), chosen(at)
    ranges = lax.axis_size("range")
    inner = swap(jnp.where(core == 0, tail, head))
    pairs = [(i, i + 1 if i % 2 else i - 1) for i in range(1, ranges - 1)]
    outer = lax.ppermute(jnp.where(core == 0, head, tail), "range", pairs)
    return cfar(pieces, inner, outer, guard, train)


def solution(mesh):
    placed = (
        P(None, None, None, ("range", "dop")),
        P(),
        P(),
        P(),
        P("dop", "range"),
        P("dop"),
        P("dop"),
    )
    return jax.shard_map(
        shards, mesh=mesh, in_specs=placed, out_specs=P("dop", "range"), check_vma=False
    )
```

```python
import functools
import jax
import jax.numpy as jnp
from jax import lax
from jax.experimental import pallas as pl
from jax.experimental.pallas import tpu as pltpu
from jax.sharding import PartitionSpec as P

CH = 16
SLOTS = 3
ST = 48
BINS = 128
BLOCK = 16
GATES = 128
TOTAL = 16384
EPS = 1e-6
HALF = 64
XN = 4
YN = 4
ZN = 4
WINDOW = 68
PACKED = ST * ST
UNROLL = 4
f32 = jnp.float32
bf16 = jnp.bfloat16
VMEM_LIMIT = 16 * 2**20

VM = pl.BlockSpec(memory_space=pltpu.VMEM)
SM = pl.BlockSpec(memory_space=pltpu.SMEM)


def core_and_dop():
    return lax.axis_index("range") % 2, lax.axis_index("dop")


def iota(shape, dim):
    return lax.broadcasted_iota(jnp.int32, shape, dim)


def split(x):
    hi = x.astype(bf16)
    return hi, (x - hi.astype(f32)).astype(bf16)


def lanes(*parts):
    return jnp.concatenate(parts, 1)


def rows(*parts):
    return jnp.concatenate(parts, 0)


def pack_kernel(echo, near, send, sems):
    core, _ = core_and_dop()
    copies = []
    for out, half in ((near, core), (send, 1 - core)):
        first = half * 64
        for start, at, count in (
            (first, 2, 64),
            ((first + BINS - 2) % BINS, 0, 2),
            ((first + 64) % BINS, 66, 2),
        ):
            copies.append(
                pltpu.make_async_copy(
                    echo.at[:, pl.ds(start, count)],
                    out.at[:, pl.ds(at, count)],
                    sems.at[len(copies)],
                )
            )
    for c in copies:
        c.start()
    for c in copies:
        c.wait()


def pack(echo):
    return pl.pallas_call(
        pack_kernel,
        out_shape=[jax.ShapeDtypeStruct((2, WINDOW, CH, GATES), f32)] * 2,
        in_specs=[pl.BlockSpec(memory_space=pltpu.HBM)],
        out_specs=[VM] * 2,
        scratch_shapes=[pltpu.SemaphoreType.DMA((6,))],
        name="pack",
        compiler_params=pltpu.CompilerParams(vmem_limit_bytes=52 * 2**20),
    )(echo)


def places(triplet):
    core, _ = core_and_dop()
    mine = lax.dynamic_slice_in_dim(triplet, core * 64, 64, 0)
    return ((mine - core * 64 + BINS + 2) & (BINS - 1)).reshape(64 * SLOTS)


def gram_kernel(second, place, near, far, mask, *refs):
    if second:
        done, whole, kept, out, sems = refs
    else:
        out, kept = refs
    core, dop = core_and_dop()
    group = (dop + 1) % 2 if second else dop % 2
    block = dop * (GATES // BLOCK) + (iota((64, 2 * GATES), 1) % GATES) // BLOCK
    block = block + 32 * (iota((64, 2 * GATES), 1) // GATES)
    pick = (iota((64, 2 * GATES), 0) == block).astype(f32)
    kept[...] = 1.0 - jnp.dot(mask[...].astype(f32), pick, preferred_element_type=f32)
    zero = jnp.zeros((16, 4 * GATES), bf16)

    def operands(i):
        m = kept[i : i + 1]
        mn = jnp.broadcast_to(m[:, :GATES], (CH, GATES)).astype(bf16)
        mf = jnp.broadcast_to(m[:, GATES:], (CH, GATES)).astype(bf16)
        hi, lo, left, right, rest, last = [], [], [], [], [], []
        for t in range(SLOTS):
            s = place[(group * 32 + i) * SLOTS + t]
            un, uf, vn, vf = split(near[0, s]), split(far[0, s]), split(near[1, s]), split(far[1, s])
            hi.append(lanes(un[0], uf[0], vn[0], vf[0]))
            lo.append(lanes(un[1], uf[1], vn[1], vf[1]))
            a, c, d, e = un[0] * mn, uf[0] * mf, vn[0] * mn, vf[0] * mf
            left.append(lanes(a, c, d, e))
            right.append(lanes(d, e, -a, -c))
            a, c, d, e = un[1] * mn, uf[1] * mf, vn[1] * mn, vf[1] * mf
            rest.append(lanes(a, c, d, e))
            last.append(lanes(d, e, -a, -c))
        return hi, lo, rows(*left, *right, *rest, *last)

    row = iota((ST, GATES), 0)
    lane = iota((ST, GATES), 1)
    low = row >= lane % HALF
    high = row <= lane % HALF
    first = lane < HALF
    lane16 = iota((CH, GATES), 1)
    mine8 = iota((8, GATES), 1) // 16 == iota((8, GATES), 0)

    def store(q, p):
        p0, p1 = p[:16], pltpu.roll(p[16:32], 48, 1)
        p2 = pltpu.roll(p[32:], 96, 1)
        tail = [pltpu.roll(p2[h : h + 8], 0, 1, stride=16, stride_axis=0) for h in (0, 8)]
        main = jnp.where(lane16 < 48, p0, jnp.where(lane16 < 96, p1, p2))
        for j in range(16):
            out[q, :, j * GATES : (j + 1) * GATES] = main[j : j + 1]
        for j in range(2):
            extra = jnp.sum(jnp.where(mine8, tail[j], 0.0), 0, keepdims=True)
            out[q, :, (16 + j) * GATES : (17 + j) * GATES] = extra

    def pair(i):
        ha, wa, la = operands(i)
        hb, wb, lb = operands(i + 1)
        rhs = rows(*ha, zero, *hb, zero, *wa, zero, *wb, zero)
        dims = (((1,), (1,)), ((), ()))
        g = lax.dot_general(rows(la, lb), rhs, dims, preferred_element_type=f32)
        ga, gb = g[:192], g[192:]
        ga = ga[:96] + ga[96:]
        gb = gb[:96] + gb[96:]
        ga = ga[:, :GATES] + ga[:, GATES:]
        gb = gb[:, :GATES] + gb[:, GATES:]
        re = jnp.where(first, ga[:ST], gb[:ST])
        im = jnp.where(first, ga[ST:], gb[ST:])
        p = jnp.where(low, re, im)
        store(i, p)
        store(i + 1, pltpu.roll(p, HALF, 1))

    copies = []

    def ship(value, first, at, count):
        copies.append(
            pltpu.make_async_copy(
                value.at[pl.ds(first, count)],
                whole.at[pl.ds(pl.multiple_of(at + first, 16), count)],
                sems.at[len(copies)],
            )
        )
        copies[-1].start()

    if second:
        ship(done, 0, (1 - group) * 32, 32)
    for i in range(0, 32, 2):
        pair(i)
        if second and i in (14, 30):
            ship(out, i - 14, group * 32, 16)
    for c in copies:
        c.wait()


def gram(second, place, near, far, *extra):
    block = (32, 1, PACKED)
    kept = pltpu.VMEM((32, 2 * GATES), f32)
    return pl.pallas_call(
        functools.partial(gram_kernel, second),
        out_shape=jax.ShapeDtypeStruct((64, 1, PACKED) if second else block, f32),
        in_specs=[SM] + [VM] * (4 if second else 3),
        out_specs=pl.BlockSpec(memory_space=pl.ANY) if second else VM,
        scratch_shapes=[kept, pltpu.VMEM(block, f32), pltpu.SemaphoreType.DMA((3,))] if second else [kept],
        name="gram_b" if second else "gram_a",
        compiler_params=pltpu.CompilerParams(vmem_limit_bytes=VMEM_LIMIT),
    )(place, near, far, *extra)


def solve_kernel(parts, sr, si, out):
    row = iota((ST, GATES), 0)
    lane = iota((ST, GATES), 1)
    line = []
    for j in range(PACKED // GATES):
        line.append(jnp.sum(parts[:, 0, j * GATES : (j + 1) * GATES], 0, keepdims=True) * (1.0 / TOTAL))
    main = rows(*line[:16])
    corner = rows(*[pltpu.roll(line[16 + j // 8], (GATES + 32 - 16 * (j % 8)) % GATES, 1) for j in range(16)])
    p2 = jnp.where(lane[:16] < 32, pltpu.roll(main, 32, 1), corner)
    p = rows(main, pltpu.roll(main, GATES - 48, 1), p2)
    full = rows(p, jnp.zeros((GATES - ST, GATES), f32)).T[:ST]
    re = jnp.where(row >= lane, p, full)
    im = jnp.where(row < lane, p, jnp.where(row == lane, 0.0, -full))
    are = jnp.where(lane < ST, re, sr[...])
    aim = jnp.where(lane < ST, im, si[...])
    for k in range(0, ST, 2):
        i0 = jnp.full((ST, GATES), k, jnp.int32)
        i1 = jnp.full((ST, GATES), k + 1, jnp.int32)
        c0r = jnp.take_along_axis(are, i0, 1)
        c0i = jnp.take_along_axis(aim, i0, 1)
        c1r = jnp.take_along_axis(are, i1, 1)
        c1i = jnp.take_along_axis(aim, i1, 1)
        r0, q0 = are[k : k + 1], aim[k : k + 1]
        r1, q1 = are[k + 1 : k + 2], aim[k + 1 : k + 2]
        a, d = c0r[k : k + 1], c1r[k + 1 : k + 2]
        br, bi = c1r[k : k + 1], c1i[k : k + 1]
        inv = 1.0 / (a * d - (br * br + bi * bi))
        a, d, br, bi = a * inv, d * inv, br * inv, bi * inv
        n0r = d * r0 - (br * r1 - bi * q1)
        n0i = d * q0 - (br * q1 + bi * r1)
        n1r = a * r1 - (br * r0 + bi * q0)
        n1i = a * q1 - (br * q0 - bi * r0)
        ur = (c0r * n0r - c0i * n0i) + (c1r * n1r - c1i * n1i)
        ui = (c0r * n0i + c0i * n0r) + (c1r * n1i + c1i * n1r)
        are = jnp.where(row == k, n0r, jnp.where(row == k + 1, n1r, are - ur))
        aim = jnp.where(row == k, n0i, jnp.where(row == k + 1, n1i, aim - ui))
    pad = jnp.zeros((GATES - ST, GATES), f32)
    wr = rows(are, pad).T[ST : ST + 1]
    wi = rows(aim, pad).T[ST : ST + 1]
    lane1 = iota((1, GATES), 1)
    w = jnp.where(lane1 < ST, wr, jnp.where(lane1 < 2 * ST, pltpu.roll(wi, ST, 1), 0.0))
    for j in range(64):
        out[j] = w


def solve(parts, sr, si):
    return pl.pallas_call(
        solve_kernel,
        out_shape=jax.ShapeDtypeStruct((64, 1, GATES), f32),
        in_specs=[VM] * 3,
        out_specs=VM,
        name="solve",
        compiler_params=pltpu.CompilerParams(vmem_limit_bytes=VMEM_LIMIT),
    )(parts, sr, si)


def power_kernel(place, near, far, w, own, other):
    core, dop = core_and_dop()
    zero = jnp.zeros((32, 2 * GATES), bf16)
    row = iota((8, GATES), 0)
    lane = iota((8, GATES), 1)

    def one(i):
        wt = jnp.broadcast_to(w[i], (8, GATES))
        turned = jnp.where(
            lane < ST,
            -pltpu.roll(wt, GATES - ST, 1),
            jnp.where(lane < 2 * ST, pltpu.roll(wt, ST, 1), 0.0),
        )
        wt = jnp.where(row % 2 == 0, wt, turned)
        hi = wt.astype(bf16).astype(f32)
        mid = (wt - hi).astype(bf16).astype(f32)
        lo = wt - hi - mid
        wt = jnp.where(row < 2, hi, jnp.where(row < 4, mid, jnp.where(row < 6, lo, 0.0)))
        lhs = rows(wt, jnp.zeros((8, GATES), f32)).astype(bf16)
        rhs = [[], [], []]
        for p in range(2):
            for t in range(SLOTS):
                s = place[i * SLOTS + t]
                x = lanes(near[p, s], far[p, s])
                hi, rest = split(x)
                x = x - hi.astype(f32)
                rhs[0].append(hi)
                rhs[1].append(rest)
                rhs[2].append((x - rest.astype(f32)).astype(bf16))
        rhs = [*rhs[0], zero, *rhs[1], zero, *rhs[2], zero]
        y = jnp.dot(lanes(lhs, lhs, lhs), rows(*rhs), preferred_element_type=f32)
        re = y[0:1] + y[2:3] + y[4:5]
        im = y[1:2] + y[3:4] + y[5:6]
        return re * re + im * im

    def step(j, c):
        k = (j // 4) ^ (dop % 2)
        y = rows(*[one(j * 8 + n) for n in range(8)])
        at = pl.ds(pl.multiple_of((j % 4) * 8, 8), 8)
        own[k, at, :] = y[:, :GATES]
        other[k, at, :] = y[:, GATES:]
        return c

    lax.fori_loop(0, 8, step, 0, unroll=UNROLL)


def power(place, near, far, w):
    return pl.pallas_call(
        power_kernel,
        out_shape=[jax.ShapeDtypeStruct((2, 32, GATES), f32)] * 2,
        in_specs=[SM] + [VM] * 3,
        out_specs=[VM] * 2,
        name="power",
        compiler_params=pltpu.CompilerParams(vmem_limit_bytes=VMEM_LIMIT),
    )(place, near, far, w)


def window_sums(p, g, t):
    width = p.shape[1]
    total = p
    acc = jnp.where((t & 1) == 1, p, 0.0)
    for k in range(1, 7):
        total = total + pltpu.roll(total, width - (1 << (k - 1)), 1)
        acc = jnp.where((t >> k) & 1 == 1, total + pltpu.roll(acc, width - (1 << k), 1), acc)
    right = acc
    shift = g + 1
    for k in range(3):
        right = jnp.where((shift >> k) & 1 == 1, pltpu.roll(right, width - (1 << k), 1), right)
    left = acc
    shift = g + t
    for k in range(7):
        left = jnp.where((shift >> k) & 1 == 1, pltpu.roll(left, 1 << k, 1), left)
    return left, right


def noise_kernel(p0, p1, p2, p3, inner, guard, train, out, line):
    core, dop = core_and_dop()
    rank = lax.axis_index("range")
    for k, ref in enumerate((p0, p1, p2, p3)):
        line[1 + (dop ^ k)] = ref[...]
    line[5 * (1 - core)] = inner[...]
    line[5 * core] = jnp.zeros((32, GATES), f32)
    p = lanes(*[line[j] for j in range(6)])
    g = guard[:, :1]
    t = train[:, :1]
    left, right = window_sums(p, g, t)
    lo, hi = GATES, GATES + 4 * GATES
    pos = rank * (4 * GATES) + iota((32, 4 * GATES), 1)
    left_count = jnp.maximum(jnp.minimum(pos - g - 1, TOTAL - 1) - jnp.maximum(pos - g - t, 0) + 1, 0)
    right_count = jnp.maximum(jnp.minimum(pos + g + t, TOTAL - 1) - jnp.maximum(pos + g + 1, 0) + 1, 0)
    out[0] = p[:, lo:hi]
    out[1] = left[:, lo:hi] + right[:, lo:hi]
    out[2] = (left_count + right_count).astype(f32)


def noise(pieces, inner, guard, train):
    return pl.pallas_call(
        noise_kernel,
        out_shape=jax.ShapeDtypeStruct((3, 32, 4 * GATES), f32),
        in_specs=[VM] * 7,
        out_specs=VM,
        scratch_shapes=[pltpu.VMEM((6, 32, GATES), f32)],
        name="noise",
        compiler_params=pltpu.CompilerParams(vmem_limit_bytes=VMEM_LIMIT),
    )(*pieces, inner, guard, train)


def cfar_kernel(known, outer, guard, train, out, line):
    core, _ = core_and_dop()
    line[core] = outer[...]
    line[1 - core] = jnp.zeros((32, GATES), f32)
    p = lanes(line[0], line[1])
    left, right = window_sums(p, guard[:, :1], train[:, :1])
    sums = known[1]
    head = sums[:, :GATES] + jnp.where(core == 0, left[:, GATES:], 0.0)
    tail = sums[:, 3 * GATES :] + jnp.where(core == 1, right[:, :GATES], 0.0)
    sums = lanes(head, sums[:, GATES : 3 * GATES], tail)
    out[...] = known[0] / (sums / known[2] + EPS)


def cfar(known, outer, guard, train):
    return pl.pallas_call(
        cfar_kernel,
        out_shape=jax.ShapeDtypeStruct((32, 4 * GATES), f32),
        in_specs=[VM] * 4,
        out_specs=VM,
        scratch_shapes=[pltpu.VMEM((2, 32, GATES), f32)],
        name="cfar",
        compiler_params=pltpu.CompilerParams(vmem_limit_bytes=VMEM_LIMIT),
    )(known, outer, guard, train)


BOTH = ("range", "dop")
CORE_SWAP = [(i, i ^ 1) for i in range(32)]
SAME_CORE = [
    [((y * XN + x) * 2 + c) * ZN + z for z in range(ZN) for y in range(YN) for x in range(XN)]
    for c in range(2)
]


def flipped(bit):
    return [(i, i ^ bit) for i in range(ZN)]


def swap(value):
    return lax.ppermute(value, "range", CORE_SWAP)


def steering(bin_taper, phases):
    core, dop = core_and_dop()
    b = core * 64 + dop * 16 + lax.axis_index("range") // 2
    taper = lax.dynamic_index_in_dim(bin_taper, b, 0, keepdims=False)

    def lay(values):
        return jnp.broadcast_to((taper[:, None] * values[None, :]).reshape(ST, 1), (ST, GATES))

    return lay(jnp.cos(phases)), lay(jnp.sin(phases))


def shards(echoes, triplet, bin_taper, phases, excluded, guard_len, train_len):
    core, dop = core_and_dop()
    place = places(triplet)
    other = swap(excluded)
    near, far = pack(echoes)
    far, other = lax.optimization_barrier((far, other))
    far = swap(far)
    mine = lanes(excluded, other)
    across = lax.ppermute(mine, "dop", flipped(2))
    m0 = jnp.where(dop // 2 == core, mine, across)
    m1 = lax.ppermute(m0, "dop", flipped(1))
    part = gram(False, place, near, far, m0)
    part = gram(True, place, near, far, m1, part)
    part = lax.all_to_all(part, BOTH, 0, 0, tiled=True, axis_index_groups=SAME_CORE)
    sr, si = steering(bin_taper, phases)
    guard = jnp.broadcast_to(guard_len[:, None], (32, GATES))
    train = jnp.broadcast_to(train_len[:, None], (32, GATES))
    sr, si, guard, train = lax.optimization_barrier((sr, si, guard, train))
    w = solve(part, sr, si)
    w = lax.all_to_all(w, BOTH, 0, 0, tiled=True, axis_index_groups=SAME_CORE)
    own, away = power(place, near, far, w)
    came = swap(away)
    pieces = [
        jnp.where((dop // 2) ^ (k // 2) == core, own[k % 2], came[k % 2]) for k in range(ZN)
    ]
    pieces = [pieces[0]] + [lax.ppermute(pieces[k], "dop", flipped(k)) for k in (1, 2, 3)]
    p0, p1, p2, p3 = pieces
    ranges = lax.axis_size("range")
    tail = jnp.where(dop == 0, p3, jnp.where(dop == 1, p2, jnp.where(dop == 2, p1, p0)))
    head = jnp.where(dop == 0, p0, jnp.where(dop == 1, p1, jnp.where(dop == 2, p2, p3)))
    inner = swap(jnp.where(core == 0, tail, head))
    pairs = [(i, i + 1 if i % 2 else i - 1) for i in range(1, ranges - 1)]
    outer = lax.ppermute(jnp.where(core == 0, head, tail), "range", pairs)
    return cfar(noise(pieces, inner, guard, train), outer, guard, train)


def solution(mesh):
    placed = (
        P(None, None, None, ("range", "dop")),
        P(),
        P(),
        P(),
        P("dop", "range"),
        P("dop"),
        P("dop"),
    )
    return jax.shard_map(
        shards, mesh=mesh, in_specs=placed, out_specs=P("dop", "range"), check_vma=False
    )
```

```python
import functools
import jax
import jax.numpy as jnp
from jax import lax
from jax.experimental import pallas as pl
from jax.experimental.pallas import tpu as pltpu
from jax.sharding import PartitionSpec as P

CH = 16
SLOTS = 3
ST = 48
BINS = 128
BLOCK = 16
GATES = 128
TOTAL = 16384
EPS = 1e-6
HALF = 64
XN = 4
YN = 4
ZN = 4
WINDOW = 20
PACKED = ST * ST
UNROLL = 4
f32 = jnp.float32
bf16 = jnp.bfloat16
VMEM_LIMIT = 16 * 2**20

VM = pl.BlockSpec(memory_space=pltpu.VMEM)
SM = pl.BlockSpec(memory_space=pltpu.SMEM)


def core_and_dop():
    return lax.axis_index("range") % 2, lax.axis_index("dop")


def iota(shape, dim):
    return lax.broadcasted_iota(jnp.int32, shape, dim)


def split(x):
    hi = x.astype(bf16)
    return hi, (x - hi.astype(f32)).astype(bf16)


def lanes(*parts):
    return jnp.concatenate(parts, 1)


def rows(*parts):
    return jnp.concatenate(parts, 0)


def pack_kernel(echo, near, send, sems):
    core, _ = core_and_dop()
    copies = []
    for out, half in ((near, core), (send, 1 - core)):
        for z in range(ZN):
            first = z * 32 + half * 16
            for start, at, count in (
                (first, 2, 16),
                ((first + BINS - 2) % BINS, 0, 2),
                ((first + 16) % BINS, 18, 2),
            ):
                copies.append(
                    pltpu.make_async_copy(
                        echo.at[:, pl.ds(start, count)],
                        out.at[:, pl.ds(z * WINDOW + at, count)],
                        sems.at[len(copies)],
                    )
                )
    for c in copies:
        c.start()
    for c in copies:
        c.wait()


def pack(echo):
    return pl.pallas_call(
        pack_kernel,
        out_shape=[jax.ShapeDtypeStruct((2, ZN * WINDOW, CH, GATES), f32)] * 2,
        in_specs=[pl.BlockSpec(memory_space=pltpu.HBM)],
        out_specs=[VM] * 2,
        scratch_shapes=[pltpu.SemaphoreType.DMA((6 * ZN,))],
        name="pack",
        compiler_params=pltpu.CompilerParams(vmem_limit_bytes=52 * 2**20),
    )(echo)


def places(triplet):
    core, _ = core_and_dop()
    mine = lax.dynamic_index_in_dim(triplet.reshape(ZN, 2, 16, SLOTS), core, 1, keepdims=False)
    group = iota((ZN, 16, SLOTS), 0)
    where = group * WINDOW + ((mine - (group * 32 + core * 16) + BINS + 2) & (BINS - 1))
    return where.reshape(ZN * 16 * SLOTS)


def gram_kernel(second, place, near, far, *refs):
    masks = refs[: 1 if second else 2]
    if second:
        done, whole, kept, out, sems = refs[1:]
    else:
        out, kept = refs[2:]
    core, dop = core_and_dop()
    block = dop * (GATES // BLOCK) + (iota((64, 2 * GATES), 1) % GATES) // BLOCK
    block = block + 32 * (iota((64, 2 * GATES), 1) // GATES)
    pick = (iota((64, 2 * GATES), 0) == block).astype(f32)
    left = 1.0 - jnp.dot(rows(*[m[...] for m in masks]).astype(f32), pick, preferred_element_type=f32)
    for k in range(2):
        kept[k] = left[16 * k : 16 * k + 16]
    zero = jnp.zeros((16, 4 * GATES), bf16)
    base = 2 if second else 0

    def operands(k, i):
        z = dop ^ (base + k)
        m = kept[k, pl.ds(i, 1), :]
        mn = jnp.broadcast_to(m[:, :GATES], (CH, GATES)).astype(bf16)
        mf = jnp.broadcast_to(m[:, GATES:], (CH, GATES)).astype(bf16)
        hi, lo, left, right, rest, last = [], [], [], [], [], []
        for t in range(SLOTS):
            s = place[(z * 16 + i) * SLOTS + t]
            un, uf, vn, vf = split(near[0, s]), split(far[0, s]), split(near[1, s]), split(far[1, s])
            hi.append(lanes(un[0], uf[0], vn[0], vf[0]))
            lo.append(lanes(un[1], uf[1], vn[1], vf[1]))
            a, c, d, e = un[0] * mn, uf[0] * mf, vn[0] * mn, vf[0] * mf
            left.append(lanes(a, c, d, e))
            right.append(lanes(d, e, -a, -c))
            a, c, d, e = un[1] * mn, uf[1] * mf, vn[1] * mn, vf[1] * mf
            rest.append(lanes(a, c, d, e))
            last.append(lanes(d, e, -a, -c))
        return hi, lo, rows(*left, *right, *rest, *last)

    row = iota((ST, GATES), 0)
    lane = iota((ST, GATES), 1)
    low = row >= lane % HALF
    high = row <= lane % HALF
    first = lane < HALF
    lane16 = iota((CH, GATES), 1)
    mine8 = iota((8, GATES), 1) // 16 == iota((8, GATES), 0)

    def store(k, i, p):
        q = k * 16 + i
        p0, p1 = p[:16], pltpu.roll(p[16:32], 48, 1)
        p2 = pltpu.roll(p[32:], 96, 1)
        tail = [pltpu.roll(p2[h : h + 8], 0, 1, stride=16, stride_axis=0) for h in (0, 8)]
        main = jnp.where(lane16 < 48, p0, jnp.where(lane16 < 96, p1, p2))
        for j in range(16):
            out[q, :, j * GATES : (j + 1) * GATES] = main[j : j + 1]
        for j in range(2):
            extra = jnp.sum(jnp.where(mine8, tail[j], 0.0), 0, keepdims=True)
            out[q, :, (16 + j) * GATES : (17 + j) * GATES] = extra

    def pair(k, i):
        ha, wa, la = operands(k, i)
        hb, wb, lb = operands(k, i + 1)
        rhs = rows(*ha, zero, *hb, zero, *wa, zero, *wb, zero)
        dims = (((1,), (1,)), ((), ()))
        g = lax.dot_general(rows(la, lb), rhs, dims, preferred_element_type=f32)
        ga, gb = g[:192], g[192:]
        ga = ga[:96] + ga[96:]
        gb = gb[:96] + gb[96:]
        ga = ga[:, :GATES] + ga[:, GATES:]
        gb = gb[:, :GATES] + gb[:, GATES:]
        re = jnp.where(first, ga[:ST], gb[:ST])
        im = jnp.where(first, ga[ST:], gb[ST:])
        p = jnp.where(low, re, im)
        store(k, i, p)
        store(k, i + 1, pltpu.roll(p, HALF, 1))

    copies = []

    def ship(value, k):
        first = pl.multiple_of((dop ^ k) * 16, 16)
        copies.append(
            pltpu.make_async_copy(
                value.at[pl.ds((k % 2) * 16, 16)], whole.at[pl.ds(first, 16)], sems.at[k]
            )
        )
        copies[-1].start()

    if second:
        ship(done, 0)
        ship(done, 1)
    for k in range(2):
        for i in range(0, 16, 2):
            pair(k, i)
        if second:
            ship(out, 2 + k)
    for c in copies:
        c.wait()


def gram(second, place, near, far, extra):
    block = (32, 1, PACKED)
    kept = pltpu.VMEM((2, 16, 2 * GATES), f32)
    return pl.pallas_call(
        functools.partial(gram_kernel, second),
        out_shape=pltpu.HBM((64, 1, PACKED), f32) if second else jax.ShapeDtypeStruct(block, f32),
        in_specs=[SM] + [VM] * 4,
        out_specs=pl.BlockSpec(memory_space=pltpu.HBM) if second else VM,
        scratch_shapes=[kept, pltpu.VMEM(block, f32), pltpu.SemaphoreType.DMA((4,))] if second else [kept],
        name="gram_b" if second else "gram_a",
        compiler_params=pltpu.CompilerParams(vmem_limit_bytes=VMEM_LIMIT),
    )(place, near, far, *extra)


def solve_kernel(parts, sr, si, out):
    row = iota((ST, GATES), 0)
    lane = iota((ST, GATES), 1)
    line = []
    for j in range(PACKED // GATES):
        line.append(jnp.sum(parts[:, 0, j * GATES : (j + 1) * GATES], 0, keepdims=True) * (1.0 / TOTAL))
    main = rows(*line[:16])
    corner = rows(*[pltpu.roll(line[16 + j // 8], (GATES + 32 - 16 * (j % 8)) % GATES, 1) for j in range(16)])
    p2 = jnp.where(lane[:16] < 32, pltpu.roll(main, 32, 1), corner)
    p = rows(main, pltpu.roll(main, GATES - 48, 1), p2)
    full = rows(p, jnp.zeros((GATES - ST, GATES), f32)).T[:ST]
    re = jnp.where(row >= lane, p, full)
    im = jnp.where(row < lane, p, jnp.where(row == lane, 0.0, -full))
    are = jnp.where(lane < ST, re, sr[...])
    aim = jnp.where(lane < ST, im, si[...])
    for k in range(0, ST, 2):
        i0 = jnp.full((ST, GATES), k, jnp.int32)
        i1 = jnp.full((ST, GATES), k + 1, jnp.int32)
        c0r = jnp.take_along_axis(are, i0, 1)
        c0i = jnp.take_along_axis(aim, i0, 1)
        c1r = jnp.take_along_axis(are, i1, 1)
        c1i = jnp.take_along_axis(aim, i1, 1)
        r0, q0 = are[k : k + 1], aim[k : k + 1]
        r1, q1 = are[k + 1 : k + 2], aim[k + 1 : k + 2]
        a, d = c0r[k : k + 1], c1r[k + 1 : k + 2]
        br, bi = c1r[k : k + 1], c1i[k : k + 1]
        inv = 1.0 / (a * d - (br * br + bi * bi))
        a, d, br, bi = a * inv, d * inv, br * inv, bi * inv
        n0r = d * r0 - (br * r1 - bi * q1)
        n0i = d * q0 - (br * q1 + bi * r1)
        n1r = a * r1 - (br * r0 + bi * q0)
        n1i = a * q1 - (br * q0 - bi * r0)
        ur = (c0r * n0r - c0i * n0i) + (c1r * n1r - c1i * n1i)
        ui = (c0r * n0i + c0i * n0r) + (c1r * n1i + c1i * n1r)
        are = jnp.where(row == k, n0r, jnp.where(row == k + 1, n1r, are - ur))
        aim = jnp.where(row == k, n0i, jnp.where(row == k + 1, n1i, aim - ui))
    pad = jnp.zeros((GATES - ST, GATES), f32)
    wr = rows(are, pad).T[ST : ST + 1]
    wi = rows(aim, pad).T[ST : ST + 1]
    lane1 = iota((1, GATES), 1)
    w = jnp.where(lane1 < ST, wr, jnp.where(lane1 < 2 * ST, pltpu.roll(wi, ST, 1), 0.0))
    for j in range(64):
        out[j] = w


def solve(parts, sr, si):
    return pl.pallas_call(
        solve_kernel,
        out_shape=jax.ShapeDtypeStruct((64, 1, GATES), f32),
        in_specs=[VM] * 3,
        out_specs=VM,
        name="solve",
        compiler_params=pltpu.CompilerParams(vmem_limit_bytes=VMEM_LIMIT),
    )(parts, sr, si)


def power_kernel(place, near, far, w, own, other):
    core, dop = core_and_dop()
    zero = jnp.zeros((32, 2 * GATES), bf16)
    row = iota((8, GATES), 0)
    lane = iota((8, GATES), 1)

    def one(k, i):
        z = dop ^ k
        wt = jnp.broadcast_to(w[z * 16 + i], (8, GATES))
        turned = jnp.where(
            lane < ST,
            -pltpu.roll(wt, GATES - ST, 1),
            jnp.where(lane < 2 * ST, pltpu.roll(wt, ST, 1), 0.0),
        )
        wt = jnp.where(row % 2 == 0, wt, turned)
        hi = wt.astype(bf16).astype(f32)
        mid = (wt - hi).astype(bf16).astype(f32)
        lo = wt - hi - mid
        wt = jnp.where(row < 2, hi, jnp.where(row < 4, mid, jnp.where(row < 6, lo, 0.0)))
        lhs = rows(wt, jnp.zeros((8, GATES), f32)).astype(bf16)
        rhs = [[], [], []]
        for p in range(2):
            for t in range(SLOTS):
                s = place[(z * 16 + i) * SLOTS + t]
                x = lanes(near[p, s], far[p, s])
                hi, rest = split(x)
                x = x - hi.astype(f32)
                rhs[0].append(hi)
                rhs[1].append(rest)
                rhs[2].append((x - rest.astype(f32)).astype(bf16))
        rhs = [*rhs[0], zero, *rhs[1], zero, *rhs[2], zero]
        y = jnp.dot(lanes(lhs, lhs, lhs), rows(*rhs), preferred_element_type=f32)
        re = y[0:1] + y[2:3] + y[4:5]
        im = y[1:2] + y[3:4] + y[5:6]
        return re * re + im * im

    def step(j, c):
        k = j // 2
        i = (j % 2) * 8
        y = rows(*[one(k, i + n) for n in range(8)])
        at = pl.ds(pl.multiple_of(i, 8), 8)
        own[k, at, :] = y[:, :GATES]
        other[k, at, :] = y[:, GATES:]
        return c

    lax.fori_loop(0, 8, step, 0, unroll=UNROLL)


def power(place, near, far, w):
    return pl.pallas_call(
        power_kernel,
        out_shape=[jax.ShapeDtypeStruct((ZN, 16, GATES), f32)] * 2,
        in_specs=[SM] + [VM] * 3,
        out_specs=[VM] * 2,
        name="power",
        compiler_params=pltpu.CompilerParams(vmem_limit_bytes=VMEM_LIMIT),
    )(place, near, far, w)


def window_sums(p, g, t):
    width = p.shape[1]
    total = p
    acc = jnp.where((t & 1) == 1, p, 0.0)
    for k in range(1, 7):
        total = total + pltpu.roll(total, width - (1 << (k - 1)), 1)
        acc = jnp.where((t >> k) & 1 == 1, total + pltpu.roll(acc, width - (1 << k), 1), acc)
    right = acc
    shift = g + 1
    for k in range(3):
        right = jnp.where((shift >> k) & 1 == 1, pltpu.roll(right, width - (1 << k), 1), right)
    left = acc
    shift = g + t
    for k in range(7):
        left = jnp.where((shift >> k) & 1 == 1, pltpu.roll(left, 1 << k, 1), left)
    return left, right


def noise_kernel(p0, p1, p2, p3, inner, guard, train, out, line):
    core, dop = core_and_dop()
    rank = lax.axis_index("range")
    for k, ref in enumerate((p0, p1, p2, p3)):
        at = 1 + (dop ^ k)
        line[at, core] = ref[0]
        line[at, 1 - core] = ref[1]
    at = 5 * (1 - core)
    line[at, 1 - core] = inner[0]
    line[at, core] = inner[1]
    line[5 * core] = jnp.zeros((2, 16, GATES), f32)
    p = lanes(*[rows(line[j, 0], line[j, 1]) for j in range(6)])
    g = guard[:, :1]
    t = train[:, :1]
    left, right = window_sums(p, g, t)
    lo, hi = GATES, GATES + 4 * GATES
    pos = rank * (4 * GATES) + iota((32, 4 * GATES), 1)
    left_count = jnp.maximum(jnp.minimum(pos - g - 1, TOTAL - 1) - jnp.maximum(pos - g - t, 0) + 1, 0)
    right_count = jnp.maximum(jnp.minimum(pos + g + t, TOTAL - 1) - jnp.maximum(pos + g + 1, 0) + 1, 0)
    out[0] = p[:, lo:hi]
    out[1] = left[:, lo:hi] + right[:, lo:hi]
    out[2] = (left_count + right_count).astype(f32)


def noise(pieces, inner, guard, train):
    return pl.pallas_call(
        noise_kernel,
        out_shape=jax.ShapeDtypeStruct((3, 32, 4 * GATES), f32),
        in_specs=[VM] * 7,
        out_specs=VM,
        scratch_shapes=[pltpu.VMEM((6, 2, 16, GATES), f32)],
        name="noise",
        compiler_params=pltpu.CompilerParams(vmem_limit_bytes=VMEM_LIMIT),
    )(*pieces, inner, guard, train)


def cfar_kernel(known, outer, guard, train, out, line):
    core, _ = core_and_dop()
    line[core, 1 - core] = outer[0]
    line[core, core] = outer[1]
    line[1 - core] = jnp.zeros((2, 16, GATES), f32)
    p = lanes(*[rows(line[j, 0], line[j, 1]) for j in range(2)])
    left, right = window_sums(p, guard[:, :1], train[:, :1])
    sums = known[1]
    head = sums[:, :GATES] + jnp.where(core == 0, left[:, GATES:], 0.0)
    tail = sums[:, 3 * GATES :] + jnp.where(core == 1, right[:, :GATES], 0.0)
    sums = lanes(head, sums[:, GATES : 3 * GATES], tail)
    out[...] = known[0] / (sums / known[2] + EPS)


def cfar(known, outer, guard, train):
    return pl.pallas_call(
        cfar_kernel,
        out_shape=jax.ShapeDtypeStruct((32, 4 * GATES), f32),
        in_specs=[VM] * 4,
        out_specs=VM,
        scratch_shapes=[pltpu.VMEM((2, 2, 16, GATES), f32)],
        name="cfar",
        compiler_params=pltpu.CompilerParams(vmem_limit_bytes=VMEM_LIMIT),
    )(known, outer, guard, train)


BOTH = ("range", "dop")
CORE_SWAP = [(i, i ^ 1) for i in range(32)]
SAME_CORE = [
    [((y * XN + x) * 2 + c) * ZN + z for z in range(ZN) for y in range(YN) for x in range(XN)]
    for c in range(2)
]


def flipped(bit):
    return [(i, i ^ bit) for i in range(ZN)]


def swap(value):
    return lax.ppermute(value, "range", CORE_SWAP)


def steering(bin_taper, phases):
    core, dop = core_and_dop()
    b = dop * 32 + core * 16 + lax.axis_index("range") // 2
    taper = lax.dynamic_index_in_dim(bin_taper, b, 0, keepdims=False)

    def lay(values):
        return jnp.broadcast_to((taper[:, None] * values[None, :]).reshape(ST, 1), (ST, GATES))

    return lay(jnp.cos(phases)), lay(jnp.sin(phases))


def shards(echoes, triplet, bin_taper, phases, excluded, guard_len, train_len):
    core, dop = core_and_dop()
    place = places(triplet)
    other = swap(excluded)
    near, far = pack(echoes)
    far, other = lax.optimization_barrier((far, other))
    far = swap(far)
    mine = lax.dynamic_slice_in_dim(lanes(excluded, other), core * 16, 16, 0)
    m1 = lax.ppermute(mine, "dop", flipped(1))
    m2 = lax.ppermute(rows(mine, m1), "dop", flipped(2))
    part = gram(False, place, near, far, [mine, m1])
    part = gram(True, place, near, far, [m2, part])
    part = lax.all_to_all(part, BOTH, 0, 0, tiled=True, axis_index_groups=SAME_CORE)
    sr, si = steering(bin_taper, phases)
    guard = jnp.broadcast_to(guard_len[:, None], (32, GATES))
    train = jnp.broadcast_to(train_len[:, None], (32, GATES))
    sr, si, guard, train = lax.optimization_barrier((sr, si, guard, train))
    w = solve(part, sr, si)
    w = lax.all_to_all(w, BOTH, 0, 0, tiled=True, axis_index_groups=SAME_CORE)
    own, away = power(place, near, far, w)
    came = swap(away)
    pieces = [jnp.stack([own[k], came[k]]) for k in range(ZN)]
    pieces = [pieces[0]] + [lax.ppermute(pieces[k], "dop", flipped(k)) for k in (1, 2, 3)]
    p0, p1, p2, p3 = pieces
    ranges = lax.axis_size("range")
    tail = jnp.where(dop == 0, p3, jnp.where(dop == 1, p2, jnp.where(dop == 2, p1, p0)))
    head = jnp.where(dop == 0, p0, jnp.where(dop == 1, p1, jnp.where(dop == 2, p2, p3)))
    inner = swap(jnp.where(core == 0, tail, head))
    pairs = [(i, i + 1 if i % 2 else i - 1) for i in range(1, ranges - 1)]
    outer = lax.ppermute(jnp.where(core == 0, head, tail), "range", pairs)
    return cfar(noise(pieces, inner, guard, train), outer, guard, train)


def solution(mesh):
    placed = (
        P(None, None, None, ("range", "dop")),
        P(),
        P(),
        P(),
        P("dop", "range"),
        P("dop"),
        P("dop"),
    )
    return jax.shard_map(
        shards, mesh=mesh, in_specs=placed, out_specs=P("dop", "range"), check_vma=False
    )
```

```python
import functools
import jax
import jax.numpy as jnp
from jax import lax
from jax.experimental import pallas as pl
from jax.experimental.pallas import tpu as pltpu
from jax.sharding import PartitionSpec as P

CH = 16
SLOTS = 3
ST = 48
BINS = 128
BLOCK = 16
GATES = 128
TOTAL = 16384
EPS = 1e-6
HALF = 64
XN = 4
YN = 4
ZN = 4
WINDOW = 20
PACKED = ST * ST
UNROLL = 4
f32 = jnp.float32
bf16 = jnp.bfloat16
VMEM_LIMIT = 16 * 2**20

VM = pl.BlockSpec(memory_space=pltpu.VMEM)
SM = pl.BlockSpec(memory_space=pltpu.SMEM)


def core_and_dop():
    return lax.axis_index("range") % 2, lax.axis_index("dop")


def iota(shape, dim):
    return lax.broadcasted_iota(jnp.int32, shape, dim)


def split(x):
    hi = x.astype(bf16)
    return hi, (x - hi.astype(f32)).astype(bf16)


def lanes(*parts):
    return jnp.concatenate(parts, 1)


def rows(*parts):
    return jnp.concatenate(parts, 0)


def pack_kernel(echo, near, send, sems):
    core, _ = core_and_dop()
    copies = []
    for out, half in ((near, core), (send, 1 - core)):
        for z in range(ZN):
            first = z * 32 + half * 16
            for start, at, count in (
                (first, 2, 16),
                ((first + BINS - 2) % BINS, 0, 2),
                ((first + 16) % BINS, 18, 2),
            ):
                copies.append(
                    pltpu.make_async_copy(
                        echo.at[:, pl.ds(start, count)],
                        out.at[:, pl.ds(z * WINDOW + at, count)],
                        sems.at[len(copies)],
                    )
                )
    for c in copies:
        c.start()
    for c in copies:
        c.wait()


def pack(echo):
    return pl.pallas_call(
        pack_kernel,
        out_shape=[jax.ShapeDtypeStruct((2, ZN * WINDOW, CH, GATES), f32)] * 2,
        in_specs=[pl.BlockSpec(memory_space=pltpu.HBM)],
        out_specs=[VM] * 2,
        scratch_shapes=[pltpu.SemaphoreType.DMA((6 * ZN,))],
        name="pack",
        compiler_params=pltpu.CompilerParams(vmem_limit_bytes=52 * 2**20),
    )(echo)


def places(triplet):
    core, _ = core_and_dop()
    mine = lax.dynamic_index_in_dim(triplet.reshape(ZN, 2, 16, SLOTS), core, 1, keepdims=False)
    group = iota((ZN, 16, SLOTS), 0)
    where = group * WINDOW + ((mine - (group * 32 + core * 16) + BINS + 2) & (BINS - 1))
    return where.reshape(ZN * 16 * SLOTS)


def gram_kernel(second, place, near, far, *refs):
    masks = refs[: 1 if second else 2]
    if second:
        done, whole, kept, out, sems = refs[1:]
    else:
        out, kept = refs[2:]
    core, dop = core_and_dop()
    block = dop * (GATES // BLOCK) + (iota((64, 2 * GATES), 1) % GATES) // BLOCK
    block = block + 32 * (iota((64, 2 * GATES), 1) // GATES)
    pick = (iota((64, 2 * GATES), 0) == block).astype(f32)
    left = 1.0 - jnp.dot(rows(*[m[...] for m in masks]).astype(f32), pick, preferred_element_type=f32)
    for k in range(2):
        kept[k] = left[16 * k : 16 * k + 16]
    zero = jnp.zeros((16, 4 * GATES), bf16)
    base = 2 if second else 0

    def operands(k, i):
        z = dop ^ (base + k)
        m = kept[k, pl.ds(i, 1), :]
        mn = jnp.broadcast_to(m[:, :GATES], (CH, GATES)).astype(bf16)
        mf = jnp.broadcast_to(m[:, GATES:], (CH, GATES)).astype(bf16)
        hi, lo, left, right, rest, last = [], [], [], [], [], []
        for t in range(SLOTS):
            s = place[(z * 16 + i) * SLOTS + t]
            un, uf, vn, vf = split(near[0, s]), split(far[0, s]), split(near[1, s]), split(far[1, s])
            hi.append(lanes(un[0], uf[0], vn[0], vf[0]))
            lo.append(lanes(un[1], uf[1], vn[1], vf[1]))
            a, c, d, e = un[0] * mn, uf[0] * mf, vn[0] * mn, vf[0] * mf
            left.append(lanes(a, c, d, e))
            right.append(lanes(d, e, -a, -c))
            a, c, d, e = un[1] * mn, uf[1] * mf, vn[1] * mn, vf[1] * mf
            rest.append(lanes(a, c, d, e))
            last.append(lanes(d, e, -a, -c))
        return hi, lo, rows(*left, *right, *rest, *last)

    row = iota((ST, GATES), 0)
    lane = iota((ST, GATES), 1)
    low = row >= lane % HALF
    high = row <= lane % HALF
    first = lane < HALF
    lane16 = iota((CH, GATES), 1)
    mine8 = iota((8, GATES), 1) // 16 == iota((8, GATES), 0)

    def store(k, i, p):
        q = k * 16 + i
        p0, p1 = p[:16], pltpu.roll(p[16:32], 48, 1)
        p2 = pltpu.roll(p[32:], 96, 1)
        tail = [pltpu.roll(p2[h : h + 8], 0, 1, stride=16, stride_axis=0) for h in (0, 8)]
        main = jnp.where(lane16 < 48, p0, jnp.where(lane16 < 96, p1, p2))
        for j in range(16):
            out[q, :, j * GATES : (j + 1) * GATES] = main[j : j + 1]
        for j in range(2):
            extra = jnp.sum(jnp.where(mine8, tail[j], 0.0), 0, keepdims=True)
            out[q, :, (16 + j) * GATES : (17 + j) * GATES] = extra

    def pair(k, i):
        ha, wa, la = operands(k, i)
        hb, wb, lb = operands(k, i + 1)
        rhs = rows(*ha, zero, *hb, zero, *wa, zero, *wb, zero)
        dims = (((1,), (1,)), ((), ()))
        g = lax.dot_general(rows(la, lb), rhs, dims, preferred_element_type=f32)
        ga, gb = g[:192], g[192:]
        ga = ga[:96] + ga[96:]
        gb = gb[:96] + gb[96:]
        ga = ga[:, :GATES] + ga[:, GATES:]
        gb = gb[:, :GATES] + gb[:, GATES:]
        re = jnp.where(first, ga[:ST], gb[:ST])
        im = jnp.where(first, ga[ST:], gb[ST:])
        p = jnp.where(low, re, im)
        store(k, i, p)
        store(k, i + 1, pltpu.roll(p, HALF, 1))

    copies = []

    def ship(value, k):
        first = pl.multiple_of((dop ^ k) * 16, 16)
        copies.append(
            pltpu.make_async_copy(
                value.at[pl.ds((k % 2) * 16, 16)], whole.at[pl.ds(first, 16)], sems.at[k]
            )
        )
        copies[-1].start()

    if second:
        ship(done, 0)
        ship(done, 1)
    for k in range(2):
        for i in range(0, 16, 2):
            pair(k, i)
        if second:
            ship(out, 2 + k)
    for c in copies:
        c.wait()


def gram(second, place, near, far, extra):
    block = (32, 1, PACKED)
    kept = pltpu.VMEM((2, 16, 2 * GATES), f32)
    return pl.pallas_call(
        functools.partial(gram_kernel, second),
        out_shape=pltpu.HBM((64, 1, PACKED), f32) if second else jax.ShapeDtypeStruct(block, f32),
        in_specs=[SM] + [VM] * 4,
        out_specs=pl.BlockSpec(memory_space=pltpu.HBM) if second else VM,
        scratch_shapes=[kept, pltpu.VMEM(block, f32), pltpu.SemaphoreType.DMA((4,))] if second else [kept],
        name="gram_b" if second else "gram_a",
        compiler_params=pltpu.CompilerParams(vmem_limit_bytes=VMEM_LIMIT),
    )(place, near, far, *extra)


def plus(a, b):
    return a[0] + b[0], a[1] + b[1]


def minus(a, b):
    return a[0] - b[0], a[1] - b[1]


def times(a, b):
    return a[0] * b[0] - a[1] * b[1], a[0] * b[1] + a[1] * b[0]


def inner(a, b):
    return a[0] * b[0] + a[1] * b[1], a[0] * b[1] - a[1] * b[0]


def half_inverse(a, d, b):
    inv = 1.0 / (a * d - (b[0] * b[0] + b[1] * b[1]))
    a, d, b = a * inv, d * inv, (b[0] * inv, b[1] * inv)

    def apply(u, v):
        bv, bu = times(b, v), inner(b, u)
        return (d * u[0] - bv[0], d * u[1] - bv[1]), (a * v[0] - bu[0], a * v[1] - bu[1])

    return apply


def solve_kernel(parts, sr, si, out):
    row = iota((ST, GATES), 0)
    lane = iota((ST, GATES), 1)
    line = []
    for j in range(PACKED // GATES):
        line.append(jnp.sum(parts[:, 0, j * GATES : (j + 1) * GATES], 0, keepdims=True) * (1.0 / TOTAL))
    main = rows(*line[:16])
    corner = rows(*[pltpu.roll(line[16 + j // 8], (GATES + 32 - 16 * (j % 8)) % GATES, 1) for j in range(16)])
    p2 = jnp.where(lane[:16] < 32, pltpu.roll(main, 32, 1), corner)
    p = rows(main, pltpu.roll(main, GATES - 48, 1), p2)
    full = rows(p, jnp.zeros((GATES - ST, GATES), f32)).T[:ST]
    re = jnp.where(row >= lane, p, full)
    im = jnp.where(row < lane, p, jnp.where(row == lane, 0.0, -full))
    are = jnp.where(lane < ST, re, sr[...])
    aim = jnp.where(lane < ST, im, si[...])
    for k in range(0, ST, 4):
        cols = []
        for j in range(4):
            at = jnp.full((ST, GATES), k + j, jnp.int32)
            cols.append((jnp.take_along_axis(are, at, 1), jnp.take_along_axis(aim, at, 1)))
        piv = [[(c[0][k + i : k + i + 1], c[1][k + i : k + i + 1]) for c in cols] for i in range(4)]
        r = [(are[k + i : k + i + 1], aim[k + i : k + i + 1]) for i in range(4)]
        first = half_inverse(piv[0][0][0], piv[1][1][0], piv[0][1])
        x = first(r[0], r[1])
        y2 = first(piv[0][2], piv[1][2])
        y3 = first(piv[0][3], piv[1][3])
        t2 = minus(piv[2][2], plus(inner(piv[0][2], y2[0]), inner(piv[1][2], y2[1])))
        t3 = minus(piv[3][3], plus(inner(piv[0][3], y3[0]), inner(piv[1][3], y3[1])))
        t23 = minus(piv[2][3], plus(inner(piv[0][2], y3[0]), inner(piv[1][2], y3[1])))
        r2 = minus(r[2], plus(inner(piv[0][2], x[0]), inner(piv[1][2], x[1])))
        r3 = minus(r[3], plus(inner(piv[0][3], x[0]), inner(piv[1][3], x[1])))
        n2, n3 = half_inverse(t2[0], t3[0], t23)(r2, r3)
        n0 = minus(x[0], plus(times(y2[0], n2), times(y3[0], n3)))
        n1 = minus(x[1], plus(times(y2[1], n2), times(y3[1], n3)))
        new = (n0, n1, n2, n3)
        ur, ui = times(cols[0], n0)
        for j in range(1, 4):
            ur, ui = plus((ur, ui), times(cols[j], new[j]))
        are, aim = are - ur, aim - ui
        for j in range(4):
            are = jnp.where(row == k + j, new[j][0], are)
            aim = jnp.where(row == k + j, new[j][1], aim)
    pad = jnp.zeros((GATES - ST, GATES), f32)
    wr = rows(are, pad).T[ST : ST + 1]
    wi = rows(aim, pad).T[ST : ST + 1]
    lane1 = iota((1, GATES), 1)
    w = jnp.where(lane1 < ST, wr, jnp.where(lane1 < 2 * ST, pltpu.roll(wi, ST, 1), 0.0))
    for j in range(64):
        out[j] = w


def solve(parts, sr, si):
    return pl.pallas_call(
        solve_kernel,
        out_shape=jax.ShapeDtypeStruct((64, 1, GATES), f32),
        in_specs=[VM] * 3,
        out_specs=VM,
        name="solve",
        compiler_params=pltpu.CompilerParams(vmem_limit_bytes=VMEM_LIMIT),
    )(parts, sr, si)


def power_kernel(place, near, far, w, own, other):
    core, dop = core_and_dop()
    zero = jnp.zeros((32, 2 * GATES), bf16)
    row = iota((8, GATES), 0)
    lane = iota((8, GATES), 1)

    def one(k, i):
        z = dop ^ k
        wt = jnp.broadcast_to(w[z * 16 + i], (8, GATES))
        turned = jnp.where(
            lane < ST,
            -pltpu.roll(wt, GATES - ST, 1),
            jnp.where(lane < 2 * ST, pltpu.roll(wt, ST, 1), 0.0),
        )
        wt = jnp.where(row % 2 == 0, wt, turned)
        hi = wt.astype(bf16).astype(f32)
        mid = (wt - hi).astype(bf16).astype(f32)
        lo = wt - hi - mid
        wt = jnp.where(row < 2, hi, jnp.where(row < 4, mid, jnp.where(row < 6, lo, 0.0)))
        lhs = rows(wt, jnp.zeros((8, GATES), f32)).astype(bf16)
        rhs = [[], [], []]
        for p in range(2):
            for t in range(SLOTS):
                s = place[(z * 16 + i) * SLOTS + t]
                x = lanes(near[p, s], far[p, s])
                hi, rest = split(x)
                x = x - hi.astype(f32)
                rhs[0].append(hi)
                rhs[1].append(rest)
                rhs[2].append((x - rest.astype(f32)).astype(bf16))
        rhs = [*rhs[0], zero, *rhs[1], zero, *rhs[2], zero]
        y = jnp.dot(lanes(lhs, lhs, lhs), rows(*rhs), preferred_element_type=f32)
        re = y[0:1] + y[2:3] + y[4:5]
        im = y[1:2] + y[3:4] + y[5:6]
        return re * re + im * im

    def step(j, c):
        k = j // 2
        i = (j % 2) * 8
        y = rows(*[one(k, i + n) for n in range(8)])
        at = pl.ds(pl.multiple_of(i, 8), 8)
        own[k, at, :] = y[:, :GATES]
        other[k, at, :] = y[:, GATES:]
        return c

    lax.fori_loop(0, 8, step, 0, unroll=UNROLL)


def power(place, near, far, w):
    return pl.pallas_call(
        power_kernel,
        out_shape=[jax.ShapeDtypeStruct((ZN, 16, GATES), f32)] * 2,
        in_specs=[SM] + [VM] * 3,
        out_specs=[VM] * 2,
        name="power",
        compiler_params=pltpu.CompilerParams(vmem_limit_bytes=VMEM_LIMIT),
    )(place, near, far, w)


def window_sums(p, g, t):
    width = p.shape[1]
    total = p
    acc = jnp.where((t & 1) == 1, p, 0.0)
    for k in range(1, 7):
        total = total + pltpu.roll(total, width - (1 << (k - 1)), 1)
        acc = jnp.where((t >> k) & 1 == 1, total + pltpu.roll(acc, width - (1 << k), 1), acc)
    right = acc
    shift = g + 1
    for k in range(3):
        right = jnp.where((shift >> k) & 1 == 1, pltpu.roll(right, width - (1 << k), 1), right)
    left = acc
    shift = g + t
    for k in range(7):
        left = jnp.where((shift >> k) & 1 == 1, pltpu.roll(left, 1 << k, 1), left)
    return left, right


def noise_kernel(p0, p1, p2, p3, inner, guard, train, whole, edge, line, ready, sem):
    core, dop = core_and_dop()
    rank = lax.axis_index("range")
    for k, ref in enumerate((p0, p1, p2, p3)):
        at = 1 + (dop ^ k)
        line[at, core] = ref[0]
        line[at, 1 - core] = ref[1]
    at = 5 * (1 - core)
    line[at, 1 - core] = inner[0]
    line[at, core] = inner[1]
    line[5 * core] = jnp.zeros((2, 16, GATES), f32)
    p = lanes(*[rows(line[j, 0], line[j, 1]) for j in range(6)])
    g = guard[:, :1]
    t = train[:, :1]
    left, right = window_sums(p, g, t)
    lo, hi = GATES, GATES + 4 * GATES
    pos = rank * (4 * GATES) + iota((32, 4 * GATES), 1)
    left_count = jnp.maximum(jnp.minimum(pos - g - 1, TOTAL - 1) - jnp.maximum(pos - g - t, 0) + 1, 0)
    right_count = jnp.maximum(jnp.minimum(pos + g + t, TOTAL - 1) - jnp.maximum(pos + g + 1, 0) + 1, 0)
    sums = left[:, lo:hi] + right[:, lo:hi]
    count = (left_count + right_count).astype(f32)
    p = p[:, lo:hi]
    ready[...] = p / (sums / count + EPS)
    copy = pltpu.make_async_copy(ready, whole, sem)
    copy.start()
    for j, value in enumerate((p, sums, count)):
        edge[j] = jnp.where(core == 0, value[:, :GATES], value[:, 3 * GATES :])
    copy.wait()


def noise(pieces, inner, guard, train):
    return pl.pallas_call(
        noise_kernel,
        out_shape=[
            pltpu.HBM((32, 4 * GATES), f32),
            jax.ShapeDtypeStruct((3, 32, GATES), f32),
        ],
        in_specs=[VM] * 7,
        out_specs=[pl.BlockSpec(memory_space=pltpu.HBM), VM],
        scratch_shapes=[
            pltpu.VMEM((6, 2, 16, GATES), f32),
            pltpu.VMEM((32, 4 * GATES), f32),
            pltpu.SemaphoreType.DMA,
        ],
        name="noise",
        compiler_params=pltpu.CompilerParams(vmem_limit_bytes=VMEM_LIMIT),
    )(*pieces, inner, guard, train)


def cfar_kernel(whole, edge, outer, guard, train, out, line, ready, sem):
    core, _ = core_and_dop()
    line[core, 1 - core] = outer[0]
    line[core, core] = outer[1]
    line[1 - core] = jnp.zeros((2, 16, GATES), f32)
    p = lanes(*[rows(line[j, 0], line[j, 1]) for j in range(2)])
    left, right = window_sums(p, guard[:, :1], train[:, :1])
    sums = edge[1] + jnp.where(core == 0, left[:, GATES:], right[:, :GATES])
    ready[...] = edge[0] / (sums / edge[2] + EPS)
    at = pl.multiple_of(core * (3 * GATES), GATES)
    copy = pltpu.make_async_copy(ready, out.at[:, pl.ds(at, GATES)], sem)
    copy.start()
    copy.wait()


def cfar(known, outer, guard, train):
    hbm = pl.BlockSpec(memory_space=pltpu.HBM)
    return pl.pallas_call(
        cfar_kernel,
        out_shape=pltpu.HBM((32, 4 * GATES), f32),
        in_specs=[hbm] + [VM] * 4,
        out_specs=hbm,
        scratch_shapes=[
            pltpu.VMEM((2, 2, 16, GATES), f32),
            pltpu.VMEM((32, GATES), f32),
            pltpu.SemaphoreType.DMA,
        ],
        input_output_aliases={0: 0},
        name="cfar",
        compiler_params=pltpu.CompilerParams(vmem_limit_bytes=VMEM_LIMIT),
    )(*known, outer, guard, train)


BOTH = ("range", "dop")
CORE_SWAP = [(i, i ^ 1) for i in range(32)]
SAME_CORE = [
    [((y * XN + x) * 2 + c) * ZN + z for z in range(ZN) for y in range(YN) for x in range(XN)]
    for c in range(2)
]


def flipped(bit):
    return [(i, i ^ bit) for i in range(ZN)]


def swap(value):
    return lax.ppermute(value, "range", CORE_SWAP)


def steering(bin_taper, phases):
    core, dop = core_and_dop()
    b = dop * 32 + core * 16 + lax.axis_index("range") // 2
    taper = lax.dynamic_index_in_dim(bin_taper, b, 0, keepdims=False)

    def lay(values):
        return jnp.broadcast_to((taper[:, None] * values[None, :]).reshape(ST, 1), (ST, GATES))

    return lay(jnp.cos(phases)), lay(jnp.sin(phases))


def shards(echoes, triplet, bin_taper, phases, excluded, guard_len, train_len):
    core, dop = core_and_dop()
    place = places(triplet)
    other = swap(excluded)
    near, far = pack(echoes)
    far, other = lax.optimization_barrier((far, other))
    far = swap(far)
    mine = lax.dynamic_slice_in_dim(lanes(excluded, other), core * 16, 16, 0)
    m1 = lax.ppermute(mine, "dop", flipped(1))
    m2 = lax.ppermute(rows(mine, m1), "dop", flipped(2))
    part = gram(False, place, near, far, [mine, m1])
    part = gram(True, place, near, far, [m2, part])
    part = lax.all_to_all(part, BOTH, 0, 0, tiled=True, axis_index_groups=SAME_CORE)
    sr, si = steering(bin_taper, phases)
    guard = jnp.broadcast_to(guard_len[:, None], (32, GATES))
    train = jnp.broadcast_to(train_len[:, None], (32, GATES))
    sr, si, guard, train = lax.optimization_barrier((sr, si, guard, train))
    w = solve(part, sr, si)
    w = lax.all_to_all(w, BOTH, 0, 0, tiled=True, axis_index_groups=SAME_CORE)
    own, away = power(place, near, far, w)
    came = swap(away)
    pieces = [jnp.stack([own[k], came[k]]) for k in range(ZN)]
    pieces = [pieces[0]] + [lax.ppermute(pieces[k], "dop", flipped(k)) for k in (1, 2, 3)]
    p0, p1, p2, p3 = pieces
    ranges = lax.axis_size("range")
    tail = jnp.where(dop == 0, p3, jnp.where(dop == 1, p2, jnp.where(dop == 2, p1, p0)))
    head = jnp.where(dop == 0, p0, jnp.where(dop == 1, p1, jnp.where(dop == 2, p2, p3)))
    inner = swap(jnp.where(core == 0, tail, head))
    pairs = [(i, i + 1 if i % 2 else i - 1) for i in range(1, ranges - 1)]
    outer = lax.ppermute(jnp.where(core == 0, head, tail), "range", pairs)
    return cfar(noise(pieces, inner, guard, train), outer, guard, train)


def solution(mesh):
    placed = (
        P(None, None, None, ("range", "dop")),
        P(),
        P(),
        P(),
        P("dop", "range"),
        P("dop"),
        P("dop"),
    )
    return jax.shard_map(
        shards, mesh=mesh, in_specs=placed, out_specs=P("dop", "range"), check_vma=False
    )
```

```python
import functools
import jax
import jax.numpy as jnp
from jax import lax
from jax.experimental import pallas as pl
from jax.experimental.pallas import tpu as pltpu
from jax.sharding import PartitionSpec as P

CH = 16
SLOTS = 3
ST = 48
BINS = 128
BLOCK = 16
GATES = 128
TOTAL = 16384
EPS = 1e-6
HALF = 64
XN = 4
YN = 4
ZN = 4
WINDOW = 20
PACKED = ST * ST
UNROLL = 4
f32 = jnp.float32
bf16 = jnp.bfloat16
VMEM_LIMIT = 16 * 2**20

VM = pl.BlockSpec(memory_space=pltpu.VMEM)
SM = pl.BlockSpec(memory_space=pltpu.SMEM)


def core_and_dop():
    return lax.axis_index("range") % 2, lax.axis_index("dop")


def iota(shape, dim):
    return lax.broadcasted_iota(jnp.int32, shape, dim)


def split(x):
    hi = x.astype(bf16)
    return hi, (x - hi.astype(f32)).astype(bf16)


def lanes(*parts):
    return jnp.concatenate(parts, 1)


def rows(*parts):
    return jnp.concatenate(parts, 0)


def pack_kernel(echo, near, send, sems):
    core, _ = core_and_dop()
    copies = []
    for out, half in ((near, core), (send, 1 - core)):
        for z in range(ZN):
            first = z * 32 + half * 16
            for start, at, count in (
                (first, 2, 16),
                ((first + BINS - 2) % BINS, 0, 2),
                ((first + 16) % BINS, 18, 2),
            ):
                copies.append(
                    pltpu.make_async_copy(
                        echo.at[:, pl.ds(start, count)],
                        out.at[:, pl.ds(z * WINDOW + at, count)],
                        sems.at[len(copies)],
                    )
                )
    for c in copies:
        c.start()
    for c in copies:
        c.wait()


def pack(echo):
    return pl.pallas_call(
        pack_kernel,
        out_shape=[jax.ShapeDtypeStruct((2, ZN * WINDOW, CH, GATES), f32)] * 2,
        in_specs=[pl.BlockSpec(memory_space=pltpu.HBM)],
        out_specs=[VM] * 2,
        scratch_shapes=[pltpu.SemaphoreType.DMA((6 * ZN,))],
        name="pack",
        compiler_params=pltpu.CompilerParams(vmem_limit_bytes=52 * 2**20),
    )(echo)


def places(triplet):
    core, _ = core_and_dop()
    mine = lax.dynamic_index_in_dim(triplet.reshape(ZN, 2, 16, SLOTS), core, 1, keepdims=False)
    group = iota((ZN, 16, SLOTS), 0)
    where = group * WINDOW + ((mine - (group * 32 + core * 16) + BINS + 2) & (BINS - 1))
    return where.reshape(ZN * 16 * SLOTS)


def gram_kernel(second, place, near, far, *refs):
    masks = refs[: 1 if second else 2]
    if second:
        done, whole, kept, out, sems = refs[1:]
    else:
        out, kept = refs[2:]
    core, dop = core_and_dop()
    block = dop * (GATES // BLOCK) + (iota((64, 2 * GATES), 1) % GATES) // BLOCK
    block = block + 32 * (iota((64, 2 * GATES), 1) // GATES)
    pick = (iota((64, 2 * GATES), 0) == block).astype(f32)
    left = 1.0 - jnp.dot(rows(*[m[...] for m in masks]).astype(f32), pick, preferred_element_type=f32)
    for k in range(2):
        kept[k] = left[16 * k : 16 * k + 16]
    zero = jnp.zeros((16, 4 * GATES), bf16)
    base = 2 if second else 0

    def operands(k, i):
        z = dop ^ (base + k)
        m = kept[k, pl.ds(i, 1), :]
        mn = jnp.broadcast_to(m[:, :GATES], (CH, GATES)).astype(bf16)
        mf = jnp.broadcast_to(m[:, GATES:], (CH, GATES)).astype(bf16)
        hi, lo, left, right, rest, last = [], [], [], [], [], []
        for t in range(SLOTS):
            s = place[(z * 16 + i) * SLOTS + t]
            un, uf, vn, vf = split(near[0, s]), split(far[0, s]), split(near[1, s]), split(far[1, s])
            hi.append(lanes(un[0], uf[0], vn[0], vf[0]))
            lo.append(lanes(un[1], uf[1], vn[1], vf[1]))
            a, c, d, e = un[0] * mn, uf[0] * mf, vn[0] * mn, vf[0] * mf
            left.append(lanes(a, c, d, e))
            right.append(lanes(d, e, -a, -c))
            a, c, d, e = un[1] * mn, uf[1] * mf, vn[1] * mn, vf[1] * mf
            rest.append(lanes(a, c, d, e))
            last.append(lanes(d, e, -a, -c))
        return hi, lo, rows(*left, *right, *rest, *last)

    row = iota((ST, GATES), 0)
    lane = iota((ST, GATES), 1)
    low = row >= lane % HALF
    high = row <= lane % HALF
    first = lane < HALF
    lane16 = iota((CH, GATES), 1)
    mine8 = iota((8, GATES), 1) // 16 == iota((8, GATES), 0)

    def store(k, i, p):
        q = k * 16 + i
        p0, p1 = p[:16], pltpu.roll(p[16:32], 48, 1)
        p2 = pltpu.roll(p[32:], 96, 1)
        tail = [pltpu.roll(p2[h : h + 8], 0, 1, stride=16, stride_axis=0) for h in (0, 8)]
        main = jnp.where(lane16 < 48, p0, jnp.where(lane16 < 96, p1, p2))
        for j in range(16):
            out[q, :, j * GATES : (j + 1) * GATES] = main[j : j + 1]
        for j in range(2):
            extra = jnp.sum(jnp.where(mine8, tail[j], 0.0), 0, keepdims=True)
            out[q, :, (16 + j) * GATES : (17 + j) * GATES] = extra

    def pair(k, i):
        ha, wa, la = operands(k, i)
        hb, wb, lb = operands(k, i + 1)
        rhs = rows(*ha, zero, *hb, zero, *wa, zero, *wb, zero)
        dims = (((1,), (1,)), ((), ()))
        g = lax.dot_general(rows(la, lb), rhs, dims, preferred_element_type=f32)
        ga, gb = g[:192], g[192:]
        ga = ga[:96] + ga[96:]
        gb = gb[:96] + gb[96:]
        ga = ga[:, :GATES] + ga[:, GATES:]
        gb = gb[:, :GATES] + gb[:, GATES:]
        re = jnp.where(first, ga[:ST], gb[:ST])
        im = jnp.where(first, ga[ST:], gb[ST:])
        p = jnp.where(low, re, im)
        store(k, i, p)
        store(k, i + 1, pltpu.roll(p, HALF, 1))

    copies = []

    def ship(value, k):
        first = pl.multiple_of((dop ^ k) * 16, 16)
        copies.append(
            pltpu.make_async_copy(
                value.at[pl.ds((k % 2) * 16, 16)], whole.at[pl.ds(first, 16)], sems.at[k]
            )
        )
        copies[-1].start()

    if second:
        ship(done, 0)
        ship(done, 1)
    for k in range(2):
        for i in range(0, 16, 2):
            pair(k, i)
        if second:
            ship(out, 2 + k)
    for c in copies:
        c.wait()


def gram(second, place, near, far, extra):
    block = (32, 1, PACKED)
    kept = pltpu.VMEM((2, 16, 2 * GATES), f32)
    return pl.pallas_call(
        functools.partial(gram_kernel, second),
        out_shape=pltpu.HBM((64, 1, PACKED), f32) if second else jax.ShapeDtypeStruct(block, f32),
        in_specs=[SM] + [VM] * 4,
        out_specs=pl.BlockSpec(memory_space=pltpu.HBM) if second else VM,
        scratch_shapes=[kept, pltpu.VMEM(block, f32), pltpu.SemaphoreType.DMA((4,))] if second else [kept],
        name="gram_b" if second else "gram_a",
        compiler_params=pltpu.CompilerParams(vmem_limit_bytes=VMEM_LIMIT),
    )(place, near, far, *extra)


def plus(a, b):
    return a[0] + b[0], a[1] + b[1]


def minus(a, b):
    return a[0] - b[0], a[1] - b[1]


def times(a, b):
    return a[0] * b[0] - a[1] * b[1], a[0] * b[1] + a[1] * b[0]


def inner(a, b):
    return a[0] * b[0] + a[1] * b[1], a[0] * b[1] - a[1] * b[0]


def half_inverse(a, d, b):
    inv = 1.0 / (a * d - (b[0] * b[0] + b[1] * b[1]))
    a, d, b = a * inv, d * inv, (b[0] * inv, b[1] * inv)

    def apply(u, v):
        bv, bu = times(b, v), inner(b, u)
        return (d * u[0] - bv[0], d * u[1] - bv[1]), (a * v[0] - bu[0], a * v[1] - bu[1])

    return apply


def solve_kernel(parts, sr, si, out):
    row = iota((ST, GATES), 0)
    lane = iota((ST, GATES), 1)
    line = []
    for j in range(PACKED // GATES):
        line.append(jnp.sum(parts[:, 0, j * GATES : (j + 1) * GATES], 0, keepdims=True) * (1.0 / TOTAL))
    main = rows(*line[:16])
    corner = rows(*[pltpu.roll(line[16 + j // 8], (GATES + 32 - 16 * (j % 8)) % GATES, 1) for j in range(16)])
    p2 = jnp.where(lane[:16] < 32, pltpu.roll(main, 32, 1), corner)
    p = rows(main, pltpu.roll(main, GATES - 48, 1), p2)
    full = rows(p, jnp.zeros((GATES - ST, GATES), f32)).T[:ST]
    re = jnp.where(row >= lane, p, full)
    im = jnp.where(row < lane, p, jnp.where(row == lane, 0.0, -full))
    are = jnp.where(lane < ST, re, sr[...])
    aim = jnp.where(lane < ST, im, si[...])
    for k in range(0, ST, 4):
        cols = []
        for j in range(4):
            at = jnp.full((ST, GATES), k + j, jnp.int32)
            cols.append((jnp.take_along_axis(are, at, 1), jnp.take_along_axis(aim, at, 1)))
        piv = [[(c[0][k + i : k + i + 1], c[1][k + i : k + i + 1]) for c in cols] for i in range(4)]
        r = [(are[k + i : k + i + 1], aim[k + i : k + i + 1]) for i in range(4)]
        first = half_inverse(piv[0][0][0], piv[1][1][0], piv[0][1])
        x = first(r[0], r[1])
        y2 = first(piv[0][2], piv[1][2])
        y3 = first(piv[0][3], piv[1][3])
        t2 = minus(piv[2][2], plus(inner(piv[0][2], y2[0]), inner(piv[1][2], y2[1])))
        t3 = minus(piv[3][3], plus(inner(piv[0][3], y3[0]), inner(piv[1][3], y3[1])))
        t23 = minus(piv[2][3], plus(inner(piv[0][2], y3[0]), inner(piv[1][2], y3[1])))
        r2 = minus(r[2], plus(inner(piv[0][2], x[0]), inner(piv[1][2], x[1])))
        r3 = minus(r[3], plus(inner(piv[0][3], x[0]), inner(piv[1][3], x[1])))
        n2, n3 = half_inverse(t2[0], t3[0], t23)(r2, r3)
        n0 = minus(x[0], plus(times(y2[0], n2), times(y3[0], n3)))
        n1 = minus(x[1], plus(times(y2[1], n2), times(y3[1], n3)))
        new = (n0, n1, n2, n3)
        ur, ui = times(cols[0], n0)
        for j in range(1, 4):
            ur, ui = plus((ur, ui), times(cols[j], new[j]))
        are, aim = are - ur, aim - ui
        for j in range(4):
            are = jnp.where(row == k + j, new[j][0], are)
            aim = jnp.where(row == k + j, new[j][1], aim)
    pad = jnp.zeros((GATES - ST, GATES), f32)
    wr = rows(are, pad).T[ST : ST + 1]
    wi = rows(aim, pad).T[ST : ST + 1]
    lane1 = iota((1, GATES), 1)
    w = jnp.where(lane1 < ST, wr, jnp.where(lane1 < 2 * ST, pltpu.roll(wi, ST, 1), 0.0))
    for j in range(64):
        out[j] = w


def solve(parts, sr, si):
    return pl.pallas_call(
        solve_kernel,
        out_shape=jax.ShapeDtypeStruct((64, 1, GATES), f32),
        in_specs=[VM] * 3,
        out_specs=VM,
        name="solve",
        compiler_params=pltpu.CompilerParams(vmem_limit_bytes=VMEM_LIMIT),
    )(parts, sr, si)


def power_kernel(place, near, far, w, own, other):
    core, dop = core_and_dop()
    zero = jnp.zeros((32, 2 * GATES), bf16)
    row = iota((8, GATES), 0)
    lane = iota((8, GATES), 1)

    def one(k, i):
        z = dop ^ k
        wt = jnp.broadcast_to(w[z * 16 + i], (8, GATES))
        turned = jnp.where(
            lane < ST,
            -pltpu.roll(wt, GATES - ST, 1),
            jnp.where(lane < 2 * ST, pltpu.roll(wt, ST, 1), 0.0),
        )
        wt = jnp.where(row % 2 == 0, wt, turned)
        hi = wt.astype(bf16).astype(f32)
        mid = (wt - hi).astype(bf16).astype(f32)
        lo = wt - hi - mid
        wt = jnp.where(row < 2, hi, jnp.where(row < 4, mid, jnp.where(row < 6, lo, 0.0)))
        lhs = rows(wt, jnp.zeros((8, GATES), f32)).astype(bf16)
        rhs = [[], [], []]
        for p in range(2):
            for t in range(SLOTS):
                s = place[(z * 16 + i) * SLOTS + t]
                x = lanes(near[p, s], far[p, s])
                hi, rest = split(x)
                x = x - hi.astype(f32)
                rhs[0].append(hi)
                rhs[1].append(rest)
                rhs[2].append((x - rest.astype(f32)).astype(bf16))
        rhs = [*rhs[0], zero, *rhs[1], zero, *rhs[2], zero]
        y = jnp.dot(lanes(lhs, lhs, lhs), rows(*rhs), preferred_element_type=f32)
        re = y[0:1] + y[2:3] + y[4:5]
        im = y[1:2] + y[3:4] + y[5:6]
        return re * re + im * im

    def step(j, c):
        k = j // 2
        i = (j % 2) * 8
        y = rows(*[one(k, i + n) for n in range(8)])
        at = pl.ds(pl.multiple_of(i, 8), 8)
        own[k, at, :] = y[:, :GATES]
        other[k, at, :] = y[:, GATES:]
        return c

    lax.fori_loop(0, 8, step, 0, unroll=UNROLL)


def power(place, near, far, w):
    return pl.pallas_call(
        power_kernel,
        out_shape=[jax.ShapeDtypeStruct((ZN, 16, GATES), f32)] * 2,
        in_specs=[SM] + [VM] * 3,
        out_specs=[VM] * 2,
        name="power",
        compiler_params=pltpu.CompilerParams(vmem_limit_bytes=VMEM_LIMIT),
    )(place, near, far, w)


def window_sums(p, g, t, left_tiles, right_tiles):
    width = p.shape[1]
    total = p
    acc = None
    for bit in (0, 2, 4):
        k = 1 << bit
        digit = (t >> bit) & 3
        shifted = [total] + [pltpu.roll(total, width - j * k, 1) for j in (1, 2, 3)]
        two = shifted[0] + shifted[1]
        three = two + shifted[2]
        part = jnp.where(digit == 1, total, jnp.where(digit == 2, two, three))
        if acc is None:
            acc = jnp.where(digit == 0, 0.0, part)
        else:
            moved = [pltpu.roll(acc, width - j * k, 1) for j in (1, 2, 3)]
            moved = jnp.where(digit == 1, moved[0], jnp.where(digit == 2, moved[1], moved[2]))
            acc = jnp.where(digit == 0, acc, part + moved)
        total = two + (shifted[2] + shifted[3])
    acc = jnp.where(t == 64, total, acc)
    tiles = [acc[:, j : j + GATES] for j in range(0, width, GATES)]
    lane = iota(tiles[0].shape, 1)

    def taken(j, other, shift, inside):
        at = (lane + shift) & (GATES - 1)
        here = jnp.take_along_axis(tiles[j], at, 1)
        return jnp.where(inside, here, jnp.take_along_axis(tiles[other], at, 1))

    back, ahead = -(g + t), g + 1
    left = [taken(j, j - 1, back, lane + back >= 0) for j in left_tiles]
    right = [taken(j, j + 1, ahead, lane + ahead < GATES) for j in right_tiles]
    return left, right


def noise_kernel(p0, p1, p2, p3, inner, guard, train, whole, edge, line, ready, sem):
    core, dop = core_and_dop()
    rank = lax.axis_index("range")
    for k, ref in enumerate((p0, p1, p2, p3)):
        at = 1 + (dop ^ k)
        line[at, core] = ref[0]
        line[at, 1 - core] = ref[1]
    at = 5 * (1 - core)
    line[at, 1 - core] = inner[0]
    line[at, core] = inner[1]
    line[5 * core] = jnp.zeros((2, 16, GATES), f32)
    p = lanes(*[rows(line[j, 0], line[j, 1]) for j in range(6)])
    g = guard[:, :1]
    t = train[:, :1]
    left, right = window_sums(p, g, t, (1, 2, 3, 4), (1, 2, 3, 4))
    lo, hi = GATES, GATES + 4 * GATES
    pos = rank * (4 * GATES) + iota((32, 4 * GATES), 1)
    left_count = jnp.maximum(jnp.minimum(pos - g - 1, TOTAL - 1) - jnp.maximum(pos - g - t, 0) + 1, 0)
    right_count = jnp.maximum(jnp.minimum(pos + g + t, TOTAL - 1) - jnp.maximum(pos + g + 1, 0) + 1, 0)
    sums = lanes(*left) + lanes(*right)
    count = (left_count + right_count).astype(f32)
    p = p[:, lo:hi]
    ready[...] = p / (sums / count + EPS)
    copy = pltpu.make_async_copy(ready, whole, sem)
    copy.start()
    for j, value in enumerate((p, sums, count)):
        edge[j] = jnp.where(core == 0, value[:, :GATES], value[:, 3 * GATES :])
    copy.wait()


def noise(pieces, inner, guard, train):
    return pl.pallas_call(
        noise_kernel,
        out_shape=[
            pltpu.HBM((32, 4 * GATES), f32),
            jax.ShapeDtypeStruct((3, 32, GATES), f32),
        ],
        in_specs=[VM] * 7,
        out_specs=[pl.BlockSpec(memory_space=pltpu.HBM), VM],
        scratch_shapes=[
            pltpu.VMEM((6, 2, 16, GATES), f32),
            pltpu.VMEM((32, 4 * GATES), f32),
            pltpu.SemaphoreType.DMA,
        ],
        name="noise",
        compiler_params=pltpu.CompilerParams(vmem_limit_bytes=VMEM_LIMIT),
    )(*pieces, inner, guard, train)


def cfar_kernel(whole, edge, outer, guard, train, out, line, ready, sem):
    core, _ = core_and_dop()
    line[core, 1 - core] = outer[0]
    line[core, core] = outer[1]
    line[1 - core] = jnp.zeros((2, 16, GATES), f32)
    p = lanes(*[rows(line[j, 0], line[j, 1]) for j in range(2)])
    left, right = window_sums(p, guard[:, :1], train[:, :1], (1,), (0,))
    sums = edge[1] + jnp.where(core == 0, left[0], right[0])
    ready[...] = edge[0] / (sums / edge[2] + EPS)
    at = pl.multiple_of(core * (3 * GATES), GATES)
    copy = pltpu.make_async_copy(ready, out.at[:, pl.ds(at, GATES)], sem)
    copy.start()
    copy.wait()


def cfar(known, outer, guard, train):
    hbm = pl.BlockSpec(memory_space=pltpu.HBM)
    return pl.pallas_call(
        cfar_kernel,
        out_shape=pltpu.HBM((32, 4 * GATES), f32),
        in_specs=[hbm] + [VM] * 4,
        out_specs=hbm,
        scratch_shapes=[
            pltpu.VMEM((2, 2, 16, GATES), f32),
            pltpu.VMEM((32, GATES), f32),
            pltpu.SemaphoreType.DMA,
        ],
        input_output_aliases={0: 0},
        name="cfar",
        compiler_params=pltpu.CompilerParams(vmem_limit_bytes=VMEM_LIMIT),
    )(*known, outer, guard, train)


BOTH = ("range", "dop")
CORE_SWAP = [(i, i ^ 1) for i in range(32)]
SAME_CORE = [
    [((y * XN + x) * 2 + c) * ZN + z for z in range(ZN) for y in range(YN) for x in range(XN)]
    for c in range(2)
]


def flipped(bit):
    return [(i, i ^ bit) for i in range(ZN)]


def swap(value):
    return lax.ppermute(value, "range", CORE_SWAP)


def steering(bin_taper, phases):
    core, dop = core_and_dop()
    b = dop * 32 + core * 16 + lax.axis_index("range") // 2
    taper = lax.dynamic_index_in_dim(bin_taper, b, 0, keepdims=False)

    def lay(values):
        return jnp.broadcast_to((taper[:, None] * values[None, :]).reshape(ST, 1), (ST, GATES))

    return lay(jnp.cos(phases)), lay(jnp.sin(phases))


def shards(echoes, triplet, bin_taper, phases, excluded, guard_len, train_len):
    core, dop = core_and_dop()
    place = places(triplet)
    other = swap(excluded)
    near, far = pack(echoes)
    far, other = lax.optimization_barrier((far, other))
    far = swap(far)
    mine = lax.dynamic_slice_in_dim(lanes(excluded, other), core * 16, 16, 0)
    m1 = lax.ppermute(mine, "dop", flipped(1))
    m2 = lax.ppermute(rows(mine, m1), "dop", flipped(2))
    part = gram(False, place, near, far, [mine, m1])
    part = gram(True, place, near, far, [m2, part])
    part = lax.all_to_all(part, BOTH, 0, 0, tiled=True, axis_index_groups=SAME_CORE)
    sr, si = steering(bin_taper, phases)
    guard = jnp.broadcast_to(guard_len[:, None], (32, GATES))
    train = jnp.broadcast_to(train_len[:, None], (32, GATES))
    sr, si, guard, train = lax.optimization_barrier((sr, si, guard, train))
    w = solve(part, sr, si)
    w = lax.all_to_all(w, BOTH, 0, 0, tiled=True, axis_index_groups=SAME_CORE)
    own, away = power(place, near, far, w)
    came = swap(away)
    pieces = [jnp.stack([own[k], came[k]]) for k in range(ZN)]
    pieces = [pieces[0]] + [lax.ppermute(pieces[k], "dop", flipped(k)) for k in (1, 2, 3)]
    p0, p1, p2, p3 = pieces
    ranges = lax.axis_size("range")
    tail = jnp.where(dop == 0, p3, jnp.where(dop == 1, p2, jnp.where(dop == 2, p1, p0)))
    head = jnp.where(dop == 0, p0, jnp.where(dop == 1, p1, jnp.where(dop == 2, p2, p3)))
    inner = swap(jnp.where(core == 0, tail, head))
    pairs = [(i, i + 1 if i % 2 else i - 1) for i in range(1, ranges - 1)]
    outer = lax.ppermute(jnp.where(core == 0, head, tail), "range", pairs)
    return cfar(noise(pieces, inner, guard, train), outer, guard, train)


def solution(mesh):
    placed = (
        P(None, None, None, ("range", "dop")),
        P(),
        P(),
        P(),
        P("dop", "range"),
        P("dop"),
        P("dop"),
    )
    return jax.shard_map(
        shards, mesh=mesh, in_specs=placed, out_specs=P("dop", "range"), check_vma=False
    )
```

```python
import functools
import jax
import jax.numpy as jnp
from jax import lax
from jax.experimental import pallas as pl
from jax.experimental.pallas import tpu as pltpu
from jax.sharding import PartitionSpec as P

CH = 16
SLOTS = 3
ST = 48
BINS = 128
BLOCK = 16
GATES = 128
TOTAL = 16384
EPS = 1e-6
HALF = 64
XN = 4
YN = 4
ZN = 4
WINDOW = 20
PACKED = ST * ST
UNROLL = 8
f32 = jnp.float32
bf16 = jnp.bfloat16
VMEM_LIMIT = 16 * 2**20

VM = pl.BlockSpec(memory_space=pltpu.VMEM)
SM = pl.BlockSpec(memory_space=pltpu.SMEM)


def core_and_dop():
    return lax.axis_index("range") % 2, lax.axis_index("dop")


def iota(shape, dim):
    return lax.broadcasted_iota(jnp.int32, shape, dim)


def split(x):
    hi = x.astype(bf16)
    return hi, (x - hi.astype(f32)).astype(bf16)


def lanes(*parts):
    return jnp.concatenate(parts, 1)


def rows(*parts):
    return jnp.concatenate(parts, 0)


def pack_kernel(echo, near, send, sems):
    core, _ = core_and_dop()
    copies = []
    for out, half in ((near, core), (send, 1 - core)):
        for z in range(ZN):
            first = z * 32 + half * 16
            for start, at, count in (
                (first, 2, 16),
                ((first + BINS - 2) % BINS, 0, 2),
                ((first + 16) % BINS, 18, 2),
            ):
                copies.append(
                    pltpu.make_async_copy(
                        echo.at[:, pl.ds(start, count)],
                        out.at[:, pl.ds(z * WINDOW + at, count)],
                        sems.at[len(copies)],
                    )
                )
    for c in copies:
        c.start()
    for c in copies:
        c.wait()


def pack(echo):
    return pl.pallas_call(
        pack_kernel,
        out_shape=[jax.ShapeDtypeStruct((2, ZN * WINDOW, CH, GATES), f32)] * 2,
        in_specs=[pl.BlockSpec(memory_space=pltpu.HBM)],
        out_specs=[VM] * 2,
        scratch_shapes=[pltpu.SemaphoreType.DMA((6 * ZN,))],
        name="pack",
        compiler_params=pltpu.CompilerParams(vmem_limit_bytes=52 * 2**20),
    )(echo)


def places(triplet):
    core, _ = core_and_dop()
    mine = lax.dynamic_index_in_dim(triplet.reshape(ZN, 2, 16, SLOTS), core, 1, keepdims=False)
    group = iota((ZN, 16, SLOTS), 0)
    where = group * WINDOW + ((mine - (group * 32 + core * 16) + BINS + 2) & (BINS - 1))
    return where.reshape(ZN * 16 * SLOTS)


def gram_kernel(second, place, near, far, *refs):
    masks = refs[: 1 if second else 2]
    if second:
        done, whole, kept, out, sems = refs[1:]
    else:
        out, kept = refs[2:]
    core, dop = core_and_dop()
    block = dop * (GATES // BLOCK) + (iota((64, 2 * GATES), 1) % GATES) // BLOCK
    block = block + 32 * (iota((64, 2 * GATES), 1) // GATES)
    pick = (iota((64, 2 * GATES), 0) == block).astype(f32)
    left = 1.0 - jnp.dot(rows(*[m[...] for m in masks]).astype(f32), pick, preferred_element_type=f32)
    for k in range(2):
        kept[k] = left[16 * k : 16 * k + 16]
    zero = jnp.zeros((16, 4 * GATES), bf16)
    base = 2 if second else 0

    def operands(k, i):
        z = dop ^ (base + k)
        m = kept[k, pl.ds(i, 1), :]
        mn = jnp.broadcast_to(m[:, :GATES], (CH, GATES)).astype(bf16)
        mf = jnp.broadcast_to(m[:, GATES:], (CH, GATES)).astype(bf16)
        hi, lo, left, right, rest, last = [], [], [], [], [], []
        for t in range(SLOTS):
            s = place[(z * 16 + i) * SLOTS + t]
            un, uf, vn, vf = split(near[0, s]), split(far[0, s]), split(near[1, s]), split(far[1, s])
            hi.append(lanes(un[0], uf[0], vn[0], vf[0]))
            lo.append(lanes(un[1], uf[1], vn[1], vf[1]))
            a, c, d, e = un[0] * mn, uf[0] * mf, vn[0] * mn, vf[0] * mf
            left.append(lanes(a, c, d, e))
            right.append(lanes(d, e, -a, -c))
            a, c, d, e = un[1] * mn, uf[1] * mf, vn[1] * mn, vf[1] * mf
            rest.append(lanes(a, c, d, e))
            last.append(lanes(d, e, -a, -c))
        return hi, lo, rows(*left, *right, *rest, *last)

    row = iota((ST, GATES), 0)
    lane = iota((ST, GATES), 1)
    low = row >= lane % HALF
    high = row <= lane % HALF
    first = lane < HALF
    lane16 = iota((CH, GATES), 1)
    mine8 = iota((8, GATES), 1) // 16 == iota((8, GATES), 0)

    def store(k, i, p):
        q = k * 16 + i
        p0, p1 = p[:16], pltpu.roll(p[16:32], 48, 1)
        p2 = pltpu.roll(p[32:], 96, 1)
        tail = [pltpu.roll(p2[h : h + 8], 0, 1, stride=16, stride_axis=0) for h in (0, 8)]
        main = jnp.where(lane16 < 48, p0, jnp.where(lane16 < 96, p1, p2))
        for j in range(16):
            out[q, :, j * GATES : (j + 1) * GATES] = main[j : j + 1]
        for j in range(2):
            extra = jnp.sum(jnp.where(mine8, tail[j], 0.0), 0, keepdims=True)
            out[q, :, (16 + j) * GATES : (17 + j) * GATES] = extra

    def pair(k, i):
        ha, wa, la = operands(k, i)
        hb, wb, lb = operands(k, i + 1)
        rhs = rows(*ha, zero, *hb, zero, *wa, zero, *wb, zero)
        dims = (((1,), (1,)), ((), ()))
        g = lax.dot_general(rows(la, lb), rhs, dims, preferred_element_type=f32)
        ga, gb = g[:192], g[192:]
        ga = ga[:96] + ga[96:]
        gb = gb[:96] + gb[96:]
        ga = ga[:, :GATES] + ga[:, GATES:]
        gb = gb[:, :GATES] + gb[:, GATES:]
        re = jnp.where(first, ga[:ST], gb[:ST])
        im = jnp.where(first, ga[ST:], gb[ST:])
        p = jnp.where(low, re, im)
        store(k, i, p)
        store(k, i + 1, pltpu.roll(p, HALF, 1))

    copies = []

    def ship(value, k):
        first = pl.multiple_of((dop ^ k) * 16, 16)
        copies.append(
            pltpu.make_async_copy(
                value.at[pl.ds((k % 2) * 16, 16)], whole.at[pl.ds(first, 16)], sems.at[k]
            )
        )
        copies[-1].start()

    if second:
        ship(done, 0)
        ship(done, 1)
    for k in range(2):
        for i in range(0, 16, 2):
            pair(k, i)
        if second:
            ship(out, 2 + k)
    for c in copies:
        c.wait()


def gram(second, place, near, far, extra):
    block = (32, 1, PACKED)
    kept = pltpu.VMEM((2, 16, 2 * GATES), f32)
    return pl.pallas_call(
        functools.partial(gram_kernel, second),
        out_shape=pltpu.HBM((64, 1, PACKED), f32) if second else jax.ShapeDtypeStruct(block, f32),
        in_specs=[SM] + [VM] * 4,
        out_specs=pl.BlockSpec(memory_space=pltpu.HBM) if second else VM,
        scratch_shapes=[kept, pltpu.VMEM(block, f32), pltpu.SemaphoreType.DMA((4,))] if second else [kept],
        name="gram_b" if second else "gram_a",
        compiler_params=pltpu.CompilerParams(vmem_limit_bytes=VMEM_LIMIT),
    )(place, near, far, *extra)


def plus(a, b):
    return a[0] + b[0], a[1] + b[1]


def minus(a, b):
    return a[0] - b[0], a[1] - b[1]


def times(a, b):
    return a[0] * b[0] - a[1] * b[1], a[0] * b[1] + a[1] * b[0]


def inner(a, b):
    return a[0] * b[0] + a[1] * b[1], a[0] * b[1] - a[1] * b[0]


def half_inverse(a, d, b):
    inv = 1.0 / (a * d - (b[0] * b[0] + b[1] * b[1]))
    a, d, b = a * inv, d * inv, (b[0] * inv, b[1] * inv)

    def apply(u, v):
        bv, bu = times(b, v), inner(b, u)
        return (d * u[0] - bv[0], d * u[1] - bv[1]), (a * v[0] - bu[0], a * v[1] - bu[1])

    return apply


def solve_kernel(parts, sr, si, out):
    row = iota((ST, GATES), 0)
    lane = iota((ST, GATES), 1)
    line = []
    for j in range(PACKED // GATES):
        line.append(jnp.sum(parts[:, 0, j * GATES : (j + 1) * GATES], 0, keepdims=True) * (1.0 / TOTAL))
    main = rows(*line[:16])
    corner = rows(*[pltpu.roll(line[16 + j // 8], (GATES + 32 - 16 * (j % 8)) % GATES, 1) for j in range(16)])
    p2 = jnp.where(lane[:16] < 32, pltpu.roll(main, 32, 1), corner)
    p = rows(main, pltpu.roll(main, GATES - 48, 1), p2)
    full = rows(p, jnp.zeros((GATES - ST, GATES), f32)).T[:ST]
    re = jnp.where(row >= lane, p, full)
    im = jnp.where(row < lane, p, jnp.where(row == lane, 0.0, -full))
    are = jnp.where(lane < ST, re, sr[...])
    aim = jnp.where(lane < ST, im, si[...])
    for k in range(0, ST, 4):
        cols = []
        for j in range(4):
            at = jnp.full((ST, GATES), k + j, jnp.int32)
            cols.append((jnp.take_along_axis(are, at, 1), jnp.take_along_axis(aim, at, 1)))
        piv = [[(c[0][k + i : k + i + 1], c[1][k + i : k + i + 1]) for c in cols] for i in range(4)]
        r = [(are[k + i : k + i + 1], aim[k + i : k + i + 1]) for i in range(4)]
        first = half_inverse(piv[0][0][0], piv[1][1][0], piv[0][1])
        x = first(r[0], r[1])
        y2 = first(piv[0][2], piv[1][2])
        y3 = first(piv[0][3], piv[1][3])
        t2 = minus(piv[2][2], plus(inner(piv[0][2], y2[0]), inner(piv[1][2], y2[1])))
        t3 = minus(piv[3][3], plus(inner(piv[0][3], y3[0]), inner(piv[1][3], y3[1])))
        t23 = minus(piv[2][3], plus(inner(piv[0][2], y3[0]), inner(piv[1][2], y3[1])))
        r2 = minus(r[2], plus(inner(piv[0][2], x[0]), inner(piv[1][2], x[1])))
        r3 = minus(r[3], plus(inner(piv[0][3], x[0]), inner(piv[1][3], x[1])))
        n2, n3 = half_inverse(t2[0], t3[0], t23)(r2, r3)
        n0 = minus(x[0], plus(times(y2[0], n2), times(y3[0], n3)))
        n1 = minus(x[1], plus(times(y2[1], n2), times(y3[1], n3)))
        new = (n0, n1, n2, n3)
        ur, ui = times(cols[0], n0)
        for j in range(1, 4):
            ur, ui = plus((ur, ui), times(cols[j], new[j]))
        are, aim = are - ur, aim - ui
        for j in range(4):
            are = jnp.where(row == k + j, new[j][0], are)
            aim = jnp.where(row == k + j, new[j][1], aim)
    pad = jnp.zeros((GATES - ST, GATES), f32)
    wr = rows(are, pad).T[ST : ST + 1]
    wi = rows(aim, pad).T[ST : ST + 1]
    lane1 = iota((1, GATES), 1)
    w = jnp.where(lane1 < ST, wr, jnp.where(lane1 < 2 * ST, pltpu.roll(wi, ST, 1), 0.0))
    for j in range(64):
        out[j] = w


def solve(parts, sr, si):
    return pl.pallas_call(
        solve_kernel,
        out_shape=jax.ShapeDtypeStruct((64, 1, GATES), f32),
        in_specs=[VM] * 3,
        out_specs=VM,
        name="solve",
        compiler_params=pltpu.CompilerParams(vmem_limit_bytes=VMEM_LIMIT),
    )(parts, sr, si)


def power_kernel(place, near, far, w, out):
    core, dop = core_and_dop()
    zero = jnp.zeros((32, 2 * GATES), bf16)
    row = iota((8, GATES), 0)
    lane = iota((8, GATES), 1)

    def one(k, i):
        z = dop ^ k
        wt = jnp.broadcast_to(w[z * 16 + i], (8, GATES))
        turned = jnp.where(
            lane < ST,
            -pltpu.roll(wt, GATES - ST, 1),
            jnp.where(lane < 2 * ST, pltpu.roll(wt, ST, 1), 0.0),
        )
        wt = jnp.where(row % 2 == 0, wt, turned)
        hi = wt.astype(bf16).astype(f32)
        mid = (wt - hi).astype(bf16).astype(f32)
        lo = wt - hi - mid
        wt = jnp.where(row < 2, hi, jnp.where(row < 4, mid, jnp.where(row < 6, lo, 0.0)))
        lhs = rows(wt, jnp.zeros((8, GATES), f32)).astype(bf16)
        rhs = [[], [], []]
        for p in range(2):
            for t in range(SLOTS):
                s = place[(z * 16 + i) * SLOTS + t]
                x = lanes(near[p, s], far[p, s])
                hi, rest = split(x)
                x = x - hi.astype(f32)
                rhs[0].append(hi)
                rhs[1].append(rest)
                rhs[2].append((x - rest.astype(f32)).astype(bf16))
        rhs = [*rhs[0], zero, *rhs[1], zero, *rhs[2], zero]
        y = jnp.dot(lanes(lhs, lhs, lhs), rows(*rhs), preferred_element_type=f32)
        re = y[0:1] + y[2:3] + y[4:5]
        im = y[1:2] + y[3:4] + y[5:6]
        return re * re + im * im

    def step(j, c):
        k = j // 2
        i = (j % 2) * 8
        y = rows(*[one(k, i + n) for n in range(8)])
        at = pl.ds(pl.multiple_of(i, 8), 8)
        out[k, 0, at, :] = y[:, :GATES]
        out[k, 1, at, :] = y[:, GATES:]
        return c

    lax.fori_loop(0, 8, step, 0, unroll=UNROLL)


def power(place, near, far, w):
    return pl.pallas_call(
        power_kernel,
        out_shape=jax.ShapeDtypeStruct((ZN, 2, 16, GATES), f32),
        in_specs=[SM] + [VM] * 3,
        out_specs=VM,
        name="power",
        compiler_params=pltpu.CompilerParams(vmem_limit_bytes=VMEM_LIMIT),
    )(place, near, far, w)


def window_sums(p, g, t, left_tiles, right_tiles):
    width = p.shape[1]
    total = p
    acc = None
    for bit in (0, 2, 4):
        k = 1 << bit
        digit = (t >> bit) & 3
        shifted = [total] + [pltpu.roll(total, width - j * k, 1) for j in (1, 2, 3)]
        two = shifted[0] + shifted[1]
        three = two + shifted[2]
        part = jnp.where(digit == 1, total, jnp.where(digit == 2, two, three))
        if acc is None:
            acc = jnp.where(digit == 0, 0.0, part)
        else:
            moved = [pltpu.roll(acc, width - j * k, 1) for j in (1, 2, 3)]
            moved = jnp.where(digit == 1, moved[0], jnp.where(digit == 2, moved[1], moved[2]))
            acc = jnp.where(digit == 0, acc, part + moved)
        total = two + (shifted[2] + shifted[3])
    acc = jnp.where(t == 64, total, acc)
    tiles = [acc[:, j : j + GATES] for j in range(0, width, GATES)]
    lane = iota(tiles[0].shape, 1)

    def taken(j, other, shift, inside):
        at = (lane + shift) & (GATES - 1)
        here = jnp.take_along_axis(tiles[j], at, 1)
        return jnp.where(inside, here, jnp.take_along_axis(tiles[other], at, 1))

    back, ahead = -(g + t), g + 1
    left = [taken(j, j - 1, back, lane + back >= 0) for j in left_tiles]
    right = [taken(j, j + 1, ahead, lane + ahead < GATES) for j in right_tiles]
    return left, right


def noise_kernel(p0, p1, p2, p3, guard, train, whole, edge, line, ready, sem):
    core, dop = core_and_dop()
    rank = lax.axis_index("range")
    for k, ref in enumerate((p0, p1, p2, p3)):
        at = 1 + (dop ^ k)
        line[at, core] = ref[0]
        line[at, 1 - core] = ref[1]
    source = dop ^ (3 * core)
    for slot, half in ((2, core), (3, 1 - core)):
        value = p0[slot]
        for k, ref in ((1, p1), (2, p2), (3, p3)):
            value = jnp.where(source == k, ref[slot], value)
        line[5 * (1 - core), half] = value
    line[5 * core] = jnp.zeros((2, 16, GATES), f32)
    p = lanes(*[rows(line[j, 0], line[j, 1]) for j in range(6)])
    g = guard[:, :1]
    t = train[:, :1]
    left, right = window_sums(p, g, t, (1, 2, 3, 4), (1, 2, 3, 4))
    lo, hi = GATES, GATES + 4 * GATES
    pos = rank * (4 * GATES) + iota((32, 4 * GATES), 1)
    left_count = jnp.maximum(jnp.minimum(pos - g - 1, TOTAL - 1) - jnp.maximum(pos - g - t, 0) + 1, 0)
    right_count = jnp.maximum(jnp.minimum(pos + g + t, TOTAL - 1) - jnp.maximum(pos + g + 1, 0) + 1, 0)
    sums = lanes(*left) + lanes(*right)
    count = (left_count + right_count).astype(f32)
    p = p[:, lo:hi]
    ready[...] = p / (sums / count + EPS)
    copy = pltpu.make_async_copy(ready, whole, sem)
    copy.start()
    for j, value in enumerate((p, sums, count)):
        edge[j] = jnp.where(core == 0, value[:, :GATES], value[:, 3 * GATES :])
    copy.wait()


def noise(pieces, guard, train):
    return pl.pallas_call(
        noise_kernel,
        out_shape=[
            pltpu.HBM((32, 4 * GATES), f32),
            jax.ShapeDtypeStruct((3, 32, GATES), f32),
        ],
        in_specs=[VM] * 6,
        out_specs=[pl.BlockSpec(memory_space=pltpu.HBM), VM],
        scratch_shapes=[
            pltpu.VMEM((6, 2, 16, GATES), f32),
            pltpu.VMEM((32, 4 * GATES), f32),
            pltpu.SemaphoreType.DMA,
        ],
        name="noise",
        compiler_params=pltpu.CompilerParams(vmem_limit_bytes=VMEM_LIMIT),
    )(*pieces, guard, train)


def cfar_kernel(whole, edge, outer, guard, train, out, line, ready, sem):
    core, _ = core_and_dop()
    line[core, 1 - core] = outer[0]
    line[core, core] = outer[1]
    line[1 - core] = jnp.zeros((2, 16, GATES), f32)
    p = lanes(*[rows(line[j, 0], line[j, 1]) for j in range(2)])
    left, right = window_sums(p, guard[:, :1], train[:, :1], (1,), (0,))
    sums = edge[1] + jnp.where(core == 0, left[0], right[0])
    ready[...] = edge[0] / (sums / edge[2] + EPS)
    at = pl.multiple_of(core * (3 * GATES), GATES)
    copy = pltpu.make_async_copy(ready, out.at[:, pl.ds(at, GATES)], sem)
    copy.start()
    copy.wait()


def cfar(known, outer, guard, train):
    hbm = pl.BlockSpec(memory_space=pltpu.HBM)
    return pl.pallas_call(
        cfar_kernel,
        out_shape=pltpu.HBM((32, 4 * GATES), f32),
        in_specs=[hbm] + [VM] * 4,
        out_specs=hbm,
        scratch_shapes=[
            pltpu.VMEM((2, 2, 16, GATES), f32),
            pltpu.VMEM((32, GATES), f32),
            pltpu.SemaphoreType.DMA,
        ],
        input_output_aliases={0: 0},
        name="cfar",
        compiler_params=pltpu.CompilerParams(vmem_limit_bytes=VMEM_LIMIT),
    )(*known, outer, guard, train)


BOTH = ("range", "dop")
CORE_SWAP = [(i, i ^ 1) for i in range(32)]
SAME_CORE = [
    [((y * XN + x) * 2 + c) * ZN + z for z in range(ZN) for y in range(YN) for x in range(XN)]
    for c in range(2)
]


def flipped(bit):
    return [(i, i ^ bit) for i in range(ZN)]


def swap(value):
    return lax.ppermute(value, "range", CORE_SWAP)


def steering(bin_taper, phases):
    core, dop = core_and_dop()
    b = dop * 32 + core * 16 + lax.axis_index("range") // 2
    taper = lax.dynamic_index_in_dim(bin_taper, b, 0, keepdims=False)

    def lay(values):
        return jnp.broadcast_to((taper[:, None] * values[None, :]).reshape(ST, 1), (ST, GATES))

    return lay(jnp.cos(phases)), lay(jnp.sin(phases))


def shards(echoes, triplet, bin_taper, phases, excluded, guard_len, train_len):
    core, dop = core_and_dop()
    place = places(triplet)
    other = swap(excluded)
    near, far = pack(echoes)
    far, other = lax.optimization_barrier((far, other))
    far = swap(far)
    mine = lax.dynamic_slice_in_dim(lanes(excluded, other), core * 16, 16, 0)
    m1 = lax.ppermute(mine, "dop", flipped(1))
    m2 = lax.ppermute(rows(mine, m1), "dop", flipped(2))
    part = gram(False, place, near, far, [mine, m1])
    part = gram(True, place, near, far, [m2, part])
    part = lax.all_to_all(part, BOTH, 0, 0, tiled=True, axis_index_groups=SAME_CORE)
    sr, si = steering(bin_taper, phases)
    guard = jnp.broadcast_to(guard_len[:, None], (32, GATES))
    train = jnp.broadcast_to(train_len[:, None], (32, GATES))
    sr, si, guard, train = lax.optimization_barrier((sr, si, guard, train))
    w = solve(part, sr, si)
    w = lax.all_to_all(w, BOTH, 0, 0, tiled=True, axis_index_groups=SAME_CORE)
    mine = power(place, near, far, w)
    came = swap(mine)
    pieces = [jnp.stack([mine[k, 0], came[k, 1], mine[k, 1], came[k, 0]]) for k in range(ZN)]
    pieces = [pieces[0]] + [lax.ppermute(pieces[k], "dop", flipped(k)) for k in (1, 2, 3)]
    ranges = lax.axis_size("range")
    p0, p1, p2, p3 = [p[:2] for p in pieces]
    tail = jnp.where(dop == 0, p3, jnp.where(dop == 1, p2, jnp.where(dop == 2, p1, p0)))
    head = jnp.where(dop == 0, p0, jnp.where(dop == 1, p1, jnp.where(dop == 2, p2, p3)))
    pairs = [(i, i + 1 if i % 2 else i - 1) for i in range(1, ranges - 1)]
    outer = lax.ppermute(jnp.where(core == 0, head, tail), "range", pairs)
    return cfar(noise(pieces, guard, train), outer, guard, train)


def solution(mesh):
    placed = (
        P(None, None, None, ("range", "dop")),
        P(),
        P(),
        P(),
        P("dop", "range"),
        P("dop"),
        P("dop"),
    )
    return jax.shard_map(
        shards, mesh=mesh, in_specs=placed, out_specs=P("dop", "range"), check_vma=False
    )
```

```python
import functools
import jax
import jax.numpy as jnp
from jax import lax
from jax.experimental import pallas as pl
from jax.experimental.pallas import tpu as pltpu
from jax.sharding import PartitionSpec as P

CH = 16
SLOTS = 3
ST = 48
BINS = 128
BLOCK = 16
GATES = 128
TOTAL = 16384
EPS = 1e-6
HALF = 64
XN = 4
YN = 4
ZN = 4
WINDOW = 20
PACKED = ST * ST
UNROLL = 8
f32 = jnp.float32
bf16 = jnp.bfloat16
VMEM_LIMIT = 16 * 2**20

VM = pl.BlockSpec(memory_space=pltpu.VMEM)
SM = pl.BlockSpec(memory_space=pltpu.SMEM)


def core_and_dop():
    return lax.axis_index("range") % 2, lax.axis_index("dop")


def iota(shape, dim):
    return lax.broadcasted_iota(jnp.int32, shape, dim)


def split(x):
    hi = x.astype(bf16)
    return hi, (x - hi.astype(f32)).astype(bf16)


def lanes(*parts):
    return jnp.concatenate(parts, 1)


def rows(*parts):
    return jnp.concatenate(parts, 0)


def pack_kernel(echo, near, send, stage, sems):
    core, _ = core_and_dop()
    loads = []
    for out, half in ((stage, 1 - core), (near, core)):
        for z in range(ZN):
            first = z * 32 + half * 16
            for start, at, count in (
                (first, 2, 16),
                ((first + BINS - 2) % BINS, 0, 2),
                ((first + 16) % BINS, 18, 2),
            ):
                loads.append(
                    pltpu.make_async_copy(
                        echo.at[:, pl.ds(start, count)],
                        out.at[:, pl.ds(z * WINDOW + at, count)],
                        sems.at[len(loads)],
                    )
                )
    for c in loads:
        c.start()
    stores = []
    for z in range(ZN):
        for c in loads[3 * z : 3 * z + 3]:
            c.wait()
        part = pl.ds(z * WINDOW, WINDOW)
        stores.append(
            pltpu.make_async_copy(stage.at[:, part], send.at[:, part], sems.at[6 * ZN + z])
        )
        stores[-1].start()
    for c in loads[3 * ZN :] + stores:
        c.wait()


def pack(echo):
    packed = (2, ZN * WINDOW, CH, GATES)
    return pl.pallas_call(
        pack_kernel,
        out_shape=[jax.ShapeDtypeStruct(packed, f32), pltpu.HBM(packed, f32)],
        in_specs=[pl.BlockSpec(memory_space=pltpu.HBM)],
        out_specs=[VM, pl.BlockSpec(memory_space=pltpu.HBM)],
        scratch_shapes=[pltpu.VMEM(packed, f32), pltpu.SemaphoreType.DMA((7 * ZN,))],
        name="pack",
        compiler_params=pltpu.CompilerParams(vmem_limit_bytes=52 * 2**20),
    )(echo)


def places(triplet):
    core, _ = core_and_dop()
    mine = lax.dynamic_index_in_dim(triplet.reshape(ZN, 2, 16, SLOTS), core, 1, keepdims=False)
    group = iota((ZN, 16, SLOTS), 0)
    where = group * WINDOW + ((mine - (group * 32 + core * 16) + BINS + 2) & (BINS - 1))
    return where.reshape(ZN * 16 * SLOTS)


def gram_kernel(second, place, near, far, *refs):
    masks = refs[: 1 if second else 2]
    if second:
        done, whole, kept, out, sems = refs[1:]
    else:
        out, kept = refs[2:]
    core, dop = core_and_dop()
    block = dop * (GATES // BLOCK) + (iota((64, 2 * GATES), 1) % GATES) // BLOCK
    block = block + 32 * (iota((64, 2 * GATES), 1) // GATES)
    pick = (iota((64, 2 * GATES), 0) == block).astype(f32)
    left = 1.0 - jnp.dot(rows(*[m[...] for m in masks]).astype(f32), pick, preferred_element_type=f32)
    for k in range(2):
        kept[k] = left[16 * k : 16 * k + 16]
    zero = jnp.zeros((16, 4 * GATES), bf16)
    base = 2 if second else 0

    def operands(k, i):
        z = dop ^ (base + k)
        m = kept[k, pl.ds(i, 1), :]
        mn = jnp.broadcast_to(m[:, :GATES], (CH, GATES)).astype(bf16)
        mf = jnp.broadcast_to(m[:, GATES:], (CH, GATES)).astype(bf16)
        hi, lo, left, right, rest, last = [], [], [], [], [], []
        for t in range(SLOTS):
            s = place[(z * 16 + i) * SLOTS + t]
            un, uf, vn, vf = split(near[0, s]), split(far[0, s]), split(near[1, s]), split(far[1, s])
            hi.append(lanes(un[0], uf[0], vn[0], vf[0]))
            lo.append(lanes(un[1], uf[1], vn[1], vf[1]))
            a, c, d, e = un[0] * mn, uf[0] * mf, vn[0] * mn, vf[0] * mf
            left.append(lanes(a, c, d, e))
            right.append(lanes(d, e, -a, -c))
            a, c, d, e = un[1] * mn, uf[1] * mf, vn[1] * mn, vf[1] * mf
            rest.append(lanes(a, c, d, e))
            last.append(lanes(d, e, -a, -c))
        return hi, lo, rows(*left, *right, *rest, *last)

    row = iota((ST, GATES), 0)
    lane = iota((ST, GATES), 1)
    low = row >= lane % HALF
    high = row <= lane % HALF
    first = lane < HALF
    lane16 = iota((CH, GATES), 1)
    mine8 = iota((8, GATES), 1) // 16 == iota((8, GATES), 0)

    def store(k, i, p):
        q = k * 16 + i
        p0, p1 = p[:16], pltpu.roll(p[16:32], 48, 1)
        p2 = pltpu.roll(p[32:], 96, 1)
        tail = [pltpu.roll(p2[h : h + 8], 0, 1, stride=16, stride_axis=0) for h in (0, 8)]
        main = jnp.where(lane16 < 48, p0, jnp.where(lane16 < 96, p1, p2))
        for j in range(16):
            out[q, :, j * GATES : (j + 1) * GATES] = main[j : j + 1]
        for j in range(2):
            extra = jnp.sum(jnp.where(mine8, tail[j], 0.0), 0, keepdims=True)
            out[q, :, (16 + j) * GATES : (17 + j) * GATES] = extra

    def pair(k, i):
        ha, wa, la = operands(k, i)
        hb, wb, lb = operands(k, i + 1)
        rhs = rows(*ha, zero, *hb, zero, *wa, zero, *wb, zero)
        dims = (((1,), (1,)), ((), ()))
        g = lax.dot_general(rows(la, lb), rhs, dims, preferred_element_type=f32)
        ga, gb = g[:192], g[192:]
        ga = ga[:96] + ga[96:]
        gb = gb[:96] + gb[96:]
        ga = ga[:, :GATES] + ga[:, GATES:]
        gb = gb[:, :GATES] + gb[:, GATES:]
        re = jnp.where(first, ga[:ST], gb[:ST])
        im = jnp.where(first, ga[ST:], gb[ST:])
        p = jnp.where(low, re, im)
        store(k, i, p)
        store(k, i + 1, pltpu.roll(p, HALF, 1))

    copies = []

    def ship(value, k):
        first = pl.multiple_of((dop ^ k) * 16, 16)
        copies.append(
            pltpu.make_async_copy(
                value.at[pl.ds((k % 2) * 16, 16)], whole.at[pl.ds(first, 16)], sems.at[k]
            )
        )
        copies[-1].start()

    if second:
        ship(done, 0)
        ship(done, 1)
    for k in range(2):
        for i in range(0, 16, 2):
            pair(k, i)
        if second:
            ship(out, 2 + k)
    for c in copies:
        c.wait()


def gram(second, place, near, far, extra):
    block = (32, 1, PACKED)
    kept = pltpu.VMEM((2, 16, 2 * GATES), f32)
    return pl.pallas_call(
        functools.partial(gram_kernel, second),
        out_shape=pltpu.HBM((64, 1, PACKED), f32) if second else jax.ShapeDtypeStruct(block, f32),
        in_specs=[SM] + [VM] * 4,
        out_specs=pl.BlockSpec(memory_space=pltpu.HBM) if second else VM,
        scratch_shapes=[kept, pltpu.VMEM(block, f32), pltpu.SemaphoreType.DMA((4,))] if second else [kept],
        name="gram_b" if second else "gram_a",
        compiler_params=pltpu.CompilerParams(vmem_limit_bytes=VMEM_LIMIT),
    )(place, near, far, *extra)


def plus(a, b):
    return a[0] + b[0], a[1] + b[1]


def minus(a, b):
    return a[0] - b[0], a[1] - b[1]


def times(a, b):
    return a[0] * b[0] - a[1] * b[1], a[0] * b[1] + a[1] * b[0]


def inner(a, b):
    return a[0] * b[0] + a[1] * b[1], a[0] * b[1] - a[1] * b[0]


def half_inverse(a, d, b):
    inv = 1.0 / (a * d - (b[0] * b[0] + b[1] * b[1]))
    a, d, b = a * inv, d * inv, (b[0] * inv, b[1] * inv)

    def apply(u, v):
        bv, bu = times(b, v), inner(b, u)
        return (d * u[0] - bv[0], d * u[1] - bv[1]), (a * v[0] - bu[0], a * v[1] - bu[1])

    return apply


def solve_kernel(parts, sr, si, out):
    row = iota((ST, GATES), 0)
    lane = iota((ST, GATES), 1)
    total = parts[0]
    for j in range(1, 64):
        total = total + parts[j]
    total = total * (1.0 / TOTAL)
    line = [total[:, j : j + GATES] for j in range(0, PACKED, GATES)]
    main = rows(*line[:16])
    corner = rows(*[pltpu.roll(line[16 + j // 8], (GATES + 32 - 16 * (j % 8)) % GATES, 1) for j in range(16)])
    p2 = jnp.where(lane[:16] < 32, pltpu.roll(main, 32, 1), corner)
    p = rows(main, pltpu.roll(main, GATES - 48, 1), p2)
    full = rows(p, jnp.zeros((GATES - ST, GATES), f32)).T[:ST]
    re = jnp.where(row >= lane, p, full)
    im = jnp.where(row < lane, p, jnp.where(row == lane, 0.0, -full))
    are = jnp.where(lane < ST, re, sr[...])
    aim = jnp.where(lane < ST, im, si[...])
    for k in range(0, ST, 4):
        cols = []
        for j in range(4):
            at = jnp.full((ST, GATES), k + j, jnp.int32)
            cols.append((jnp.take_along_axis(are, at, 1), jnp.take_along_axis(aim, at, 1)))
        piv = [[(c[0][k + i : k + i + 1], c[1][k + i : k + i + 1]) for c in cols] for i in range(4)]
        r = [(are[k + i : k + i + 1], aim[k + i : k + i + 1]) for i in range(4)]
        first = half_inverse(piv[0][0][0], piv[1][1][0], piv[0][1])
        x = first(r[0], r[1])
        y2 = first(piv[0][2], piv[1][2])
        y3 = first(piv[0][3], piv[1][3])
        t2 = minus(piv[2][2], plus(inner(piv[0][2], y2[0]), inner(piv[1][2], y2[1])))
        t3 = minus(piv[3][3], plus(inner(piv[0][3], y3[0]), inner(piv[1][3], y3[1])))
        t23 = minus(piv[2][3], plus(inner(piv[0][2], y3[0]), inner(piv[1][2], y3[1])))
        r2 = minus(r[2], plus(inner(piv[0][2], x[0]), inner(piv[1][2], x[1])))
        r3 = minus(r[3], plus(inner(piv[0][3], x[0]), inner(piv[1][3], x[1])))
        n2, n3 = half_inverse(t2[0], t3[0], t23)(r2, r3)
        n0 = minus(x[0], plus(times(y2[0], n2), times(y3[0], n3)))
        n1 = minus(x[1], plus(times(y2[1], n2), times(y3[1], n3)))
        new = (n0, n1, n2, n3)
        ur, ui = times(cols[0], n0)
        for j in range(1, 4):
            ur, ui = plus((ur, ui), times(cols[j], new[j]))
        are, aim = are - ur, aim - ui
        for j in range(4):
            are = jnp.where(row == k + j, new[j][0], are)
            aim = jnp.where(row == k + j, new[j][1], aim)
    pad = jnp.zeros((GATES - ST, GATES), f32)
    wr = rows(are, pad).T[ST : ST + 1]
    wi = rows(aim, pad).T[ST : ST + 1]
    lane1 = iota((1, GATES), 1)
    w = jnp.where(lane1 < ST, wr, jnp.where(lane1 < 2 * ST, pltpu.roll(wi, ST, 1), 0.0))
    for j in range(64):
        out[j] = w


def solve(parts, sr, si):
    return pl.pallas_call(
        solve_kernel,
        out_shape=jax.ShapeDtypeStruct((64, 1, GATES), f32),
        in_specs=[VM] * 3,
        out_specs=VM,
        name="solve",
        compiler_params=pltpu.CompilerParams(vmem_limit_bytes=VMEM_LIMIT),
    )(parts, sr, si)


def power_kernel(place, near, far, w, out):
    core, dop = core_and_dop()
    zero = jnp.zeros((32, 2 * GATES), bf16)
    row = iota((8, GATES), 0)
    lane = iota((8, GATES), 1)

    def one(k, i):
        z = dop ^ k
        wt = jnp.broadcast_to(w[z * 16 + i], (8, GATES))
        turned = jnp.where(
            lane < ST,
            -pltpu.roll(wt, GATES - ST, 1),
            jnp.where(lane < 2 * ST, pltpu.roll(wt, ST, 1), 0.0),
        )
        wt = jnp.where(row % 2 == 0, wt, turned)
        hi = wt.astype(bf16).astype(f32)
        mid = (wt - hi).astype(bf16).astype(f32)
        lo = wt - hi - mid
        wt = jnp.where(row < 2, hi, jnp.where(row < 4, mid, jnp.where(row < 6, lo, 0.0)))
        lhs = rows(wt, jnp.zeros((8, GATES), f32)).astype(bf16)
        rhs = [[], [], []]
        for p in range(2):
            for t in range(SLOTS):
                s = place[(z * 16 + i) * SLOTS + t]
                x = lanes(near[p, s], far[p, s])
                hi, rest = split(x)
                x = x - hi.astype(f32)
                rhs[0].append(hi)
                rhs[1].append(rest)
                rhs[2].append((x - rest.astype(f32)).astype(bf16))
        rhs = [*rhs[0], zero, *rhs[1], zero, *rhs[2], zero]
        y = jnp.dot(lanes(lhs, lhs, lhs), rows(*rhs), preferred_element_type=f32)
        re = y[0:1] + y[2:3] + y[4:5]
        im = y[1:2] + y[3:4] + y[5:6]
        return re * re + im * im

    def step(j, c):
        k = j // 2
        i = (j % 2) * 8
        y = rows(*[one(k, i + n) for n in range(8)])
        at = pl.ds(pl.multiple_of(i, 8), 8)
        out[k, 0, at, :] = y[:, :GATES]
        out[k, 1, at, :] = y[:, GATES:]
        return c

    lax.fori_loop(0, 8, step, 0, unroll=UNROLL)


def power(place, near, far, w):
    return pl.pallas_call(
        power_kernel,
        out_shape=jax.ShapeDtypeStruct((ZN, 2, 16, GATES), f32),
        in_specs=[SM] + [VM] * 3,
        out_specs=VM,
        name="power",
        compiler_params=pltpu.CompilerParams(vmem_limit_bytes=VMEM_LIMIT),
    )(place, near, far, w)


def window_sums(p, g, t, left_tiles, right_tiles):
    width = p.shape[1]
    total = p
    acc = None
    for bit in (0, 2, 4):
        k = 1 << bit
        digit = (t >> bit) & 3
        shifted = [total] + [pltpu.roll(total, width - j * k, 1) for j in (1, 2, 3)]
        two = shifted[0] + shifted[1]
        three = two + shifted[2]
        part = jnp.where(digit == 1, total, jnp.where(digit == 2, two, three))
        if acc is None:
            acc = jnp.where(digit == 0, 0.0, part)
        else:
            moved = [pltpu.roll(acc, width - j * k, 1) for j in (1, 2, 3)]
            moved = jnp.where(digit == 1, moved[0], jnp.where(digit == 2, moved[1], moved[2]))
            acc = jnp.where(digit == 0, acc, part + moved)
        total = two + (shifted[2] + shifted[3])
    acc = jnp.where(t == 64, total, acc)
    tiles = [acc[:, j : j + GATES] for j in range(0, width, GATES)]
    lane = iota(tiles[0].shape, 1)

    def taken(j, other, shift, inside):
        at = (lane + shift) & (GATES - 1)
        here = jnp.take_along_axis(tiles[j], at, 1)
        return jnp.where(inside, here, jnp.take_along_axis(tiles[other], at, 1))

    back, ahead = -(g + t), g + 1
    left = [taken(j, j - 1, back, lane + back >= 0) for j in left_tiles]
    right = [taken(j, j + 1, ahead, lane + ahead < GATES) for j in right_tiles]
    return left, right


def noise_kernel(p0, p1, p2, p3, guard, train, whole, edge, line, ready, sem):
    core, dop = core_and_dop()
    rank = lax.axis_index("range")
    for k, ref in enumerate((p0, p1, p2, p3)):
        at = 1 + (dop ^ k)
        line[at, core] = ref[0]
        line[at, 1 - core] = ref[1]
    source = dop ^ (3 * core)
    for slot, half in ((2, core), (3, 1 - core)):
        value = p0[slot]
        for k, ref in ((1, p1), (2, p2), (3, p3)):
            value = jnp.where(source == k, ref[slot], value)
        line[5 * (1 - core), half] = value
    line[5 * core] = jnp.zeros((2, 16, GATES), f32)
    p = lanes(*[rows(line[j, 0], line[j, 1]) for j in range(6)])
    g = guard[:, :1]
    t = train[:, :1]
    left, right = window_sums(p, g, t, (1, 2, 3, 4), (1, 2, 3, 4))
    lo, hi = GATES, GATES + 4 * GATES
    pos = rank * (4 * GATES) + iota((32, 4 * GATES), 1)
    left_count = jnp.maximum(jnp.minimum(pos - g - 1, TOTAL - 1) - jnp.maximum(pos - g - t, 0) + 1, 0)
    right_count = jnp.maximum(jnp.minimum(pos + g + t, TOTAL - 1) - jnp.maximum(pos + g + 1, 0) + 1, 0)
    sums = lanes(*left) + lanes(*right)
    count = (left_count + right_count).astype(f32)
    p = p[:, lo:hi]
    ready[...] = p / (sums / count + EPS)
    copy = pltpu.make_async_copy(ready, whole, sem)
    copy.start()
    for j, value in enumerate((p, sums, count)):
        edge[j] = jnp.where(core == 0, value[:, :GATES], value[:, 3 * GATES :])
    copy.wait()


def noise(pieces, guard, train):
    return pl.pallas_call(
        noise_kernel,
        out_shape=[
            pltpu.HBM((32, 4 * GATES), f32),
            jax.ShapeDtypeStruct((3, 32, GATES), f32),
        ],
        in_specs=[VM] * 6,
        out_specs=[pl.BlockSpec(memory_space=pltpu.HBM), VM],
        scratch_shapes=[
            pltpu.VMEM((6, 2, 16, GATES), f32),
            pltpu.VMEM((32, 4 * GATES), f32),
            pltpu.SemaphoreType.DMA,
        ],
        name="noise",
        compiler_params=pltpu.CompilerParams(vmem_limit_bytes=VMEM_LIMIT),
    )(*pieces, guard, train)


def cfar_kernel(whole, edge, outer, guard, train, out, line, ready, sem):
    core, _ = core_and_dop()
    line[core, 1 - core] = outer[0]
    line[core, core] = outer[1]
    line[1 - core] = jnp.zeros((2, 16, GATES), f32)
    p = lanes(*[rows(line[j, 0], line[j, 1]) for j in range(2)])
    left, right = window_sums(p, guard[:, :1], train[:, :1], (1,), (0,))
    sums = edge[1] + jnp.where(core == 0, left[0], right[0])
    ready[...] = edge[0] / (sums / edge[2] + EPS)
    at = pl.multiple_of(core * (3 * GATES), GATES)
    copy = pltpu.make_async_copy(ready, out.at[:, pl.ds(at, GATES)], sem)
    copy.start()
    copy.wait()


def cfar(known, outer, guard, train):
    hbm = pl.BlockSpec(memory_space=pltpu.HBM)
    return pl.pallas_call(
        cfar_kernel,
        out_shape=pltpu.HBM((32, 4 * GATES), f32),
        in_specs=[hbm] + [VM] * 4,
        out_specs=hbm,
        scratch_shapes=[
            pltpu.VMEM((2, 2, 16, GATES), f32),
            pltpu.VMEM((32, GATES), f32),
            pltpu.SemaphoreType.DMA,
        ],
        input_output_aliases={0: 0},
        name="cfar",
        compiler_params=pltpu.CompilerParams(vmem_limit_bytes=VMEM_LIMIT),
    )(*known, outer, guard, train)


BOTH = ("range", "dop")
CORE_SWAP = [(i, i ^ 1) for i in range(32)]
SAME_CORE = [
    [((y * XN + x) * 2 + c) * ZN + z for z in range(ZN) for y in range(YN) for x in range(XN)]
    for c in range(2)
]


def flipped(bit):
    return [(i, i ^ bit) for i in range(ZN)]


def swap(value):
    return lax.ppermute(value, "range", CORE_SWAP)


def steering(bin_taper, phases):
    core, dop = core_and_dop()
    b = dop * 32 + core * 16 + lax.axis_index("range") // 2
    taper = lax.dynamic_index_in_dim(bin_taper, b, 0, keepdims=False)

    def lay(values):
        return jnp.broadcast_to((taper[:, None] * values[None, :]).reshape(ST, 1), (ST, GATES))

    return lay(jnp.cos(phases)), lay(jnp.sin(phases))


def shards(echoes, triplet, bin_taper, phases, excluded, guard_len, train_len):
    core, dop = core_and_dop()
    place = places(triplet)
    other = swap(excluded)
    near, far = pack(echoes)
    far, other = lax.optimization_barrier((far, other))
    far = swap(far)
    mine = lax.dynamic_slice_in_dim(lanes(excluded, other), core * 16, 16, 0)
    m1 = lax.ppermute(mine, "dop", flipped(1))
    m2 = lax.ppermute(rows(mine, m1), "dop", flipped(2))
    part = gram(False, place, near, far, [mine, m1])
    part = gram(True, place, near, far, [m2, part])
    part = lax.all_to_all(part, BOTH, 0, 0, tiled=True, axis_index_groups=SAME_CORE)
    sr, si = steering(bin_taper, phases)
    guard = jnp.broadcast_to(guard_len[:, None], (32, GATES))
    train = jnp.broadcast_to(train_len[:, None], (32, GATES))
    sr, si, guard, train = lax.optimization_barrier((sr, si, guard, train))
    w = solve(part, sr, si)
    w = lax.all_to_all(w, BOTH, 0, 0, tiled=True, axis_index_groups=SAME_CORE)
    mine = power(place, near, far, w)
    came = swap(mine)
    pieces = [jnp.stack([mine[k, 0], came[k, 1], mine[k, 1], came[k, 0]]) for k in range(ZN)]
    pieces = [pieces[0]] + [lax.ppermute(pieces[k], "dop", flipped(k)) for k in (1, 2, 3)]
    ranges = lax.axis_size("range")
    p0, p1, p2, p3 = [p[:2] for p in pieces]
    tail = jnp.where(dop == 0, p3, jnp.where(dop == 1, p2, jnp.where(dop == 2, p1, p0)))
    head = jnp.where(dop == 0, p0, jnp.where(dop == 1, p1, jnp.where(dop == 2, p2, p3)))
    pairs = [(i, i + 1 if i % 2 else i - 1) for i in range(1, ranges - 1)]
    outer = lax.ppermute(jnp.where(core == 0, head, tail), "range", pairs)
    return cfar(noise(pieces, guard, train), outer, guard, train)


def solution(mesh):
    placed = (
        P(None, None, None, ("range", "dop")),
        P(),
        P(),
        P(),
        P("dop", "range"),
        P("dop"),
        P("dop"),
    )
    return jax.shard_map(
        shards, mesh=mesh, in_specs=placed, out_specs=P("dop", "range"), check_vma=False
    )
```

```python
import functools
import jax
import jax.numpy as jnp
from jax import lax
from jax.experimental import pallas as pl
from jax.experimental.pallas import tpu as pltpu
from jax.sharding import PartitionSpec as P

CH = 16
SLOTS = 3
ST = 48
BINS = 128
BLOCK = 16
GATES = 128
TOTAL = 16384
EPS = 1e-6
HALF = 64
XN = 4
YN = 4
ZN = 4
WINDOW = 20
PACKED = ST * ST
UNROLL = 8
f32 = jnp.float32
bf16 = jnp.bfloat16
VMEM_LIMIT = 16 * 2**20

VM = pl.BlockSpec(memory_space=pltpu.VMEM)
SM = pl.BlockSpec(memory_space=pltpu.SMEM)


def core_and_dop():
    return lax.axis_index("range") % 2, lax.axis_index("dop")


def iota(shape, dim):
    return lax.broadcasted_iota(jnp.int32, shape, dim)


def split(x):
    hi = x.astype(bf16)
    return hi, (x - hi.astype(f32)).astype(bf16)


def lanes(*parts):
    return jnp.concatenate(parts, 1)


def rows(*parts):
    return jnp.concatenate(parts, 0)


def pack_kernel(echo, near, send, stage, sems):
    core, _ = core_and_dop()
    loads = []
    for out, half in ((stage, 1 - core), (near, core)):
        for z in range(ZN):
            first = z * 32 + half * 16
            for start, at, count in (
                (first, 2, 16),
                ((first + BINS - 2) % BINS, 0, 2),
                ((first + 16) % BINS, 18, 2),
            ):
                loads.append(
                    pltpu.make_async_copy(
                        echo.at[:, pl.ds(start, count)],
                        out.at[:, pl.ds(z * WINDOW + at, count)],
                        sems.at[len(loads)],
                    )
                )
    for c in loads:
        c.start()
    stores = []
    for z in range(ZN):
        for c in loads[3 * z : 3 * z + 3]:
            c.wait()
        part = pl.ds(z * WINDOW, WINDOW)
        stores.append(
            pltpu.make_async_copy(stage.at[:, part], send.at[:, part], sems.at[6 * ZN + z])
        )
        stores[-1].start()
    for c in loads[3 * ZN :] + stores:
        c.wait()


def pack(echo):
    packed = (2, ZN * WINDOW, CH, GATES)
    return pl.pallas_call(
        pack_kernel,
        out_shape=[jax.ShapeDtypeStruct(packed, f32), pltpu.HBM(packed, f32)],
        in_specs=[pl.BlockSpec(memory_space=pltpu.HBM)],
        out_specs=[VM, pl.BlockSpec(memory_space=pltpu.HBM)],
        scratch_shapes=[pltpu.VMEM(packed, f32), pltpu.SemaphoreType.DMA((7 * ZN,))],
        name="pack",
        compiler_params=pltpu.CompilerParams(vmem_limit_bytes=52 * 2**20),
    )(echo)


def places(triplet):
    core, _ = core_and_dop()
    mine = lax.dynamic_index_in_dim(triplet.reshape(ZN, 2, 16, SLOTS), core, 1, keepdims=False)
    group = iota((ZN, 16, SLOTS), 0)
    where = group * WINDOW + ((mine - (group * 32 + core * 16) + BINS + 2) & (BINS - 1))
    return where.reshape(ZN * 16 * SLOTS)


def gram_kernel(second, place, near, far, *refs):
    masks = refs[:2]
    if second:
        done, whole, kept, out, sems = refs[2:]
    else:
        out, kept = refs[2:]
    core, dop = core_and_dop()
    block = dop * (GATES // BLOCK) + (iota((64, 2 * GATES), 1) % GATES) // BLOCK
    block = block + 32 * (iota((64, 2 * GATES), 1) // GATES)
    pick = (iota((64, 2 * GATES), 0) == block).astype(f32)
    left = 1.0 - jnp.dot(rows(*[m[...] for m in masks]).astype(f32), pick, preferred_element_type=f32)
    for k in range(2):
        kept[k] = left[16 * k : 16 * k + 16]
    zero = jnp.zeros((16, 4 * GATES), bf16)
    base = 2 if second else 0

    def operands(k, i):
        z = dop ^ (base + k)
        m = kept[k, pl.ds(i, 1), :]
        mn = jnp.broadcast_to(m[:, :GATES], (CH, GATES)).astype(bf16)
        mf = jnp.broadcast_to(m[:, GATES:], (CH, GATES)).astype(bf16)
        hi, lo, left, right, rest, last = [], [], [], [], [], []
        for t in range(SLOTS):
            s = place[(z * 16 + i) * SLOTS + t]
            un, uf, vn, vf = split(near[0, s]), split(far[0, s]), split(near[1, s]), split(far[1, s])
            hi.append(lanes(un[0], uf[0], vn[0], vf[0]))
            lo.append(lanes(un[1], uf[1], vn[1], vf[1]))
            a, c, d, e = un[0] * mn, uf[0] * mf, vn[0] * mn, vf[0] * mf
            left.append(lanes(a, c, d, e))
            right.append(lanes(d, e, -a, -c))
            a, c, d, e = un[1] * mn, uf[1] * mf, vn[1] * mn, vf[1] * mf
            rest.append(lanes(a, c, d, e))
            last.append(lanes(d, e, -a, -c))
        return hi, lo, rows(*left, *right, *rest, *last)

    row = iota((ST, GATES), 0)
    lane = iota((ST, GATES), 1)
    low = row >= lane % HALF
    high = row <= lane % HALF
    first = lane < HALF
    lane16 = iota((CH, GATES), 1)
    mine8 = iota((8, GATES), 1) // 16 == iota((8, GATES), 0)

    def store(k, i, p):
        q = k * 16 + i
        p0, p1 = p[:16], pltpu.roll(p[16:32], 48, 1)
        p2 = pltpu.roll(p[32:], 96, 1)
        tail = [pltpu.roll(p2[h : h + 8], 0, 1, stride=16, stride_axis=0) for h in (0, 8)]
        main = jnp.where(lane16 < 48, p0, jnp.where(lane16 < 96, p1, p2))
        for j in range(16):
            out[q, :, j * GATES : (j + 1) * GATES] = main[j : j + 1]
        for j in range(2):
            extra = jnp.sum(jnp.where(mine8, tail[j], 0.0), 0, keepdims=True)
            out[q, :, (16 + j) * GATES : (17 + j) * GATES] = extra

    def pair(k, i):
        ha, wa, la = operands(k, i)
        hb, wb, lb = operands(k, i + 1)
        rhs = rows(*ha, zero, *hb, zero, *wa, zero, *wb, zero)
        dims = (((1,), (1,)), ((), ()))
        g = lax.dot_general(rows(la, lb), rhs, dims, preferred_element_type=f32)
        ga, gb = g[:192], g[192:]
        ga = ga[:96] + ga[96:]
        gb = gb[:96] + gb[96:]
        ga = ga[:, :GATES] + ga[:, GATES:]
        gb = gb[:, :GATES] + gb[:, GATES:]
        re = jnp.where(first, ga[:ST], gb[:ST])
        im = jnp.where(first, ga[ST:], gb[ST:])
        p = jnp.where(low, re, im)
        store(k, i, p)
        store(k, i + 1, pltpu.roll(p, HALF, 1))

    copies = []

    def ship(value, k):
        first = pl.multiple_of((dop ^ k) * 16, 16)
        copies.append(
            pltpu.make_async_copy(
                value.at[pl.ds((k % 2) * 16, 16)], whole.at[pl.ds(first, 16)], sems.at[k]
            )
        )
        copies[-1].start()

    if second:
        ship(done, 0)
        ship(done, 1)
    for k in range(2):
        for i in range(0, 16, 2):
            pair(k, i)
        if second:
            ship(out, 2 + k)
    for c in copies:
        c.wait()


def gram(second, place, near, far, extra):
    block = (32, 1, PACKED)
    kept = pltpu.VMEM((2, 16, 2 * GATES), f32)
    return pl.pallas_call(
        functools.partial(gram_kernel, second),
        out_shape=pltpu.HBM((64, 1, PACKED), f32) if second else jax.ShapeDtypeStruct(block, f32),
        in_specs=[SM] + [VM] * (2 + len(extra)),
        out_specs=pl.BlockSpec(memory_space=pltpu.HBM) if second else VM,
        scratch_shapes=[kept, pltpu.VMEM(block, f32), pltpu.SemaphoreType.DMA((4,))] if second else [kept],
        name="gram_b" if second else "gram_a",
        compiler_params=pltpu.CompilerParams(vmem_limit_bytes=VMEM_LIMIT),
    )(place, near, far, *extra)


def plus(a, b):
    return a[0] + b[0], a[1] + b[1]


def minus(a, b):
    return a[0] - b[0], a[1] - b[1]


def times(a, b):
    return a[0] * b[0] - a[1] * b[1], a[0] * b[1] + a[1] * b[0]


def inner(a, b):
    return a[0] * b[0] + a[1] * b[1], a[0] * b[1] - a[1] * b[0]


def half_inverse(a, d, b):
    inv = 1.0 / (a * d - (b[0] * b[0] + b[1] * b[1]))
    a, d, b = a * inv, d * inv, (b[0] * inv, b[1] * inv)

    def apply(u, v):
        bv, bu = times(b, v), inner(b, u)
        return (d * u[0] - bv[0], d * u[1] - bv[1]), (a * v[0] - bu[0], a * v[1] - bu[1])

    return apply


def solve_kernel(parts, sr, si, out):
    row = iota((ST, GATES), 0)
    lane = iota((ST, GATES), 1)
    total = parts[0]
    for j in range(1, 64):
        total = total + parts[j]
    total = total * (1.0 / TOTAL)
    line = [total[:, j : j + GATES] for j in range(0, PACKED, GATES)]
    main = rows(*line[:16])
    corner = rows(*[pltpu.roll(line[16 + j // 8], (GATES + 32 - 16 * (j % 8)) % GATES, 1) for j in range(16)])
    p2 = jnp.where(lane[:16] < 32, pltpu.roll(main, 32, 1), corner)
    p = rows(main, pltpu.roll(main, GATES - 48, 1), p2)
    full = rows(p, jnp.zeros((GATES - ST, GATES), f32)).T[:ST]
    re = jnp.where(row >= lane, p, full)
    im = jnp.where(row < lane, p, jnp.where(row == lane, 0.0, -full))
    are = jnp.where(lane < ST, re, sr[...])
    aim = jnp.where(lane < ST, im, si[...])
    for k in range(0, ST, 4):
        cols = []
        for j in range(4):
            at = jnp.full((ST, GATES), k + j, jnp.int32)
            cols.append((jnp.take_along_axis(are, at, 1), jnp.take_along_axis(aim, at, 1)))
        piv = [[(c[0][k + i : k + i + 1], c[1][k + i : k + i + 1]) for c in cols] for i in range(4)]
        r = [(are[k + i : k + i + 1], aim[k + i : k + i + 1]) for i in range(4)]
        first = half_inverse(piv[0][0][0], piv[1][1][0], piv[0][1])
        x = first(r[0], r[1])
        y2 = first(piv[0][2], piv[1][2])
        y3 = first(piv[0][3], piv[1][3])
        t2 = minus(piv[2][2], plus(inner(piv[0][2], y2[0]), inner(piv[1][2], y2[1])))
        t3 = minus(piv[3][3], plus(inner(piv[0][3], y3[0]), inner(piv[1][3], y3[1])))
        t23 = minus(piv[2][3], plus(inner(piv[0][2], y3[0]), inner(piv[1][2], y3[1])))
        r2 = minus(r[2], plus(inner(piv[0][2], x[0]), inner(piv[1][2], x[1])))
        r3 = minus(r[3], plus(inner(piv[0][3], x[0]), inner(piv[1][3], x[1])))
        n2, n3 = half_inverse(t2[0], t3[0], t23)(r2, r3)
        n0 = minus(x[0], plus(times(y2[0], n2), times(y3[0], n3)))
        n1 = minus(x[1], plus(times(y2[1], n2), times(y3[1], n3)))
        new = (n0, n1, n2, n3)
        ur, ui = times(cols[0], n0)
        for j in range(1, 4):
            ur, ui = plus((ur, ui), times(cols[j], new[j]))
        are, aim = are - ur, aim - ui
        for j in range(4):
            are = jnp.where(row == k + j, new[j][0], are)
            aim = jnp.where(row == k + j, new[j][1], aim)
    pad = jnp.zeros((GATES - ST, GATES), f32)
    wr = rows(are, pad).T[ST : ST + 1]
    wi = rows(aim, pad).T[ST : ST + 1]
    lane1 = iota((1, GATES), 1)
    w = jnp.where(lane1 < ST, wr, jnp.where(lane1 < 2 * ST, pltpu.roll(wi, ST, 1), 0.0))
    for j in range(64):
        out[j] = w


def solve(parts, sr, si):
    return pl.pallas_call(
        solve_kernel,
        out_shape=jax.ShapeDtypeStruct((64, 1, GATES), f32),
        in_specs=[VM] * 3,
        out_specs=VM,
        name="solve",
        compiler_params=pltpu.CompilerParams(vmem_limit_bytes=VMEM_LIMIT),
    )(parts, sr, si)


def power_kernel(place, near, far, w, out):
    core, dop = core_and_dop()
    zero = jnp.zeros((32, 2 * GATES), bf16)
    row = iota((8, GATES), 0)
    lane = iota((8, GATES), 1)

    def one(k, i):
        z = dop ^ k
        wt = jnp.broadcast_to(w[z * 16 + i], (8, GATES))
        turned = jnp.where(
            lane < ST,
            -pltpu.roll(wt, GATES - ST, 1),
            jnp.where(lane < 2 * ST, pltpu.roll(wt, ST, 1), 0.0),
        )
        wt = jnp.where(row % 2 == 0, wt, turned)
        hi = wt.astype(bf16).astype(f32)
        mid = (wt - hi).astype(bf16).astype(f32)
        lo = wt - hi - mid
        wt = jnp.where(row < 2, hi, jnp.where(row < 4, mid, jnp.where(row < 6, lo, 0.0)))
        lhs = rows(wt, jnp.zeros((8, GATES), f32)).astype(bf16)
        rhs = [[], [], []]
        for p in range(2):
            for t in range(SLOTS):
                s = place[(z * 16 + i) * SLOTS + t]
                x = lanes(near[p, s], far[p, s])
                hi, rest = split(x)
                x = x - hi.astype(f32)
                rhs[0].append(hi)
                rhs[1].append(rest)
                rhs[2].append((x - rest.astype(f32)).astype(bf16))
        rhs = [*rhs[0], zero, *rhs[1], zero, *rhs[2], zero]
        y = jnp.dot(lanes(lhs, lhs, lhs), rows(*rhs), preferred_element_type=f32)
        re = y[0:1] + y[2:3] + y[4:5]
        im = y[1:2] + y[3:4] + y[5:6]
        return re * re + im * im

    def step(j, c):
        k = j // 2
        i = (j % 2) * 8
        y = rows(*[one(k, i + n) for n in range(8)])
        at = pl.ds(pl.multiple_of(i, 8), 8)
        out[k, 0, at, :] = y[:, :GATES]
        out[k, 1, at, :] = y[:, GATES:]
        return c

    lax.fori_loop(0, 8, step, 0, unroll=UNROLL)


def power(place, near, far, w):
    return pl.pallas_call(
        power_kernel,
        out_shape=jax.ShapeDtypeStruct((ZN, 2, 16, GATES), f32),
        in_specs=[SM] + [VM] * 3,
        out_specs=VM,
        name="power",
        compiler_params=pltpu.CompilerParams(vmem_limit_bytes=VMEM_LIMIT),
    )(place, near, far, w)


def window_sums(p, g, t, left_tiles, right_tiles):
    width = p.shape[1]
    total = p
    acc = None
    for bit in (0, 2, 4):
        k = 1 << bit
        digit = (t >> bit) & 3
        shifted = [total] + [pltpu.roll(total, width - j * k, 1) for j in (1, 2, 3)]
        two = shifted[0] + shifted[1]
        three = two + shifted[2]
        part = jnp.where(digit == 1, total, jnp.where(digit == 2, two, three))
        if acc is None:
            acc = jnp.where(digit == 0, 0.0, part)
        else:
            moved = [pltpu.roll(acc, width - j * k, 1) for j in (1, 2, 3)]
            moved = jnp.where(digit == 1, moved[0], jnp.where(digit == 2, moved[1], moved[2]))
            acc = jnp.where(digit == 0, acc, part + moved)
        total = two + (shifted[2] + shifted[3])
    acc = jnp.where(t == 64, total, acc)
    tiles = [acc[:, j : j + GATES] for j in range(0, width, GATES)]
    lane = iota(tiles[0].shape, 1)

    def taken(j, other, shift, inside):
        at = (lane + shift) & (GATES - 1)
        here = jnp.take_along_axis(tiles[j], at, 1)
        return jnp.where(inside, here, jnp.take_along_axis(tiles[other], at, 1))

    back, ahead = -(g + t), g + 1
    left = [taken(j, j - 1, back, lane + back >= 0) for j in left_tiles]
    right = [taken(j, j + 1, ahead, lane + ahead < GATES) for j in right_tiles]
    return left, right


def noise_kernel(p0, p1, p2, p3, guard, train, whole, edge, line, ready, sem):
    core, dop = core_and_dop()
    rank = lax.axis_index("range")
    for k, ref in enumerate((p0, p1, p2, p3)):
        at = 1 + (dop ^ k)
        line[at, core] = ref[0]
        line[at, 1 - core] = ref[1]
    source = dop ^ (3 * core)
    for slot, half in ((2, core), (3, 1 - core)):
        value = p0[slot]
        for k, ref in ((1, p1), (2, p2), (3, p3)):
            value = jnp.where(source == k, ref[slot], value)
        line[5 * (1 - core), half] = value
    line[5 * core] = jnp.zeros((2, 16, GATES), f32)
    p = lanes(*[rows(line[j, 0], line[j, 1]) for j in range(6)])
    g = guard[:, :1]
    t = train[:, :1]
    left, right = window_sums(p, g, t, (1, 2, 3, 4), (1, 2, 3, 4))
    lo, hi = GATES, GATES + 4 * GATES
    pos = rank * (4 * GATES) + iota((32, 4 * GATES), 1)
    left_count = jnp.maximum(jnp.minimum(pos - g - 1, TOTAL - 1) - jnp.maximum(pos - g - t, 0) + 1, 0)
    right_count = jnp.maximum(jnp.minimum(pos + g + t, TOTAL - 1) - jnp.maximum(pos + g + 1, 0) + 1, 0)
    sums = lanes(*left) + lanes(*right)
    count = (left_count + right_count).astype(f32)
    p = p[:, lo:hi]
    ready[...] = p / (sums / count + EPS)
    copy = pltpu.make_async_copy(ready, whole, sem)
    copy.start()
    for j, value in enumerate((p, sums, count)):
        edge[j] = jnp.where(core == 0, value[:, :GATES], value[:, 3 * GATES :])
    copy.wait()


def noise(pieces, guard, train):
    return pl.pallas_call(
        noise_kernel,
        out_shape=[
            pltpu.HBM((32, 4 * GATES), f32),
            jax.ShapeDtypeStruct((3, 32, GATES), f32),
        ],
        in_specs=[VM] * 6,
        out_specs=[pl.BlockSpec(memory_space=pltpu.HBM), VM],
        scratch_shapes=[
            pltpu.VMEM((6, 2, 16, GATES), f32),
            pltpu.VMEM((32, 4 * GATES), f32),
            pltpu.SemaphoreType.DMA,
        ],
        name="noise",
        compiler_params=pltpu.CompilerParams(vmem_limit_bytes=VMEM_LIMIT),
    )(*pieces, guard, train)


def cfar_kernel(whole, edge, outer, guard, train, out, line, ready, sem):
    core, _ = core_and_dop()
    line[core, 1 - core] = outer[0]
    line[core, core] = outer[1]
    line[1 - core] = jnp.zeros((2, 16, GATES), f32)
    p = lanes(*[rows(line[j, 0], line[j, 1]) for j in range(2)])
    left, right = window_sums(p, guard[:, :1], train[:, :1], (1,), (0,))
    sums = edge[1] + jnp.where(core == 0, left[0], right[0])
    ready[...] = edge[0] / (sums / edge[2] + EPS)
    at = pl.multiple_of(core * (3 * GATES), GATES)
    copy = pltpu.make_async_copy(ready, out.at[:, pl.ds(at, GATES)], sem)
    copy.start()
    copy.wait()


def cfar(known, outer, guard, train):
    hbm = pl.BlockSpec(memory_space=pltpu.HBM)
    return pl.pallas_call(
        cfar_kernel,
        out_shape=pltpu.HBM((32, 4 * GATES), f32),
        in_specs=[hbm] + [VM] * 4,
        out_specs=hbm,
        scratch_shapes=[
            pltpu.VMEM((2, 2, 16, GATES), f32),
            pltpu.VMEM((32, GATES), f32),
            pltpu.SemaphoreType.DMA,
        ],
        input_output_aliases={0: 0},
        name="cfar",
        compiler_params=pltpu.CompilerParams(vmem_limit_bytes=VMEM_LIMIT),
    )(*known, outer, guard, train)


BOTH = ("range", "dop")
CORE_SWAP = [(i, i ^ 1) for i in range(32)]
SAME_CORE = [
    [((y * XN + x) * 2 + c) * ZN + z for z in range(ZN) for y in range(YN) for x in range(XN)]
    for c in range(2)
]


def flipped(bit):
    return [(i, i ^ bit) for i in range(ZN)]


def swap(value):
    return lax.ppermute(value, "range", CORE_SWAP)


def steering(bin_taper, phases):
    core, dop = core_and_dop()
    b = dop * 32 + core * 16 + lax.axis_index("range") // 2
    taper = lax.dynamic_index_in_dim(bin_taper, b, 0, keepdims=False)

    def lay(values):
        return jnp.broadcast_to((taper[:, None] * values[None, :]).reshape(ST, 1), (ST, GATES))

    return lay(jnp.cos(phases)), lay(jnp.sin(phases))


def shards(echoes, triplet, bin_taper, phases, excluded, guard_len, train_len):
    core, dop = core_and_dop()
    place = places(triplet)
    other = swap(excluded)
    near, far = pack(echoes)
    far, other = lax.optimization_barrier((far, other))
    far = swap(far)
    mine = lax.dynamic_slice_in_dim(lanes(excluded, other), core * 16, 16, 0)
    m1, m2, m3 = [lax.ppermute(mine, "dop", flipped(k)) for k in (1, 2, 3)]
    part = gram(False, place, near, far, [mine, m1])
    part = gram(True, place, near, far, [m2, m3, part])
    part = lax.all_to_all(part, BOTH, 0, 0, tiled=True, axis_index_groups=SAME_CORE)
    sr, si = steering(bin_taper, phases)
    guard = jnp.broadcast_to(guard_len[:, None], (32, GATES))
    train = jnp.broadcast_to(train_len[:, None], (32, GATES))
    sr, si, guard, train = lax.optimization_barrier((sr, si, guard, train))
    w = solve(part, sr, si)
    w = lax.all_to_all(w, BOTH, 0, 0, tiled=True, axis_index_groups=SAME_CORE)
    mine = power(place, near, far, w)
    came = swap(mine)
    pieces = [jnp.stack([mine[k, 0], came[k, 1], mine[k, 1], came[k, 0]]) for k in range(ZN)]
    pieces = [pieces[0]] + [lax.ppermute(pieces[k], "dop", flipped(k)) for k in (1, 2, 3)]
    ranges = lax.axis_size("range")
    p0, p1, p2, p3 = [p[:2] for p in pieces]
    tail = jnp.where(dop == 0, p3, jnp.where(dop == 1, p2, jnp.where(dop == 2, p1, p0)))
    head = jnp.where(dop == 0, p0, jnp.where(dop == 1, p1, jnp.where(dop == 2, p2, p3)))
    pairs = [(i, i + 1 if i % 2 else i - 1) for i in range(1, ranges - 1)]
    outer = lax.ppermute(jnp.where(core == 0, head, tail), "range", pairs)
    return cfar(noise(pieces, guard, train), outer, guard, train)


def solution(mesh):
    placed = (
        P(None, None, None, ("range", "dop")),
        P(),
        P(),
        P(),
        P("dop", "range"),
        P("dop"),
        P("dop"),
    )
    return jax.shard_map(
        shards, mesh=mesh, in_specs=placed, out_specs=P("dop", "range"), check_vma=False
    )
```

```python
import functools
import jax
import jax.numpy as jnp
from jax import lax
from jax.experimental import pallas as pl
from jax.experimental.pallas import tpu as pltpu
from jax.sharding import PartitionSpec as P

CH = 16
SLOTS = 3
ST = 48
BINS = 128
BLOCK = 16
GATES = 128
TOTAL = 16384
EPS = 1e-6
HALF = 64
XN = 4
YN = 4
ZN = 4
WINDOW = 20
PACKED = ST * ST
UNROLL = 8
f32 = jnp.float32
bf16 = jnp.bfloat16
VMEM_LIMIT = 16 * 2**20

VM = pl.BlockSpec(memory_space=pltpu.VMEM)
SM = pl.BlockSpec(memory_space=pltpu.SMEM)


def core_and_dop():
    return lax.axis_index("range") % 2, lax.axis_index("dop")


def iota(shape, dim):
    return lax.broadcasted_iota(jnp.int32, shape, dim)


def split(x):
    hi = x.astype(bf16)
    return hi, (x - hi.astype(f32)).astype(bf16)


def lanes(*parts):
    return jnp.concatenate(parts, 1)


def rows(*parts):
    return jnp.concatenate(parts, 0)


def pack_kernel(echo, near, send, stage, sems):
    core, _ = core_and_dop()
    loads = []
    for out, half in ((stage, 1 - core), (near, core)):
        for z in range(ZN):
            first = z * 32 + half * 16
            for start, at, count in (
                (first, 2, 16),
                ((first + BINS - 2) % BINS, 0, 2),
                ((first + 16) % BINS, 18, 2),
            ):
                loads.append(
                    pltpu.make_async_copy(
                        echo.at[:, pl.ds(start, count)],
                        out.at[:, pl.ds(z * WINDOW + at, count)],
                        sems.at[len(loads)],
                    )
                )
    for c in loads:
        c.start()
    stores = []
    for z in range(ZN):
        for c in loads[3 * z : 3 * z + 3]:
            c.wait()
        part = pl.ds(z * WINDOW, WINDOW)
        stores.append(
            pltpu.make_async_copy(stage.at[:, part], send.at[:, part], sems.at[6 * ZN + z])
        )
        stores[-1].start()
    for c in loads[3 * ZN :] + stores:
        c.wait()


def pack(echo):
    packed = (2, ZN * WINDOW, CH, GATES)
    return pl.pallas_call(
        pack_kernel,
        out_shape=[jax.ShapeDtypeStruct(packed, f32), pltpu.HBM(packed, f32)],
        in_specs=[pl.BlockSpec(memory_space=pltpu.HBM)],
        out_specs=[VM, pl.BlockSpec(memory_space=pltpu.HBM)],
        scratch_shapes=[pltpu.VMEM(packed, f32), pltpu.SemaphoreType.DMA((7 * ZN,))],
        name="pack",
        compiler_params=pltpu.CompilerParams(vmem_limit_bytes=52 * 2**20),
    )(echo)


def places(triplet):
    core, _ = core_and_dop()
    mine = lax.dynamic_index_in_dim(triplet.reshape(ZN, 2, 16, SLOTS), core, 1, keepdims=False)
    group = iota((ZN, 16, SLOTS), 0)
    where = group * WINDOW + ((mine - (group * 32 + core * 16) + BINS + 2) & (BINS - 1))
    return where.reshape(ZN * 16 * SLOTS)


def gram_kernel(second, place, near, far, *refs):
    masks = refs[: 1 if second else 2]
    if second:
        done, whole, kept, out, sems = refs[1:]
    else:
        out, kept = refs[2:]
    _, dop = core_and_dop()
    block = dop * (GATES // BLOCK) + (iota((64, 2 * GATES), 1) % GATES) // BLOCK
    block = block + 32 * (iota((64, 2 * GATES), 1) // GATES)
    pick = (iota((64, 2 * GATES), 0) == block).astype(f32)
    left = 1.0 - jnp.dot(rows(*[m[...] for m in masks]).astype(f32), pick, preferred_element_type=f32)
    for k in range(2):
        kept[k] = left[16 * k : 16 * k + 16]
    zero = jnp.zeros((16, 4 * GATES), bf16)
    base = 2 if second else 0

    def operands(k, i):
        z = dop ^ (base + k)
        m = kept[k, pl.ds(i, 1), :]
        mn = jnp.broadcast_to(m[:, :GATES], (CH, GATES)).astype(bf16)
        mf = jnp.broadcast_to(m[:, GATES:], (CH, GATES)).astype(bf16)
        hi, lo, left, right, rest, last = [], [], [], [], [], []
        for t in range(SLOTS):
            s = place[(z * 16 + i) * SLOTS + t]
            un, uf, vn, vf = split(near[0, s]), split(far[0, s]), split(near[1, s]), split(far[1, s])
            hi.append(lanes(un[0], uf[0], vn[0], vf[0]))
            lo.append(lanes(un[1], uf[1], vn[1], vf[1]))
            a, c, d, e = un[0] * mn, uf[0] * mf, vn[0] * mn, vf[0] * mf
            left.append(lanes(a, c, d, e))
            right.append(lanes(d, e, -a, -c))
            a, c, d, e = un[1] * mn, uf[1] * mf, vn[1] * mn, vf[1] * mf
            rest.append(lanes(a, c, d, e))
            last.append(lanes(d, e, -a, -c))
        return hi, lo, rows(*left, *right, *rest, *last)

    row = iota((ST, GATES), 0)
    lane = iota((ST, GATES), 1)
    low = row >= lane % HALF
    first = lane < HALF
    lane16 = iota((CH, GATES), 1)
    mine8 = iota((8, GATES), 1) // 16 == iota((8, GATES), 0)

    def store(k, i, p):
        q = k * 16 + i
        p0, p1 = p[:16], pltpu.roll(p[16:32], 48, 1)
        p2 = pltpu.roll(p[32:], 96, 1)
        tail = [pltpu.roll(p2[h : h + 8], 0, 1, stride=16, stride_axis=0) for h in (0, 8)]
        main = jnp.where(lane16 < 48, p0, jnp.where(lane16 < 96, p1, p2))
        for j in range(16):
            out[q, :, j * GATES : (j + 1) * GATES] = main[j : j + 1]
        for j in range(2):
            extra = jnp.sum(jnp.where(mine8, tail[j], 0.0), 0, keepdims=True)
            out[q, :, (16 + j) * GATES : (17 + j) * GATES] = extra

    def pair(k, i):
        ha, wa, la = operands(k, i)
        hb, wb, lb = operands(k, i + 1)
        rhs = rows(*ha, zero, *hb, zero, *wa, zero, *wb, zero)
        dims = (((1,), (1,)), ((), ()))
        g = lax.dot_general(rows(la, lb), rhs, dims, preferred_element_type=f32)
        ga, gb = g[:192], g[192:]
        ga = ga[:96] + ga[96:]
        gb = gb[:96] + gb[96:]
        ga = ga[:, :GATES] + ga[:, GATES:]
        gb = gb[:, :GATES] + gb[:, GATES:]
        re = jnp.where(first, ga[:ST], gb[:ST])
        im = jnp.where(first, ga[ST:], gb[ST:])
        p = jnp.where(low, re, im)
        store(k, i, p)
        store(k, i + 1, pltpu.roll(p, HALF, 1))

    copies = []

    def ship(value, k):
        first = pl.multiple_of((dop ^ k) * 16, 16)
        copies.append(
            pltpu.make_async_copy(
                value.at[pl.ds((k % 2) * 16, 16)], whole.at[pl.ds(first, 16)], sems.at[k]
            )
        )
        copies[-1].start()

    if second:
        ship(done, 0)
        ship(done, 1)
    for k in range(2):
        for i in range(0, 16, 2):
            pair(k, i)
        if second:
            ship(out, 2 + k)
    for c in copies:
        c.wait()


def gram(second, place, near, far, extra):
    block = (32, 1, PACKED)
    kept = pltpu.VMEM((2, 16, 2 * GATES), f32)
    return pl.pallas_call(
        functools.partial(gram_kernel, second),
        out_shape=pltpu.HBM((64, 1, PACKED), f32) if second else jax.ShapeDtypeStruct(block, f32),
        in_specs=[SM] + [VM] * 4,
        out_specs=pl.BlockSpec(memory_space=pltpu.HBM) if second else VM,
        scratch_shapes=[kept, pltpu.VMEM(block, f32), pltpu.SemaphoreType.DMA((4,))] if second else [kept],
        name="gram_b" if second else "gram_a",
        compiler_params=pltpu.CompilerParams(vmem_limit_bytes=VMEM_LIMIT),
    )(place, near, far, *extra)


def plus(a, b):
    return a[0] + b[0], a[1] + b[1]


def minus(a, b):
    return a[0] - b[0], a[1] - b[1]


def times(a, b):
    return a[0] * b[0] - a[1] * b[1], a[0] * b[1] + a[1] * b[0]


def inner(a, b):
    return a[0] * b[0] + a[1] * b[1], a[0] * b[1] - a[1] * b[0]


def half_inverse(a, d, b):
    inv = 1.0 / (a * d - (b[0] * b[0] + b[1] * b[1]))
    a, d, b = a * inv, d * inv, (b[0] * inv, b[1] * inv)

    def apply(u, v):
        bv, bu = times(b, v), inner(b, u)
        return (d * u[0] - bv[0], d * u[1] - bv[1]), (a * v[0] - bu[0], a * v[1] - bu[1])

    return apply


def solve_kernel(parts, sr, si, out):
    row = iota((ST, GATES), 0)
    lane = iota((ST, GATES), 1)
    total = parts[0]
    for j in range(1, 64):
        total = total + parts[j]
    total = total * (1.0 / TOTAL)
    line = [total[:, j : j + GATES] for j in range(0, PACKED, GATES)]
    main = rows(*line[:16])
    corner = rows(*[pltpu.roll(line[16 + j // 8], (GATES + 32 - 16 * (j % 8)) % GATES, 1) for j in range(16)])
    p2 = jnp.where(lane[:16] < 32, pltpu.roll(main, 32, 1), corner)
    p = rows(main, pltpu.roll(main, GATES - 48, 1), p2)
    full = rows(p, jnp.zeros((GATES - ST, GATES), f32)).T[:ST]
    re = jnp.where(row >= lane, p, full)
    im = jnp.where(row < lane, p, jnp.where(row == lane, 0.0, -full))
    are = jnp.where(lane < ST, re, sr[...])
    aim = jnp.where(lane < ST, im, si[...])
    for k in range(0, ST, 4):
        cols = []
        for j in range(4):
            at = jnp.full((ST, GATES), k + j, jnp.int32)
            cols.append((jnp.take_along_axis(are, at, 1), jnp.take_along_axis(aim, at, 1)))
        piv = [[(c[0][k + i : k + i + 1], c[1][k + i : k + i + 1]) for c in cols] for i in range(4)]
        r = [(are[k + i : k + i + 1], aim[k + i : k + i + 1]) for i in range(4)]
        first = half_inverse(piv[0][0][0], piv[1][1][0], piv[0][1])
        x = first(r[0], r[1])
        y2 = first(piv[0][2], piv[1][2])
        y3 = first(piv[0][3], piv[1][3])
        t2 = minus(piv[2][2], plus(inner(piv[0][2], y2[0]), inner(piv[1][2], y2[1])))
        t3 = minus(piv[3][3], plus(inner(piv[0][3], y3[0]), inner(piv[1][3], y3[1])))
        t23 = minus(piv[2][3], plus(inner(piv[0][2], y3[0]), inner(piv[1][2], y3[1])))
        r2 = minus(r[2], plus(inner(piv[0][2], x[0]), inner(piv[1][2], x[1])))
        r3 = minus(r[3], plus(inner(piv[0][3], x[0]), inner(piv[1][3], x[1])))
        n2, n3 = half_inverse(t2[0], t3[0], t23)(r2, r3)
        n0 = minus(x[0], plus(times(y2[0], n2), times(y3[0], n3)))
        n1 = minus(x[1], plus(times(y2[1], n2), times(y3[1], n3)))
        new = (n0, n1, n2, n3)
        ur, ui = times(cols[0], n0)
        for j in range(1, 4):
            ur, ui = plus((ur, ui), times(cols[j], new[j]))
        are, aim = are - ur, aim - ui
        for j in range(4):
            are = jnp.where(row == k + j, new[j][0], are)
            aim = jnp.where(row == k + j, new[j][1], aim)
    pad = jnp.zeros((GATES - ST, GATES), f32)
    wr = rows(are, pad).T[ST : ST + 1]
    wi = rows(aim, pad).T[ST : ST + 1]
    lane1 = iota((1, GATES), 1)
    w = jnp.where(lane1 < ST, wr, jnp.where(lane1 < 2 * ST, pltpu.roll(wi, ST, 1), 0.0))
    for j in range(64):
        out[j] = w


def solve(parts, sr, si):
    return pl.pallas_call(
        solve_kernel,
        out_shape=jax.ShapeDtypeStruct((64, 1, GATES), f32),
        in_specs=[VM] * 3,
        out_specs=VM,
        name="solve",
        compiler_params=pltpu.CompilerParams(vmem_limit_bytes=VMEM_LIMIT),
    )(parts, sr, si)


def power_kernel(place, near, far, w, out):
    _, dop = core_and_dop()
    zero = jnp.zeros((32, 2 * GATES), bf16)
    row = iota((8, GATES), 0)
    lane = iota((8, GATES), 1)

    def one(k, i):
        z = dop ^ k
        wt = jnp.broadcast_to(w[z * 16 + i], (8, GATES))
        turned = jnp.where(
            lane < ST,
            -pltpu.roll(wt, GATES - ST, 1),
            jnp.where(lane < 2 * ST, pltpu.roll(wt, ST, 1), 0.0),
        )
        wt = jnp.where(row % 2 == 0, wt, turned)
        hi = wt.astype(bf16).astype(f32)
        mid = (wt - hi).astype(bf16).astype(f32)
        lo = wt - hi - mid
        wt = jnp.where(row < 2, hi, jnp.where(row < 4, mid, jnp.where(row < 6, lo, 0.0)))
        lhs = rows(wt, jnp.zeros((8, GATES), f32)).astype(bf16)
        rhs = [[], [], []]
        for p in range(2):
            for t in range(SLOTS):
                s = place[(z * 16 + i) * SLOTS + t]
                x = lanes(near[p, s], far[p, s])
                hi, rest = split(x)
                x = x - hi.astype(f32)
                rhs[0].append(hi)
                rhs[1].append(rest)
                rhs[2].append((x - rest.astype(f32)).astype(bf16))
        rhs = [*rhs[0], zero, *rhs[1], zero, *rhs[2], zero]
        y = jnp.dot(lanes(lhs, lhs, lhs), rows(*rhs), preferred_element_type=f32)
        re = y[0:1] + y[2:3] + y[4:5]
        im = y[1:2] + y[3:4] + y[5:6]
        return re * re + im * im

    def step(j, c):
        k = j // 2
        i = (j % 2) * 8
        y = rows(*[one(k, i + n) for n in range(8)])
        at = pl.ds(pl.multiple_of(i, 8), 8)
        out[k, 0, at, :] = y[:, :GATES]
        out[k, 1, at, :] = y[:, GATES:]
        return c

    lax.fori_loop(0, 8, step, 0, unroll=UNROLL)


def power(place, near, far, w):
    return pl.pallas_call(
        power_kernel,
        out_shape=jax.ShapeDtypeStruct((ZN, 2, 16, GATES), f32),
        in_specs=[SM] + [VM] * 3,
        out_specs=VM,
        name="power",
        compiler_params=pltpu.CompilerParams(vmem_limit_bytes=VMEM_LIMIT),
    )(place, near, far, w)


def window_sums(p, g, t, left_tiles, right_tiles):
    width = p.shape[1]
    total = p
    acc = None
    for bit in (0, 2, 4):
        k = 1 << bit
        digit = (t >> bit) & 3
        shifted = [total] + [pltpu.roll(total, width - j * k, 1) for j in (1, 2, 3)]
        two = shifted[0] + shifted[1]
        three = two + shifted[2]
        part = jnp.where(digit == 1, total, jnp.where(digit == 2, two, three))
        if acc is None:
            acc = jnp.where(digit == 0, 0.0, part)
        else:
            moved = [pltpu.roll(acc, width - j * k, 1) for j in (1, 2, 3)]
            moved = jnp.where(digit == 1, moved[0], jnp.where(digit == 2, moved[1], moved[2]))
            acc = jnp.where(digit == 0, acc, part + moved)
        total = two + (shifted[2] + shifted[3])
    acc = jnp.where(t == 64, total, acc)
    tiles = [acc[:, j : j + GATES] for j in range(0, width, GATES)]
    lane = iota(tiles[0].shape, 1)

    def taken(j, other, shift, inside):
        at = (lane + shift) & (GATES - 1)
        here = jnp.take_along_axis(tiles[j], at, 1)
        return jnp.where(inside, here, jnp.take_along_axis(tiles[other], at, 1))

    back, ahead = -(g + t), g + 1
    left = [taken(j, j - 1, back, lane + back >= 0) for j in left_tiles]
    right = [taken(j, j + 1, ahead, lane + ahead < GATES) for j in right_tiles]
    return left, right


def noise_kernel(p0, p1, p2, p3, guard, train, whole, edge, line, ready, sem):
    core, dop = core_and_dop()
    rank = lax.axis_index("range")
    for k, ref in enumerate((p0, p1, p2, p3)):
        at = 1 + (dop ^ k)
        line[at, core] = ref[0]
        line[at, 1 - core] = ref[1]
    source = dop ^ (3 * core)
    for slot, half in ((2, core), (3, 1 - core)):
        value = p0[slot]
        for k, ref in ((1, p1), (2, p2), (3, p3)):
            value = jnp.where(source == k, ref[slot], value)
        line[5 * (1 - core), half] = value
    line[5 * core] = jnp.zeros((2, 16, GATES), f32)
    p = lanes(*[rows(line[j, 0], line[j, 1]) for j in range(6)])
    g = guard[:, :1]
    t = train[:, :1]
    left, right = window_sums(p, g, t, (1, 2, 3, 4), (1, 2, 3, 4))
    lo, hi = GATES, GATES + 4 * GATES
    pos = rank * (4 * GATES) + iota((32, 4 * GATES), 1)
    left_count = jnp.maximum(jnp.minimum(pos - g - 1, TOTAL - 1) - jnp.maximum(pos - g - t, 0) + 1, 0)
    right_count = jnp.maximum(jnp.minimum(pos + g + t, TOTAL - 1) - jnp.maximum(pos + g + 1, 0) + 1, 0)
    sums = lanes(*left) + lanes(*right)
    count = (left_count + right_count).astype(f32)
    p = p[:, lo:hi]
    ready[...] = p / (sums / count + EPS)
    copy = pltpu.make_async_copy(ready, whole, sem)
    copy.start()
    for j, value in enumerate((p, sums, count)):
        edge[j] = jnp.where(core == 0, value[:, :GATES], value[:, 3 * GATES :])
    copy.wait()


def noise(pieces, guard, train):
    return pl.pallas_call(
        noise_kernel,
        out_shape=[
            pltpu.HBM((32, 4 * GATES), f32),
            jax.ShapeDtypeStruct((3, 32, GATES), f32),
        ],
        in_specs=[VM] * 6,
        out_specs=[pl.BlockSpec(memory_space=pltpu.HBM), VM],
        scratch_shapes=[
            pltpu.VMEM((6, 2, 16, GATES), f32),
            pltpu.VMEM((32, 4 * GATES), f32),
            pltpu.SemaphoreType.DMA,
        ],
        name="noise",
        compiler_params=pltpu.CompilerParams(vmem_limit_bytes=VMEM_LIMIT),
    )(*pieces, guard, train)


def cfar_kernel(whole, edge, outer, guard, train, out, line, ready, sem):
    core, _ = core_and_dop()
    line[core, 1 - core] = outer[0]
    line[core, core] = outer[1]
    line[1 - core] = jnp.zeros((2, 16, GATES), f32)
    p = lanes(*[rows(line[j, 0], line[j, 1]) for j in range(2)])
    left, right = window_sums(p, guard[:, :1], train[:, :1], (1,), (0,))
    sums = edge[1] + jnp.where(core == 0, left[0], right[0])
    ready[...] = edge[0] / (sums / edge[2] + EPS)
    at = pl.multiple_of(core * (3 * GATES), GATES)
    copy = pltpu.make_async_copy(ready, out.at[:, pl.ds(at, GATES)], sem)
    copy.start()
    copy.wait()


def cfar(known, outer, guard, train):
    hbm = pl.BlockSpec(memory_space=pltpu.HBM)
    return pl.pallas_call(
        cfar_kernel,
        out_shape=pltpu.HBM((32, 4 * GATES), f32),
        in_specs=[hbm] + [VM] * 4,
        out_specs=hbm,
        scratch_shapes=[
            pltpu.VMEM((2, 2, 16, GATES), f32),
            pltpu.VMEM((32, GATES), f32),
            pltpu.SemaphoreType.DMA,
        ],
        input_output_aliases={0: 0},
        name="cfar",
        compiler_params=pltpu.CompilerParams(vmem_limit_bytes=VMEM_LIMIT),
    )(*known, outer, guard, train)


BOTH = ("range", "dop")
CORE_SWAP = [(i, i ^ 1) for i in range(32)]
SAME_CORE = [
    [((y * XN + x) * 2 + c) * ZN + z for z in range(ZN) for y in range(YN) for x in range(XN)]
    for c in range(2)
]


def flipped(bit):
    return [(i, i ^ bit) for i in range(ZN)]


def swap(value):
    return lax.ppermute(value, "range", CORE_SWAP)


def steering(bin_taper, phases):
    core, dop = core_and_dop()
    b = dop * 32 + core * 16 + lax.axis_index("range") // 2
    taper = lax.dynamic_index_in_dim(bin_taper, b, 0, keepdims=False)

    def lay(values):
        return jnp.broadcast_to((taper[:, None] * values[None, :]).reshape(ST, 1), (ST, GATES))

    return lay(jnp.cos(phases)), lay(jnp.sin(phases))


def shards(echoes, triplet, bin_taper, phases, excluded, guard_len, train_len):
    core, dop = core_and_dop()
    place = places(triplet)
    other = swap(excluded)
    near, far = pack(echoes)
    far, other = lax.optimization_barrier((far, other))
    far = swap(far)
    mine = lax.dynamic_slice_in_dim(lanes(excluded, other), core * 16, 16, 0)
    m1 = lax.ppermute(mine, "dop", flipped(1))
    m2 = lax.ppermute(rows(mine, m1), "dop", flipped(2))
    part = gram(False, place, near, far, [mine, m1])
    part = gram(True, place, near, far, [m2, part])
    part = lax.all_to_all(part, BOTH, 0, 0, tiled=True, axis_index_groups=SAME_CORE)
    sr, si = steering(bin_taper, phases)
    guard = jnp.broadcast_to(guard_len[:, None], (32, GATES))
    train = jnp.broadcast_to(train_len[:, None], (32, GATES))
    sr, si, guard, train = lax.optimization_barrier((sr, si, guard, train))
    w = solve(part, sr, si)
    w = lax.all_to_all(w, BOTH, 0, 0, tiled=True, axis_index_groups=SAME_CORE)
    mine = power(place, near, far, w)
    came = swap(mine)
    pieces = [jnp.stack([mine[k, 0], came[k, 1], mine[k, 1], came[k, 0]]) for k in range(ZN)]
    p2 = lax.ppermute(pieces[2], "dop", flipped(2))
    p1, p3 = [lax.ppermute(pieces[k], "dop", flipped(k)) for k in (1, 3)]
    pieces = [pieces[0], p1, p2, p3]
    ranges = lax.axis_size("range")
    p0, p1, p2, p3 = [p[:2] for p in pieces]
    tail = jnp.where(dop == 0, p3, jnp.where(dop == 1, p2, jnp.where(dop == 2, p1, p0)))
    head = jnp.where(dop == 0, p0, jnp.where(dop == 1, p1, jnp.where(dop == 2, p2, p3)))
    pairs = [(i, i + 1 if i % 2 else i - 1) for i in range(1, ranges - 1)]
    outer = lax.ppermute(jnp.where(core == 0, head, tail), "range", pairs)
    return cfar(noise(pieces, guard, train), outer, guard, train)


def solution(mesh):
    placed = (
        P(None, None, None, ("range", "dop")),
        P(),
        P(),
        P(),
        P("dop", "range"),
        P("dop"),
        P("dop"),
    )
    return jax.shard_map(
        shards, mesh=mesh, in_specs=placed, out_specs=P("dop", "range"), check_vma=False
    )
```
